128 devices in a mesh: vx: 8 (over x, z_hi), vy: 16 (over z_lo, y, core).
Axes of the slice: x: 4, y: 4, z: 4 (z_hi: 2, z_lo: 2; z = z_hi * 2 + z_lo), core: 2. Of those that a mesh axis runs over, the one named last changes fastest.
Arguments:
- tokens: bfloat16 [128, 1, 1024, 1024], P(('vx', 'vy')), may hold values from -256 to 256
- var_embed: bfloat16 [91, 1024], replicated, may hold values from -2 to 2
- query: bfloat16 [1024], replicated, may hold values from -6 to 6
- key_weight: bfloat16 [1024, 1024], P('vy'), may hold values from -1 to 1
- value_weight: bfloat16 [1024, 1024], P('vy'), may hold values from -0.1875 to 0.1875
- out_weight: bfloat16 [1024, 1024], P('vy'), may hold values from -0.1875 to 0.1875
- var_slot: int32 [91], replicated, may hold values from 0 to 127, as said below
Outputs:
- aggregated: bfloat16 [1, 1024, 1024], P(None, ('vx', 'vy'))
The draws below stay inside these ranges and needn't reach their ends.
Inputs may be any that keep to these rules, and one draw needn't show every extreme that they name: `var_slot`: distinct slot numbers; at least one device's slot holds a variable.
All inputs are finite; a program needn't handle non-finite values.
Results may differ from the reference program's by a relative error of at most 0.0096.
Values may be sent and summed in bfloat16 or wider, within the bound.
A program may use at most 64 MiB of HBM per device.

```python
import math
import jax
import jax.numpy as jnp
from jax import lax

D = 1024
HEADS = 16
VARS = 91
B = 1
PATCH_DEV = 8
PATCH = 1024
SLOT_DEV = 1
SLOTS = 128


def shared_params(key):
    first, second, third = jax.random.split(jax.random.fold_in(key, 7), 3)
    key_matrix = jax.random.truncated_normal(first, -6.0, 6.0, (D, D), jnp.float32) * D ** (-0.5)
    query_vector = jax.random.truncated_normal(second, -4.0, 4.0, (D,), jnp.float32) * 1.5
    embeddings = jax.random.truncated_normal(third, -4.0, 4.0, (VARS, D), jnp.float32) * 0.5
    return (key_matrix, query_vector, embeddings)


def slot_table(key):
    first, second, third = jax.random.split(jax.random.fold_in(key, 19), 3)
    ranking = jax.random.permutation(first, SLOTS).astype(jnp.int32)
    full_device = jax.random.randint(second, (), 0, SLOTS // SLOT_DEV)
    slot_index = jnp.arange(SLOTS, dtype=jnp.int32)
    priority = jnp.where(slot_index // SLOT_DEV == full_device, slot_index % SLOT_DEV - SLOT_DEV, ranking)
    ordering = jnp.argsort(priority, stable=True)
    occupied = ordering[:VARS]
    return occupied[jax.random.permutation(third, VARS)].astype(jnp.int32)


def draw_var_slot(key, part):
    return slot_table(key)


def draw_key_weight(key, part):
    return shared_params(key)[0].astype(jnp.bfloat16)


def draw_query(key, part):
    return shared_params(key)[1].astype(jnp.bfloat16)


def draw_var_embed(key, part):
    return shared_params(key)[2].astype(jnp.bfloat16)


def draw_tokens(key, part):
    keys_all = jax.random.split(jax.random.fold_in(key, 31), 1)
    return jax.random.truncated_normal(keys_all[0], -6.0, 6.0, (SLOTS, B, PATCH, D), jnp.float32).astype(jnp.bfloat16)


def steps_of(stream_key, extent, cuts, low, largest):
    def one(dim, parts):
        heights = jax.random.uniform(jax.random.fold_in(jax.random.fold_in(stream_key, 6), dim), (parts,), jnp.float32, low / len(cuts), largest / len(cuts))
        return jnp.repeat(jnp.exp(heights), extent[dim] // parts).reshape((-1,) + (1,) * (len(extent) - dim - 1))

    factor_of = one(*cuts[0])
    for cut in cuts[1:]:
        factor_of = factor_of * one(*cut)
    return factor_of


def bell_draw(rng, dims, deviation, reach, cuts=(), kind=jnp.bfloat16):
    array = deviation * jax.random.normal(rng, dims, jnp.float32)
    if cuts:
        array = array * steps_of(rng, dims, cuts, -0.22, 0.18)
    return jnp.clip(array, -reach, reach).astype(kind)


def setup_inputs(seed: int = 0) -> dict:
    key_list = jax.random.split(jax.random.key(seed), 8)
    return {
        "tokens": draw_tokens(jax.random.fold_in(key_list[7], 71), 0),
        "var_embed": draw_var_embed(jax.random.fold_in(key_list[7], 71), 0),
        "query": draw_query(jax.random.fold_in(key_list[7], 71), 0),
        "key_weight": draw_key_weight(jax.random.fold_in(key_list[7], 71), 0),
        "value_weight": bell_draw(key_list[4], (D, D), D ** -0.5, 0.1875, ((0, 16),)),
        "out_weight": bell_draw(key_list[5], (D, D), D ** -0.5, 0.1875, ((0, 16),)),
        "var_slot": draw_var_slot(jax.random.fold_in(key_list[7], 71), 0),
    }


def reference(tokens, var_embed, query, key_weight, value_weight, out_weight, var_slot):
    head_dim = D // HEADS
    scale = 1.0 / math.sqrt(head_dim)
    query_heads = query.astype(jnp.float32).reshape(HEADS, head_dim)
    embed_float = var_embed.astype(jnp.float32)

    def block(index):
        start = (index * PATCH_DEV).astype(jnp.int32)
        window = lax.dynamic_slice_in_dim(tokens, start, PATCH_DEV, 2)
        selected = jnp.take(window, var_slot.astype(jnp.int32), axis=0)
        mixed = (selected.astype(jnp.float32) + embed_float[:, None, None, :]).astype(jnp.bfloat16)
        flattened = mixed.reshape(-1, D)
        keys = jnp.dot(flattened.astype(jnp.float32), key_weight.astype(jnp.float32), preferred_element_type=jnp.float32).astype(jnp.bfloat16)
        values = jnp.dot(flattened.astype(jnp.float32), value_weight.astype(jnp.float32), preferred_element_type=jnp.float32).astype(jnp.bfloat16)
        keys = keys.reshape(VARS, B, PATCH_DEV, HEADS, head_dim)
        values = values.reshape(VARS, B, PATCH_DEV, HEADS, head_dim)
        scores = jnp.einsum('vbphe,he->vbph', keys.astype(jnp.float32), query_heads) * scale
        highest = lax.optimization_barrier(jnp.max(scores, axis=0, keepdims=True))
        exponent = jnp.exp(scores - highest)
        weights = (exponent / lax.optimization_barrier(jnp.sum(exponent, axis=0, keepdims=True))).astype(jnp.bfloat16)
        context = jnp.einsum('vbph,vbphe->bphe', weights.astype(jnp.float32), values.astype(jnp.float32))
        context = context.astype(jnp.bfloat16).reshape(B * PATCH_DEV, D)
        result = jnp.dot(context.astype(jnp.float32), out_weight.astype(jnp.float32), preferred_element_type=jnp.float32).astype(jnp.bfloat16)
        return result.reshape(B, PATCH_DEV, D)
    blocks = lax.map(block, jnp.arange(PATCH // PATCH_DEV, dtype=jnp.int32))
    return jnp.transpose(blocks, (1, 0, 2, 3)).reshape(B, PATCH, D)
```

```python
import functools

import jax
import jax.numpy as jnp
from jax import lax
from jax.experimental import pallas as pl
from jax.experimental.pallas import tpu as pltpu
from jax.sharding import PartitionSpec as P

MESH = pl.DeviceIdType.MESH
F32, BF16 = jnp.float32, jnp.bfloat16
HEADS = 16
D = 1024
BIG = -1e30

NAT = ("x", "z", "y")
PARTS = ((0, 512, ("x", "y", "z")), (512, 512, ("y", "x", "z")))
SEND_SEMS = 200
DIRECT_OPP = False


def device_of(x, y, z, c):
    return (x * 2 + z // 2, (z % 2) * 8 + y * 2 + c)


class Copies:
    def __init__(self, send, recv, local):
        self.send, self.recv, self.local = send, recv, local
        self.n, self.k, self.open = 0, 0, []

    def remote(self, src, dst, device):
        copy = pltpu.make_async_remote_copy(
            src_ref=src,
            dst_ref=dst,
            send_sem=self.send.at[self.n],
            recv_sem=self.recv.at[self.n],
            device_id=device,
            device_id_type=MESH,
        )
        self.n += 1
        copy.start()
        self.open.append(copy)
        return copy

    def here(self, src, dst):
        copy = pltpu.make_async_copy(src, dst, self.local.at[self.k])
        self.k += 1
        copy.start()
        return copy


def lanes_iota(rows):
    return lax.broadcasted_iota(jnp.int32, (rows, 128), 1)


def hilo(a):
    lane = lanes_iota(a.shape[0])
    high = a.astype(BF16).astype(F32)
    low = pltpu.roll(a - high, 16, axis=1)
    both = jnp.where(lane < 16, high, jnp.where(lane < 32, low, 0.0))
    return both.astype(BF16)


def fold(rows):
    lane = lanes_iota(rows.shape[0])
    rows = jnp.where(lane < 32, rows, 0.0)
    q = rows.shape[0] // 4
    out = rows[:q]
    for g in range(1, 4):
        out = out + pltpu.roll(rows[g * q : (g + 1) * q], 32 * g, axis=1)
    return out


def unfold(packed):
    pieces = [packed]
    for g in range(1, 4):
        pieces.append(pltpu.roll(packed, 128 - 32 * g, axis=1))
    return jnp.concatenate(pieces, axis=0)


def pack_stats(m, l):
    lane = lanes_iota(m.shape[0])
    return jnp.where(lane < 16, m, jnp.where(lane < 32, pltpu.roll(l, 16, axis=1), 0.0))


def merge_stats(stats):
    m = functools.reduce(jnp.maximum, stats)
    scales = [jnp.exp(s - m) for s in stats]
    l = sum(a * pltpu.roll(s, 112, axis=1) for a, s in zip(scales, stats))
    return m, l, scales


def pick(ref, axis, index, lanes, ndim):
    where = [slice(None)] * (ndim + 2)
    where[axis] = index
    where[-1] = lanes
    got = ref[tuple(where)]
    return got.reshape(-1, got.shape[-1])


def kernel(tok, emb, query, wk, wv, wo, vslot, out, wk_v, tokv, mixed, gv, go, V, Pacc, wx, st0, qk_o, qk_p, qkc,
           qkg, qkt, e2, er, used, sc, *rest):
    ssem, rsem, lsem = rest[-3:]
    per_part = [rest[i * 17 : (i + 1) * 17] for i in range(len(PARTS))]
    names = ("s1", "r1", "s2", "r2", "s3", "r3", "m1", "m2", "ts1", "tr1", "ts2", "tr2", "ts3", "tr3", "ax1", "ax2", "ax3")
    T = [dict(zip(names, p)) for p in per_part]
    cp = Copies(ssem, rsem, lsem)

    vx, vy = lax.axis_index("vx"), lax.axis_index("vy")
    x, z = vx // 2, (vx % 2) * 2 + vy // 8
    y, c = (vy // 2) % 4, vy % 2
    zl = z % 2
    zmate = z + 1 - 2 * zl
    me = {"x": x, "y": y, "z": z}

    def peer(dim, offset):
        at = dict(me)
        at[dim] = (me[dim] + offset) % 4
        return device_of(at["x"], at["y"], at["z"], c)

    other = device_of(x, y, z, 1 - c)
    chips = [device_of(x, y, zmate, c)]
    for o in (1, 2, 3):
        chips.append(device_of(x, (y + o) % 4, z, c))
        chips.append(device_of(x, (y + o) % 4, zmate, c))

    load_wk = cp.here(wk, wk_v)
    load_tok = cp.here(tok.at[:, c], tokv.at[0])

    barrier = pltpu.get_barrier_semaphore()
    partners = [other] + [peer(d, o) for d in ("x", "y", "z") for o in (1, 2, 3)]
    partners += [device_of(x, (y + o) % 4, zmate, c) for o in (1, 2, 3)]
    for p in partners:
        pl.semaphore_signal(barrier, inc=1, device_id=p, device_id_type=MESH)

    def row_of(yy, zz, cc):
        return pl.multiple_of(((zz * 4 + yy) * 2 + cc) * 64, 64)

    load_wv = cp.here(wv, gv.at[pl.ds(row_of(y, zl, c), 64), :])
    load_wo = cp.here(wo, go.at[pl.ds(row_of(y, zl, c), 64), :])

    head_lane = lax.broadcasted_iota(jnp.int32, (HEADS, D), 1) // 64
    head_row = lax.broadcasted_iota(jnp.int32, (HEADS, D), 0)
    own_head = head_lane == head_row
    q_matrix = jnp.where(own_head, query[...].astype(F32), 0.0).astype(BF16)
    load_wk.wait()
    nt = (((1,), (1,)), ((), ()))
    qk = lax.dot_general(q_matrix, wk_v[...], nt, preferred_element_type=F32) * 0.125
    qk_hi = qk.astype(BF16)
    qk_lo = (qk - qk_hi.astype(F32)).astype(BF16)
    qk_both = jnp.concatenate([qk_hi, qk_lo], axis=0)
    qk_o[...] = qk_both

    ones = own_head.astype(F32).astype(BF16)
    e2[...] = jnp.concatenate([ones, ones, jnp.zeros((96, D), BF16)], axis=0)
    position = vx * 16 + vy
    partner_pos = position + 1 - 2 * c
    n_vars = vslot.shape[1]
    row8 = lax.broadcasted_iota(jnp.int32, (8, n_vars), 0)
    slot_id = jnp.where(row8 == 0, position, jnp.where(row8 == 1, partner_pos, -1))
    match = (vslot[...] == slot_id).astype(F32)
    er[...] = jnp.dot(match.astype(BF16), emb[...], preferred_element_type=F32)
    used[...] = jnp.broadcast_to(jnp.sum(match, axis=1, keepdims=True), (8, 128))

    pl.semaphore_wait(barrier, len(partners))

    qk_copy = cp.remote(qk_o, qk_p, other)
    tok_copy = cp.remote(tok.at[:, 1 - c], tokv.at[1], other)

    class Gather:
        def __init__(self, src, g, local):
            self.src, self.g = src, g
            local.wait()
            own = row_of(y, zl, c)
            self.from_left = self.put(own, 64, peer("y", 1))
            self.from_right = self.put(own, 64, peer("y", 3))
            self.own_z = self.halves(y)
            self.core = {0: self.put(own, 64, other)}
            self.core_z, self.z = {}, {}

        def put(self, row, rows, device):
            ref = self.g.at[pl.ds(row, rows), :]
            return cp.remote(ref, ref, device)

        def halves(self, yy):
            row = row_of(yy, zl, c)
            return (self.put(row, 32, peer("z", 1)), self.put(pl.multiple_of(row + 32, 32), 32, peer("z", 3)))

        def y_arrived(self):
            self.from_left.wait_recv()
            left = (y + 3) % 4
            self.opp_a = self.put(row_of(left, zl, c), 32, peer("y", 1))
            self.from_right.wait_recv()
            right = (y + 1) % 4
            self.opp_b = self.put(pl.multiple_of(row_of(right, zl, c) + 32, 32), 32, peer("y", 3))

        def y_to_z(self):
            for o in (3, 1):
                self.z[o] = self.halves((y + o) % 4)

        def y_to_core(self):
            for o in (3, 1):
                self.core[o] = self.put(row_of((y + o) % 4, zl, c), 64, other)

        def opp_arrived(self):
            self.opp_a.wait_recv()
            self.opp_b.wait_recv()

        def opp_to_z(self):
            self.z[2] = self.halves((y + 2) % 4)

        def opp_to_core(self):
            self.core[2] = self.put(row_of((y + 2) % 4, zl, c), 64, other)

        def z_arrived(self, o):
            pair = self.own_z if o == 0 else self.z[o]
            pair[0].wait_recv()
            pair[1].wait_recv()
            self.core_z[o] = self.put(row_of((y + o) % 4, 1 - zl, c), 64, other)

        def complete(self, o):
            self.core[o].wait_recv()
            self.core_z[o].wait_recv()

    A = Gather(wv, gv, load_wv)

    qk_copy.wait_recv()
    qk_other = qk_p[...]
    first = jnp.where(c == 0, qk_both.astype(F32), qk_other.astype(F32))
    second = jnp.where(c == 0, qk_other.astype(F32), qk_both.astype(F32))
    qkc[...] = jnp.concatenate([first, second], axis=1).astype(BF16)
    chip = zl * 4 + y
    qk_copies = [cp.remote(qkc, qkg.at[chip], p) for p in chips]

    def mix(k):
        def step(i, carry):
            t = tokv[k, pl.ds(i * 8, 8)].astype(F32).reshape(64, D)
            mixed[pl.ds(pl.multiple_of(k * 512 + i * 64, 64), 64), :] = (t + er[k : k + 1, :]).astype(BF16)
            return carry

        lax.fori_loop(0, 8, step, 0)

    load_tok.wait()
    mix(0)
    tok_copy.wait_recv()
    mix(1)

    A.y_arrived()
    A.y_to_z()
    A.y_to_core()
    B = Gather(wo, go, load_wo) if False else None

    for k in qk_copies:
        k.wait_recv()
    qkg[chip] = qkc[...]
    qkt[...] = jnp.concatenate(
        [jnp.concatenate([qkg[i] for i in range(8)], axis=1), jnp.zeros((96, D), BF16)], axis=0
    )

    def score(i, carry):
        rows = pl.multiple_of(i * 128, 128)
        d = lax.dot_general(mixed[pl.ds(rows, 128), :], qkt[...], nt, preferred_element_type=F32)
        sc[i] = d + pltpu.roll(d, 112, axis=1)
        return carry

    lax.fori_loop(0, 8, score, 0)
    use0, use1 = used[0:1, :], used[1:2, :]

    def pair(i, carry):
        s0 = jnp.where(use0 > 0, sc[i], BIG)
        s1 = jnp.where(use1 > 0, sc[4 + i], BIG)
        m = jnp.maximum(s0, s1)
        w0 = use0 * jnp.exp(s0 - m)
        w1 = use1 * jnp.exp(s1 - m)
        st0[i] = pack_stats(m, w0 + w1).reshape(4, 4, 8, 128)
        rows = pl.ds(pl.multiple_of(i * 128, 128), 128)
        wx[0, rows, :] = jnp.dot(hilo(w0), e2[...], preferred_element_type=F32)
        wx[1, rows, :] = jnp.dot(hilo(w1), e2[...], preferred_element_type=F32)
        return carry

    lax.fori_loop(0, 4, pair, 0)

    for t, (l0, w, dims) in zip(T, PARTS):
        axis = NAT.index(dims[0])
        t["sc1"] = []
        for o in (1, 2, 3):
            rows = pick(st0, axis, (me[dims[0]] + o) % 4, slice(None), 3)
            t["ts1"][o - 1] = fold(rows)
            t["sc1"].append(cp.remote(t["ts1"].at[o - 1], t["tr1"].at[o - 1], peer(dims[0], o)))

    def expand(a, l0, w):
        return jnp.dot(hilo(a), e2[:, l0 : l0 + w], preferred_element_type=F32)

    def stats1():
        for t, (l0, w, dims) in zip(T, PARTS):
            for k in t["sc1"]:
                k.wait_recv()
            own = pick(st0, NAT.index(dims[0]), me[dims[0]], slice(None), 3)
            m, l, scales = merge_stats([own] + [unfold(t["tr1"][o]) for o in range(3)])
            for k, a in enumerate(scales):
                t["ax1"][k] = expand(a, l0, w)
            left = [d for d in NAT if d != dims[0]]
            axis = left.index(dims[1])
            t["st1"] = pack_stats(m, l).reshape(4, 4, 8, 128)
            stats = t["st1"]
            pieces = [(stats[i] if axis == 0 else stats[:, i]).reshape(32, 128) for i in range(4)]
            t["own1"] = choose(pieces, me[dims[1]])
            t["sc2"] = []
            for o in (1, 2, 3):
                t["ts2"][o - 1] = fold(choose(pieces, (me[dims[1]] + o) % 4))
                t["sc2"].append(cp.remote(t["ts2"].at[o - 1], t["tr2"].at[o - 1], peer(dims[1], o)))

    def choose(pieces, index):
        got = pieces[3]
        for i in (2, 1, 0):
            got = jnp.where(index == i, pieces[i], got)
        return got

    def stats2():
        for t, (l0, w, dims) in zip(T, PARTS):
            for k in t["sc2"]:
                k.wait_recv()
            m, l, scales = merge_stats([t["own1"]] + [unfold(t["tr2"][o]) for o in range(3)])
            for k, a in enumerate(scales):
                t["ax2"][k] = expand(a, l0, w)
            stats = pack_stats(m, l)
            pieces = [stats[8 * i : 8 * i + 8] for i in range(4)]
            t["own2"] = choose(pieces, me[dims[2]])
            t["sc3"] = []
            for o in (1, 2, 3):
                t["ts3"][o - 1] = choose(pieces, (me[dims[2]] + o) % 4)
                t["sc3"].append(cp.remote(t["ts3"].at[o - 1], t["tr3"].at[o - 1], peer(dims[2], o)))

    def stats3():
        for t, (l0, w, dims) in zip(T, PARTS):
            for k in t["sc3"]:
                k.wait_recv()
            m, l, scales = merge_stats([t["own2"]] + [t["tr3"][o] for o in range(3)])
            for k, a in enumerate(scales):
                t["ax3"][k] = expand(a / l, l0, w)

    def offsets(o):
        yy = (y + o) % 4
        return pl.multiple_of(yy * 128, 128), pl.multiple_of((4 + yy) * 128, 128)

    def left_rows(start, rows, a, b):
        at = pl.ds(pl.multiple_of(start, rows), rows)
        return jnp.concatenate([mixed[at, pl.ds(a, 128)], mixed[at, pl.ds(b, 128)]], axis=1)

    def group(o, fresh):
        a, b = offsets(o)

        def step(i, carry):
            rhs = jnp.concatenate([gv[pl.ds(a, 128), :], gv[pl.ds(b, 128), :]], axis=0)
            r = jnp.dot(left_rows(i * 256, 256, a, b), rhs, preferred_element_type=F32)
            at = pl.ds(pl.multiple_of(i * 256, 256), 256)
            V[at, :] = r if fresh else V[at, :] + r
            return carry

        lax.fori_loop(0, 4, step, 0)

    def last_group(o, l0, w):
        a, b = offsets(o)
        cols = slice(l0, l0 + w)

        def step(i, carry):
            rhs = jnp.concatenate([gv[pl.ds(a, 128), cols], gv[pl.ds(b, 128), cols]], axis=0)
            total = None
            for k in range(2):
                r = jnp.dot(left_rows(k * 512 + i * 128, 128, a, b), rhs, preferred_element_type=F32)
                at = pl.ds(pl.multiple_of(k * 512 + i * 128, 128), 128)
                part = (V[at, cols] + r) * wx[k, pl.ds(pl.multiple_of(i * 128, 128), 128), cols]
                total = part if total is None else total + part
            Pacc[i, :, :, :, cols] = total.reshape(4, 4, 8, w)
            return carry

        lax.fori_loop(0, 4, step, 0)

    A.opp_arrived()
    A.opp_to_z()
    A.opp_to_core()
    A.z_arrived(0)
    B = Gather(wo, go, load_wo)
    A.complete(0)
    group(0, True)
    stats1()
    A.z_arrived(3)
    A.z_arrived(1)
    A.complete(3)
    group(3, False)
    B.y_arrived()
    B.y_to_core()
    stats2()
    A.complete(1)
    group(1, False)
    A.z_arrived(2)
    stats3()
    A.complete(2)

    for t, (l0, w, dims) in zip(T, PARTS):
        last_group(2, l0, w)
        axis = NAT.index(dims[0])
        t["c1"] = []
        for o in (2, 1, 3):
            t["s1"][o - 1] = pick(Pacc, axis, (me[dims[0]] + o) % 4, slice(l0, l0 + w), 3).astype(BF16)
            t["c1"].append(cp.remote(t["s1"].at[o - 1], t["r1"].at[o - 1], peer(dims[0], o)))
    B.opp_arrived()
    B.opp_to_core()
    B.y_to_z()
    B.opp_to_z()
    B.z_arrived(0)

    for t, (l0, w, dims) in zip(T, PARTS):
        own = pick(Pacc, NAT.index(dims[0]), me[dims[0]], slice(l0, l0 + w), 3)
        total = t["ax1"][0] * own
        for k in t["c1"]:
            k.wait_recv()
        for o in range(3):
            total = total + t["ax1"][o + 1] * t["r1"][o].astype(F32)
        t["m1"][...] = total.reshape(4, 4, 8, w)
        left = [d for d in NAT if d != dims[0]]
        axis = left.index(dims[1])
        t["c2"] = []
        for o in (2, 1, 3):
            t["s2"][o - 1] = pick(t["m1"], axis, (me[dims[1]] + o) % 4, slice(None), 2).astype(BF16)
            t["c2"].append(cp.remote(t["s2"].at[o - 1], t["r2"].at[o - 1], peer(dims[1], o)))

    for t, (l0, w, dims) in zip(T, PARTS):
        left = [d for d in NAT if d != dims[0]]
        own = pick(t["m1"], left.index(dims[1]), me[dims[1]], slice(None), 2)
        total = t["ax2"][0] * own
        for k in t["c2"]:
            k.wait_recv()
        for o in range(3):
            total = total + t["ax2"][o + 1] * t["r2"][o].astype(F32)
        t["m2"][...] = total.reshape(4, 8, w)
        t["c3"] = []
        for o in (2, 1, 3):
            t["s3"][o - 1] = t["m2"][(me[dims[2]] + o) % 4]
            t["c3"].append(cp.remote(t["s3"].at[o - 1], t["r3"].at[o - 1], peer(dims[2], o)))

    for o in (3, 1, 2):
        B.z_arrived(o)
    context = []
    for t, (l0, w, dims) in sorted(zip(T, PARTS), key=lambda tp: tp[1][0]):
        total = t["ax3"][0] * t["m2"][me[dims[2]]]
        for k in t["c3"]:
            k.wait_recv()
        for o in range(3):
            total = total + t["ax3"][o + 1] * t["r3"][o]
        context.append(total)
    for o in (0, 3, 1, 2):
        B.complete(o)
    context = jnp.concatenate(context, axis=1).astype(BF16)
    out[...] = jnp.dot(context, go[...], preferred_element_type=F32).astype(BF16)
    for k in cp.open:
        k.wait_send()


def shards(tokens, var_embed, query, key_weight, value_weight, out_weight, var_slot):
    vm = pl.BlockSpec(memory_space=pltpu.VMEM)
    hbm = pl.BlockSpec(memory_space=pl.ANY)
    V = pltpu.VMEM
    part = []
    for _, w, _ in PARTS:
        part += [
            V((3, 128, w), BF16), V((3, 128, w), BF16),
            V((3, 32, w), BF16), V((3, 32, w), BF16),
            V((3, 8, w), F32), V((3, 8, w), F32),
            V((4, 4, 8, w), F32), V((4, 8, w), F32),
            V((3, 32, 128), F32), V((3, 32, 128), F32),
            V((3, 8, 128), F32), V((3, 8, 128), F32),
            V((3, 8, 128), F32), V((3, 8, 128), F32),
            V((4, 128, w), F32), V((4, 32, w), F32), V((4, 8, w), F32),
        ]
    result = pl.pallas_call(
        kernel,
        out_shape=jax.ShapeDtypeStruct((8, D), BF16),
        in_specs=[hbm, vm, vm, hbm, hbm, hbm, vm],
        out_specs=vm,
        scratch_shapes=[
            V((64, D), BF16), V((2, 64, 8, D), BF16), V((1024, D), BF16), V((D, D), BF16), V((D, D), BF16),
            V((1024, D), F32), V((4, 4, 4, 8, D), F32), V((2, 512, D), F32), V((4, 4, 4, 8, 128), F32),
            V((32, 64), BF16), V((32, 64), BF16), V((32, 128), BF16), V((8, 32, 128), BF16), V((128, D), BF16),
            V((128, D), BF16), V((8, D), F32), V((8, 128), F32), V((8, 128, 128), F32),
            *part,
            pltpu.SemaphoreType.DMA((SEND_SEMS,)), pltpu.SemaphoreType.DMA((SEND_SEMS,)), pltpu.SemaphoreType.DMA((8,)),
        ],
        compiler_params=pltpu.CompilerParams(
            collective_id=0, has_side_effects=True, vmem_limit_bytes=60 * 1024 * 1024
        ),
    )(
        tokens.reshape(64, 2, 8, D), var_embed, query.reshape(1, D), key_weight, value_weight, out_weight,
        var_slot.reshape(1, -1),
    )
    return result.reshape(1, 8, D)


def solution(mesh):
    placed = (
        P(("vx", "vy"), None, None, None), P(), P(), P("vy", None), P("vy", None), P("vy", None), P(),
    )
    return jax.shard_map(
        shards, mesh=mesh, in_specs=placed, out_specs=P(None, ("vx", "vy"), None), check_vma=False
    )
```

```python
import contextlib
import functools

import jax
import jax.numpy as jnp
from jax import lax
from jax.experimental import pallas as pl
from jax.experimental.pallas import tpu as pltpu
from jax.sharding import PartitionSpec as P

MESH = pl.DeviceIdType.MESH
F32, BF16 = jnp.float32, jnp.bfloat16
HEADS = 16
D = 1024
BIG = -1e30

NAT = ("x", "z", "y")
PARTS = ((0, 512, ("x", "y", "z")), (512, 512, ("y", "x", "z")))
SEND_SEMS = 200


def scope(name):
    return contextlib.nullcontext()


def device_of(x, y, z, c):
    return (x * 2 + z // 2, (z % 2) * 8 + y * 2 + c)


class Copies:
    def __init__(self, send, recv, local):
        self.send, self.recv, self.local = send, recv, local
        self.n, self.k, self.open = 0, 0, []

    def remote(self, src, dst, device):
        copy = pltpu.make_async_remote_copy(
            src_ref=src,
            dst_ref=dst,
            send_sem=self.send.at[self.n],
            recv_sem=self.recv.at[self.n],
            device_id=device,
            device_id_type=MESH,
        )
        self.n += 1
        copy.start()
        self.open.append(copy)
        return copy

    def here(self, src, dst):
        copy = pltpu.make_async_copy(src, dst, self.local.at[self.k])
        self.k += 1
        copy.start()
        return copy


def lanes_iota(rows):
    return lax.broadcasted_iota(jnp.int32, (rows, 128), 1)


def hilo(a):
    lane = lanes_iota(a.shape[0])
    high = a.astype(BF16).astype(F32)
    low = pltpu.roll(a - high, 16, axis=1)
    both = jnp.where(lane < 16, high, jnp.where(lane < 32, low, 0.0))
    return both.astype(BF16)


def fold(rows):
    lane = lanes_iota(rows.shape[0])
    rows = jnp.where(lane < 32, rows, 0.0)
    q = rows.shape[0] // 4
    out = rows[:q]
    for g in range(1, 4):
        out = out + pltpu.roll(rows[g * q : (g + 1) * q], 32 * g, axis=1)
    return out


def unfold(packed):
    pieces = [packed]
    for g in range(1, 4):
        pieces.append(pltpu.roll(packed, 128 - 32 * g, axis=1))
    return jnp.concatenate(pieces, axis=0)


def pack_stats(m, l):
    lane = lanes_iota(m.shape[0])
    return jnp.where(lane < 16, m, jnp.where(lane < 32, pltpu.roll(l, 16, axis=1), 0.0))


def merge_stats(stats):
    m = functools.reduce(jnp.maximum, stats)
    scales = [jnp.exp(s - m) for s in stats]
    l = sum(a * pltpu.roll(s, 112, axis=1) for a, s in zip(scales, stats))
    return m, l, scales


def pick(ref, axis, index, lanes, ndim):
    where = [slice(None)] * (ndim + 2)
    where[axis] = index
    where[-1] = lanes
    got = ref[tuple(where)]
    return got.reshape(-1, got.shape[-1])


def kernel(tok, emb_h, query, wk, wv, wo, vslot, out, emb, wk_v, tokv, mixed, gv, go, V, Pacc, wx, st0, qk_o, qkg, qkt,
           e2, er, used, sc, *rest):
    ssem, rsem, lsem = rest[-3:]
    per_part = [rest[i * 17 : (i + 1) * 17] for i in range(len(PARTS))]
    names = ("s1", "r1", "s2", "r2", "s3", "r3", "m1", "m2", "ts1", "tr1", "ts2", "tr2", "ts3", "tr3", "ax1", "ax2", "ax3")
    T = [dict(zip(names, p)) for p in per_part]
    cp = Copies(ssem, rsem, lsem)

    vx, vy = lax.axis_index("vx"), lax.axis_index("vy")
    x, z = vx // 2, (vx % 2) * 2 + vy // 8
    y, c = (vy // 2) % 4, vy % 2
    zl = z % 2
    zmate = z + 1 - 2 * zl
    me = {"x": x, "y": y, "z": z}

    def peer(dim, offset):
        at = dict(me)
        at[dim] = (me[dim] + offset) % 4
        return device_of(at["x"], at["y"], at["z"], c)

    other = device_of(x, y, z, 1 - c)
    group_peers = [other, device_of(x, y, zmate, c), device_of(x, y, zmate, 1 - c)]
    for o in (1, 2, 3):
        group_peers += [device_of(x, (y + o) % 4, zz, cc) for zz in (z, zmate) for cc in (c, 1 - c)]

    barrier = pltpu.get_barrier_semaphore()
    partners = group_peers + [peer("x", o) for o in (1, 2, 3)] + [device_of(x, y, (zmate + 2) % 4, c), peer("z", 2)]
    for p in partners:
        pl.semaphore_signal(barrier, inc=1, device_id=p, device_id_type=MESH)
    load_wk = cp.here(wk, wk_v.at[pl.ds(0, 64), :])
    load_emb = cp.here(emb_h, emb)
    load_tok = cp.here(tok.at[:, c], tokv.at[0])

    def row_of(yy, zz, cc):
        return pl.multiple_of(((zz * 4 + yy) * 2 + cc) * 64, 64)

    load_wv = cp.here(wv, gv.at[pl.ds(row_of(y, zl, c), 64), :])
    load_wo = cp.here(wo, go.at[pl.ds(row_of(y, zl, c), 64), :])

    head_lane = lax.broadcasted_iota(jnp.int32, (HEADS, D), 1) // 64
    head_row = lax.broadcasted_iota(jnp.int32, (HEADS, D), 0)
    own_head = head_lane == head_row
    wk_v[64:128, :] = jnp.zeros((64, D), BF16)
    q8 = query[...].astype(F32)
    q_row = jnp.concatenate([q8[k : k + 1, :] for k in range(8)], axis=1)
    q_matrix = jnp.where(own_head, q_row, 0.0).astype(BF16)
    with scope("w_wk"):
        load_wk.wait()
    nt = (((1,), (1,)), ((), ()))
    qk = lax.dot_general(q_matrix, wk_v[...], nt, preferred_element_type=F32) * 0.125
    qk_o[...] = qk[:8] + pltpu.roll(qk[8:], 64, axis=1)

    ones = own_head.astype(F32).astype(BF16)
    e2[...] = jnp.concatenate([ones, ones, jnp.zeros((96, D), BF16)], axis=0)
    position = vx * 16 + vy
    partner_pos = position + 1 - 2 * c
    n_vars = vslot.shape[1]
    row8 = lax.broadcasted_iota(jnp.int32, (8, n_vars), 0)
    slot_id = jnp.where(row8 == 0, position, jnp.where(row8 == 1, partner_pos, -1))
    match = (vslot[...] == slot_id).astype(F32)
    load_emb.wait()
    er[...] = jnp.dot(match.astype(BF16), emb[...], preferred_element_type=F32)
    used[...] = jnp.broadcast_to(jnp.sum(match, axis=1, keepdims=True), (8, 128))

    with scope("w_barrier"):
        pl.semaphore_wait(barrier, len(partners))

    mine = (zl * 4 + y) * 2 + c
    qk_copies = [cp.remote(qk_o, qkg.at[mine], p) for p in group_peers]

    class Gather:
        def __init__(self, g, local):
            self.g = g
            local.wait()
            self.y, self.z, self.core = {}, {}, {}

        def put(self, o, half, zz, device):
            rows = 64 if half is None else 32
            start = row_of((y + o) % 4, zz, c) + (half or 0) * 32
            ref = self.g.at[pl.ds(pl.multiple_of(start, 32), rows), :]
            return cp.remote(ref, ref, device)

        def to_y(self):
            self.y[3, 0] = self.put(0, 0, zl, peer("y", 1))
            self.y[1, 1] = self.put(0, 1, zl, peer("y", 3))
            self.y[3, 1] = self.put(0, 1, zl, peer("y", 1))
            self.y[1, 0] = self.put(0, 0, zl, peer("y", 3))

        def to_opposite(self, half):
            self.y[2, half] = self.put(3 if half == 0 else 1, half, zl, peer("y", 1 if half == 0 else 3))

        def to_z(self, o, half):
            self.z[o, half] = self.put(o, half, zl, peer("z", 1 if half == 0 else 3))

        def to_core(self, o, half, far):
            self.core.setdefault(o, []).append(self.put(o, half, 1 - zl if far else zl, other))

        def wait_y(self, o, half):
            self.y[o, half].wait_recv()

        def wait_z(self, o, half):
            self.z[o, half].wait_recv()

        def complete(self, o):
            for k in self.core[o]:
                k.wait_recv()

        def y_wave(self, first):
            for o, half in ((3, 0), (1, 1)) if first else ((3, 1), (1, 0)):
                self.wait_y(o, half)
                if first:
                    self.to_opposite(half)
                self.to_z(o, half)
                self.to_core(o, half, False)

        def opposite(self):
            for half in (0, 1):
                self.wait_y(2, half)
                self.to_z(2, half)
            self.to_core(2, None, False)

        def z_both(self, o):
            self.wait_z(o, 0)
            self.wait_z(o, 1)
            self.to_core(o, None, True)

        def z_wave(self, first):
            for o, half in ((3, 0), (1, 1)) if first else ((3, 1), (1, 0)):
                self.wait_z(o, half)
                self.to_core(o, half, True)

    with scope("gatherA"):
        A = Gather(gv, load_wv)
        A.to_y()
        A.to_z(0, 0)
        A.to_z(0, 1)
        tok_copy = cp.remote(tok.at[:, 1 - c], tokv.at[1], other)
        A.to_core(0, None, False)

    def mix(k):
        def step(i, carry):
            t = tokv[k, pl.ds(i * 8, 8)].astype(F32).reshape(64, D)
            mixed[pl.ds(pl.multiple_of(k * 512 + i * 64, 64), 64), :] = (t + er[k : k + 1, :]).astype(BF16)
            return carry

        lax.fori_loop(0, 8, step, 0)

    def score(k):
        rows = slice(k * 512, k * 512 + 512)
        d = lax.dot_general(mixed[rows, :], qkt[...], nt, preferred_element_type=F32)
        d = d + pltpu.roll(d, 112, axis=1)
        sc[rows, :] = jnp.where(used[k : k + 1, :] > 0, d, BIG)

    def pair_stats(i, carry):
        low, high = pl.ds(pl.multiple_of(i * 128, 128), 128), pl.ds(pl.multiple_of(512 + i * 128, 128), 128)
        s0, s1 = sc[low, :], sc[high, :]
        m = jnp.maximum(s0, s1)
        w0 = used[0:1, :] * jnp.exp(s0 - m)
        w1 = used[1:2, :] * jnp.exp(s1 - m)
        st0[i] = pack_stats(m, w0 + w1).reshape(4, 4, 8, 128)
        sc[low, :] = w0
        sc[high, :] = w1
        return carry

    def pair_expand(i, carry):
        for k in range(2):
            rows = pl.ds(pl.multiple_of(i * 128, 128), 128)
            w = sc[pl.ds(pl.multiple_of(k * 512 + i * 128, 128), 128), :]
            wx[k, rows, :] = jnp.dot(hilo(w), e2[...], preferred_element_type=F32)
        return carry

    with scope("mix0"):
        load_tok.wait()
        mix(0)
    with scope("A_y1"):
        A.y_wave(True)
    with scope("A_z0"):
        A.z_both(0)
    with scope("w_tok"):
        tok_copy.wait_recv()
    with scope("mix1"):
        mix(1)
    with scope("w_qk"):
        for k in qk_copies:
            k.wait_recv()
    with scope("qkt"):
        qkg[mine] = qk_o[...]
        left = lax.broadcasted_iota(jnp.int32, (8, 128), 1) < 64
        columns = []
        for k in range(8):
            a, b = qkg[2 * k], qkg[2 * k + 1]
            top = jnp.where(left, a, pltpu.roll(b, 64, axis=1))
            bottom = jnp.where(left, pltpu.roll(a, 64, axis=1), b)
            columns.append(jnp.concatenate([top, bottom], axis=0))
        q_keys = jnp.concatenate(columns, axis=1)
        q_high = q_keys.astype(BF16)
        q_low = (q_keys - q_high.astype(F32)).astype(BF16)
        qkt[...] = jnp.concatenate([q_high, q_low, jnp.zeros((96, D), BF16)], axis=0)
    with scope("score0"):
        score(0)
    with scope("A_y2"):
        A.y_wave(False)
    with scope("gatherB"):
        B = Gather(go, load_wo)
        B.to_y()
    with scope("score1"):
        score(1)
    with scope("pair_stats"):
        lax.fori_loop(0, 4, pair_stats, 0)

    for t, (l0, w, dims) in zip(T, PARTS):
        axis = NAT.index(dims[0])
        t["sc1"] = []
        for o in (1, 2, 3):
            rows = pick(st0, axis, (me[dims[0]] + o) % 4, slice(None), 3)
            t["ts1"][o - 1] = fold(rows)
            t["sc1"].append(cp.remote(t["ts1"].at[o - 1], t["tr1"].at[o - 1], peer(dims[0], o)))

    def expand(a, l0, w):
        return jnp.dot(hilo(a), e2[:, l0 : l0 + w], preferred_element_type=F32)

    def stats1():
        for t, (l0, w, dims) in zip(T, PARTS):
            for k in t["sc1"]:
                k.wait_recv()
            own = pick(st0, NAT.index(dims[0]), me[dims[0]], slice(None), 3)
            m, l, scales = merge_stats([own] + [unfold(t["tr1"][o]) for o in range(3)])
            for k, a in enumerate(scales):
                t["ax1"][k] = expand(a, l0, w)
            left = [d for d in NAT if d != dims[0]]
            axis = left.index(dims[1])
            t["st1"] = pack_stats(m, l).reshape(4, 4, 8, 128)
            stats = t["st1"]
            pieces = [(stats[i] if axis == 0 else stats[:, i]).reshape(32, 128) for i in range(4)]
            t["own1"] = choose(pieces, me[dims[1]])
            t["sc2"] = []
            for o in (1, 2, 3):
                t["ts2"][o - 1] = fold(choose(pieces, (me[dims[1]] + o) % 4))
                t["sc2"].append(cp.remote(t["ts2"].at[o - 1], t["tr2"].at[o - 1], peer(dims[1], o)))

    def choose(pieces, index):
        got = pieces[3]
        for i in (2, 1, 0):
            got = jnp.where(index == i, pieces[i], got)
        return got

    def stats2():
        for t, (l0, w, dims) in zip(T, PARTS):
            for k in t["sc2"]:
                k.wait_recv()
            m, l, scales = merge_stats([t["own1"]] + [unfold(t["tr2"][o]) for o in range(3)])
            for k, a in enumerate(scales):
                t["ax2"][k] = expand(a, l0, w)
            stats = pack_stats(m, l)
            pieces = [stats[8 * i : 8 * i + 8] for i in range(4)]
            t["own2"] = choose(pieces, me[dims[2]])
            t["sc3"] = []
            for o in (1, 2, 3):
                t["ts3"][o - 1] = choose(pieces, (me[dims[2]] + o) % 4)
                t["sc3"].append(cp.remote(t["ts3"].at[o - 1], t["tr3"].at[o - 1], peer(dims[2], o)))

    def stats3():
        for t, (l0, w, dims) in zip(T, PARTS):
            for k in t["sc3"]:
                k.wait_recv()
            m, l, scales = merge_stats([t["own2"]] + [t["tr3"][o] for o in range(3)])
            for k, a in enumerate(scales):
                t["ax3"][k] = expand(a / l, l0, w)

    def offsets(o):
        yy = (y + o) % 4
        return pl.multiple_of(yy * 128, 128), pl.multiple_of((4 + yy) * 128, 128)

    def left_rows(start, rows, a, b):
        at = pl.ds(pl.multiple_of(start, rows), rows)
        return jnp.concatenate([mixed[at, pl.ds(a, 128)], mixed[at, pl.ds(b, 128)]], axis=1)

    def group(o, fresh):
        a, b = offsets(o)

        def step(i, carry):
            rhs = jnp.concatenate([gv[pl.ds(a, 128), :], gv[pl.ds(b, 128), :]], axis=0)
            r = jnp.dot(left_rows(i * 256, 256, a, b), rhs, preferred_element_type=F32)
            at = pl.ds(pl.multiple_of(i * 256, 256), 256)
            V[at, :] = r if fresh else V[at, :] + r
            return carry

        lax.fori_loop(0, 4, step, 0)

    def last_rows(o, l0, w, i):
        a, b = offsets(o)
        cols = slice(l0, l0 + w)
        rhs = jnp.concatenate([gv[pl.ds(a, 128), cols], gv[pl.ds(b, 128), cols]], axis=0)
        total = None
        for k in range(2):
            r = jnp.dot(left_rows(k * 512 + i * 128, 128, a, b), rhs, preferred_element_type=F32)
            at = pl.ds(pl.multiple_of(k * 512 + i * 128, 128), 128)
            part = (V[at, cols] + r) * wx[k, pl.ds(pl.multiple_of(i * 128, 128), 128), cols]
            total = part if total is None else total + part
        return total

    def last_group(o, l0, w):
        def step(i, carry):
            Pacc[i, :, :, :, l0 : l0 + w] = last_rows(o, l0, w, i).reshape(4, 4, 8, w)
            return carry

        lax.fori_loop(0, 4, step, 0)

    with scope("pair_expand"):
        lax.fori_loop(0, 4, pair_expand, 0)
    with scope("A_opp"):
        A.opposite()
    with scope("A_z1"):
        A.z_wave(True)
    with scope("A_c0"):
        A.complete(0)
    with scope("g0"):
        group(0, True)
    with scope("A_z2"):
        A.z_wave(False)
        B.to_z(0, 0)
        B.to_z(0, 1)
        B.to_core(0, None, False)
    with scope("stats1"):
        stats1()
    with scope("A_c3"):
        A.complete(3)
    with scope("g3"):
        group(3, False)
    with scope("A_zo"):
        A.z_both(2)
    with scope("B_y"):
        B.y_wave(True)
        B.y_wave(False)
    with scope("A_c1"):
        A.complete(1)
    with scope("g1"):
        group(1, False)
    with scope("B_o"):
        B.opposite()
    with scope("A_c2"):
        A.complete(2)

    t, (l0, w, dims) = T[1], PARTS[1]
    with scope("last1"):
        last_group(2, l0, w)
        t["c1"] = []
        for o in (2, 1, 3):
            t["s1"][o - 1] = pick(Pacc, NAT.index(dims[0]), (me[dims[0]] + o) % 4, slice(l0, l0 + w), 3).astype(BF16)
            t["c1"].append(cp.remote(t["s1"].at[o - 1], t["r1"].at[o - 1], peer(dims[0], o)))
    t, (l0, w, dims) = T[0], PARTS[0]
    with scope("last0"):
        t["c1"] = []
        for o in (2, 1, 3):
            t["s1"][o - 1] = last_rows(2, l0, w, (x + o) % 4).astype(BF16)
            t["c1"].append(cp.remote(t["s1"].at[o - 1], t["r1"].at[o - 1], peer("x", o)))
        Pacc[x, :, :, :, l0 : l0 + w] = last_rows(2, l0, w, x).reshape(4, 4, 8, w)
    with scope("stats2"):
        stats2()
    with scope("B_z"):
        B.z_both(0)
        B.z_wave(True)
        B.z_wave(False)
        B.z_both(2)

    for t, (l0, w, dims) in list(zip(T, PARTS))[::-1]:
        own = pick(Pacc, NAT.index(dims[0]), me[dims[0]], slice(l0, l0 + w), 3)
        total = t["ax1"][0] * own
        with scope("w_c1"):
            for k in t["c1"]:
                k.wait_recv()
        for o in range(3):
            total = total + t["ax1"][o + 1] * t["r1"][o].astype(F32)
        t["m1"][...] = total.reshape(4, 4, 8, w)
        left = [d for d in NAT if d != dims[0]]
        axis = left.index(dims[1])
        t["c2"] = []
        for o in (2, 1, 3):
            t["s2"][o - 1] = pick(t["m1"], axis, (me[dims[1]] + o) % 4, slice(None), 2).astype(BF16)
            t["c2"].append(cp.remote(t["s2"].at[o - 1], t["r2"].at[o - 1], peer(dims[1], o)))

    for t, (l0, w, dims) in list(zip(T, PARTS))[::-1]:
        left = [d for d in NAT if d != dims[0]]
        own = pick(t["m1"], left.index(dims[1]), me[dims[1]], slice(None), 2)
        total = t["ax2"][0] * own
        with scope("w_c2"):
            for k in t["c2"]:
                k.wait_recv()
        for o in range(3):
            total = total + t["ax2"][o + 1] * t["r2"][o].astype(F32)
        t["m2"][...] = total.reshape(4, 8, w)
        t["c3"] = []
        for o in (2, 1, 3):
            t["s3"][o - 1] = t["m2"][(me[dims[2]] + o) % 4]
            t["c3"].append(cp.remote(t["s3"].at[o - 1], t["r3"].at[o - 1], peer(dims[2], o)))

    with scope("stats3"):
        stats3()
    context = []
    for t, (l0, w, dims) in sorted(zip(T, PARTS), key=lambda tp: tp[1][0]):
        total = t["ax3"][0] * t["m2"][me[dims[2]]]
        with scope("w_c3"):
            for k in t["c3"]:
                k.wait_recv()
        for o in range(3):
            total = total + t["ax3"][o + 1] * t["r3"][o]
        context.append(total)
    with scope("B_c"):
        for o in (0, 3, 1, 2):
            B.complete(o)
    with scope("tail"):
        context = jnp.concatenate(context, axis=1).astype(BF16)
        out[...] = jnp.dot(context, go[...], preferred_element_type=F32).astype(BF16)
    with scope("w_sends"):
        for k in cp.open:
            k.wait_send()


def shards(tokens, var_embed, query, key_weight, value_weight, out_weight, var_slot):
    vm = pl.BlockSpec(memory_space=pltpu.VMEM)
    hbm = pl.BlockSpec(memory_space=pl.ANY)
    V = pltpu.VMEM
    part = []
    for _, w, _ in PARTS:
        part += [
            V((3, 128, w), BF16), V((3, 128, w), BF16),
            V((3, 32, w), BF16), V((3, 32, w), BF16),
            V((3, 8, w), F32), V((3, 8, w), F32),
            V((4, 4, 8, w), F32), V((4, 8, w), F32),
            V((3, 32, 128), F32), V((3, 32, 128), F32),
            V((3, 8, 128), F32), V((3, 8, 128), F32),
            V((3, 8, 128), F32), V((3, 8, 128), F32),
            V((4, 128, w), F32), V((4, 32, w), F32), V((4, 8, w), F32),
        ]
    result = pl.pallas_call(
        kernel,
        out_shape=jax.ShapeDtypeStruct((8, D), BF16),
        in_specs=[hbm, hbm, vm, hbm, hbm, hbm, vm],
        out_specs=vm,
        scratch_shapes=[
            V((91, D), BF16), V((128, D), BF16), V((2, 64, 8, D), BF16), V((1024, D), BF16), V((D, D), BF16), V((D, D), BF16),
            V((1024, D), F32), V((4, 4, 4, 8, D), F32), V((2, 512, D), F32), V((4, 4, 4, 8, 128), F32),
            V((8, 128), F32), V((16, 8, 128), F32), V((128, D), BF16),
            V((128, D), BF16), V((8, D), F32), V((8, 128), F32), V((1024, 128), F32),
            *part,
            pltpu.SemaphoreType.DMA((SEND_SEMS,)), pltpu.SemaphoreType.DMA((SEND_SEMS,)), pltpu.SemaphoreType.DMA((8,)),
        ],
        compiler_params=pltpu.CompilerParams(
            collective_id=0, has_side_effects=True, vmem_limit_bytes=60 * 1024 * 1024
        ),
    )(
        tokens.reshape(64, 2, 8, D), var_embed, query.reshape(8, 128), key_weight, value_weight, out_weight,
        var_slot.reshape(1, -1),
    )
    return result.reshape(1, 8, D)


def solution(mesh):
    placed = (
        P(("vx", "vy"), None, None, None), P(), P(), P("vy", None), P("vy", None), P("vy", None), P(),
    )
    return jax.shard_map(
        shards, mesh=mesh, in_specs=placed, out_specs=P(None, ("vx", "vy"), None), check_vma=False
    )
```

```python
import contextlib
import functools

import jax
import jax.numpy as jnp
from jax import lax
from jax.experimental import pallas as pl
from jax.experimental.pallas import tpu as pltpu
from jax.sharding import PartitionSpec as P

MESH = pl.DeviceIdType.MESH
F32, BF16 = jnp.float32, jnp.bfloat16
HEADS = 16
D = 1024
BIG = -1e30

NAT = ("x", "z", "y")
PARTS = ((640, 384, ("y", "z", "x")), (0, 384, ("x", "y", "z")), (384, 256, ("z", "x", "y")))
SEND_SEMS = 160


def scope(name):
    return contextlib.nullcontext()


def device_of(x, y, z, c):
    return (x * 2 + z // 2, (z % 2) * 8 + y * 2 + c)


class Copies:
    def __init__(self, send, recv, local):
        self.send, self.recv, self.local = send, recv, local
        self.n, self.k, self.open = 0, 0, []

    def remote(self, src, dst, device):
        copy = pltpu.make_async_remote_copy(
            src_ref=src,
            dst_ref=dst,
            send_sem=self.send.at[self.n],
            recv_sem=self.recv.at[self.n],
            device_id=device,
            device_id_type=MESH,
        )
        self.n += 1
        copy.start()
        self.open.append(copy)
        return copy

    def here(self, src, dst):
        copy = pltpu.make_async_copy(src, dst, self.local.at[self.k])
        self.k += 1
        copy.start()
        return copy


def lanes_iota(rows):
    return lax.broadcasted_iota(jnp.int32, (rows, 128), 1)


def expand(a, l0, w):
    half = lanes_iota(a.shape[0]) // 64
    tiles = [jnp.take_along_axis(a, half + 2 * t, axis=1, mode="promise_in_bounds") for t in range(l0 // 128, (l0 + w) // 128)]
    return jnp.concatenate(tiles, axis=1)


def fold(rows):
    lane = lanes_iota(rows.shape[0])
    rows = jnp.where(lane < 32, rows, 0.0)
    q = rows.shape[0] // 4
    out = rows[:q]
    for g in range(1, 4):
        out = out + pltpu.roll(rows[g * q : (g + 1) * q], 32 * g, axis=1)
    return out


def unfold(packed):
    pieces = [packed]
    for g in range(1, 4):
        pieces.append(pltpu.roll(packed, 128 - 32 * g, axis=1))
    return jnp.concatenate(pieces, axis=0)


def pack_stats(m, l):
    lane = lanes_iota(m.shape[0])
    return jnp.where(lane < 16, m, jnp.where(lane < 32, pltpu.roll(l, 16, axis=1), 0.0))


def merge_stats(stats):
    m = functools.reduce(jnp.maximum, stats)
    scales = [jnp.exp(s - m) for s in stats]
    l = sum(a * pltpu.roll(s, 112, axis=1) for a, s in zip(scales, stats))
    return m, l, scales


def pick(ref, axis, index, lanes, ndim):
    where = [slice(None)] * (ndim + 2)
    where[axis] = index
    where[-1] = lanes
    got = ref[tuple(where)]
    return got.reshape(-1, got.shape[-1])


def kernel(tok, emb_h, query, wk, wv, wo, vslot, out, emb, wk_v, tokv, mixed, gv, go, V, Pacc, st0, qk_o, qkg, qkt,
           er, used, sc, *rest):
    ssem, rsem, lsem = rest[-3:]
    per_part = [rest[i * 17 : (i + 1) * 17] for i in range(len(PARTS))]
    names = ("s1", "r1", "s2", "r2", "s3", "r3", "m1", "m2", "ts1", "tr1", "ts2", "tr2", "ts3", "tr3", "ax1", "ax2", "ax3")
    T = [dict(zip(names, p)) for p in per_part]
    cp = Copies(ssem, rsem, lsem)

    vx, vy = lax.axis_index("vx"), lax.axis_index("vy")
    x, z = vx // 2, (vx % 2) * 2 + vy // 8
    y, c = (vy // 2) % 4, vy % 2
    zl = z % 2
    zmate = z + 1 - 2 * zl
    me = {"x": x, "y": y, "z": z}

    def peer(dim, offset):
        at = dict(me)
        at[dim] = (me[dim] + offset) % 4
        return device_of(at["x"], at["y"], at["z"], c)

    other = device_of(x, y, z, 1 - c)
    group_peers = [other, device_of(x, y, zmate, c), device_of(x, y, zmate, 1 - c)]
    for o in (1, 2, 3):
        group_peers += [device_of(x, (y + o) % 4, zz, cc) for zz in (z, zmate) for cc in (c, 1 - c)]

    barrier = pltpu.get_barrier_semaphore()
    partners = group_peers + [peer("x", o) for o in (1, 2, 3)] + [device_of(x, y, (zmate + 2) % 4, c), peer("z", 2)]
    for p in partners:
        pl.semaphore_signal(barrier, inc=1, device_id=p, device_id_type=MESH)
    load_wk = cp.here(wk, wk_v.at[pl.ds(0, 64), :])
    load_emb = cp.here(emb_h, emb)
    load_tok = cp.here(tok.at[:, c], tokv.at[0])

    def row_of(yy, zz, cc):
        return pl.multiple_of(((zz * 4 + yy) * 2 + cc) * 64, 64)

    load_wv = cp.here(wv, gv.at[pl.ds(row_of(y, zl, c), 64), :])
    load_wo = cp.here(wo, go.at[pl.ds(row_of(y, zl, c), 64), :])

    head_lane = lax.broadcasted_iota(jnp.int32, (HEADS, D), 1) // 64
    head_row = lax.broadcasted_iota(jnp.int32, (HEADS, D), 0)
    own_head = head_lane == head_row
    wk_v[64:128, :] = jnp.zeros((64, D), BF16)
    q8 = query[...].astype(F32)
    q_row = jnp.concatenate([q8[k : k + 1, :] for k in range(8)], axis=1)
    q_matrix = jnp.where(own_head, q_row, 0.0).astype(BF16)
    with scope("w_wk"):
        load_wk.wait()
    nt = (((1,), (1,)), ((), ()))
    qk = lax.dot_general(q_matrix, wk_v[...], nt, preferred_element_type=F32) * 0.125
    qk_o[...] = qk[:8] + pltpu.roll(qk[8:], 64, axis=1)

    position = vx * 16 + vy
    partner_pos = position + 1 - 2 * c
    n_vars = vslot.shape[1]
    row8 = lax.broadcasted_iota(jnp.int32, (8, n_vars), 0)
    slot_id = jnp.where(row8 == 0, position, jnp.where(row8 == 1, partner_pos, -1))
    match = (vslot[...] == slot_id).astype(F32)
    load_emb.wait()
    er[...] = jnp.dot(match.astype(BF16), emb[...], preferred_element_type=F32)
    used[...] = jnp.broadcast_to(jnp.sum(match, axis=1, keepdims=True), (8, 128))

    with scope("w_barrier"):
        pl.semaphore_wait(barrier, len(partners))

    mine = (zl * 4 + y) * 2 + c
    qk_copies = [cp.remote(qk_o, qkg.at[mine], p) for p in group_peers]

    class Gather:
        def __init__(self, g, local):
            self.g = g
            local.wait()
            self.y, self.z, self.core = {}, {}, {}

        def put(self, o, half, zz, device):
            rows = 64 if half is None else 32
            start = row_of((y + o) % 4, zz, c) + (half or 0) * 32
            ref = self.g.at[pl.ds(pl.multiple_of(start, 32), rows), :]
            return cp.remote(ref, ref, device)

        def to_y(self):
            self.y[3, 0] = self.put(0, 0, zl, peer("y", 1))
            self.y[1, 1] = self.put(0, 1, zl, peer("y", 3))
            self.y[3, 1] = self.put(0, 1, zl, peer("y", 1))
            self.y[1, 0] = self.put(0, 0, zl, peer("y", 3))

        def to_opposite(self, half):
            self.y[2, half] = self.put(3 if half == 0 else 1, half, zl, peer("y", 1 if half == 0 else 3))

        def to_z(self, o, half):
            self.z[o, half] = self.put(o, half, zl, peer("z", 1 if half == 0 else 3))

        def to_core(self, o, half, far):
            self.core.setdefault(o, []).append(self.put(o, half, 1 - zl if far else zl, other))

        def wait_y(self, o, half):
            self.y[o, half].wait_recv()

        def wait_z(self, o, half):
            self.z[o, half].wait_recv()

        def complete(self, o):
            for k in self.core[o]:
                k.wait_recv()

        def y_wave(self, first):
            for o, half in ((3, 0), (1, 1)) if first else ((3, 1), (1, 0)):
                self.wait_y(o, half)
                if first:
                    self.to_opposite(half)
                self.to_z(o, half)
                self.to_core(o, half, False)

        def opposite(self):
            for half in (0, 1):
                self.wait_y(2, half)
                self.to_z(2, half)
            self.to_core(2, None, False)

        def z_both(self, o):
            self.wait_z(o, 0)
            self.wait_z(o, 1)
            self.to_core(o, None, True)

        def z_wave(self, first):
            for o, half in ((3, 0), (1, 1)) if first else ((3, 1), (1, 0)):
                self.wait_z(o, half)
                self.to_core(o, half, True)

    with scope("gatherA"):
        A = Gather(gv, load_wv)
        A.to_y()
        A.to_z(0, 0)
        A.to_z(0, 1)
        tok_copy = cp.remote(tok.at[:, 1 - c], tokv.at[1], other)
        A.to_core(0, None, False)

    def mix(k):
        def step(i, carry):
            t = tokv[k, pl.ds(i * 8, 8)].astype(F32).reshape(64, D)
            mixed[pl.ds(pl.multiple_of(k * 512 + i * 64, 64), 64), :] = (t + er[k : k + 1, :]).astype(BF16)
            return carry

        lax.fori_loop(0, 8, step, 0)

    def score(k):
        rows = slice(k * 512, k * 512 + 512)
        d = lax.dot_general(mixed[rows, :], qkt[...], nt, preferred_element_type=F32)
        d = d + pltpu.roll(d, 112, axis=1)
        sc[rows, :] = jnp.where(used[k : k + 1, :] > 0, d, BIG)

    def pair_stats(i, carry):
        low, high = pl.ds(pl.multiple_of(i * 128, 128), 128), pl.ds(pl.multiple_of(512 + i * 128, 128), 128)
        s0, s1 = sc[low, :], sc[high, :]
        m = jnp.maximum(s0, s1)
        w0 = used[0:1, :] * jnp.exp(s0 - m)
        w1 = used[1:2, :] * jnp.exp(s1 - m)
        st0[i] = pack_stats(m, w0 + w1).reshape(4, 4, 8, 128)
        sc[low, :] = w0
        sc[high, :] = w1
        return carry

    with scope("mix0"):
        load_tok.wait()
        mix(0)
    with scope("A_y1"):
        A.y_wave(True)
    with scope("A_z0"):
        A.z_both(0)
    with scope("w_tok"):
        tok_copy.wait_recv()
    with scope("mix1"):
        mix(1)
    with scope("w_qk"):
        for k in qk_copies:
            k.wait_recv()
    with scope("qkt"):
        qkg[mine] = qk_o[...]
        left = lax.broadcasted_iota(jnp.int32, (8, 128), 1) < 64
        columns = []
        for k in range(8):
            a, b = qkg[2 * k], qkg[2 * k + 1]
            top = jnp.where(left, a, pltpu.roll(b, 64, axis=1))
            bottom = jnp.where(left, pltpu.roll(a, 64, axis=1), b)
            columns.append(jnp.concatenate([top, bottom], axis=0))
        q_keys = jnp.concatenate(columns, axis=1)
        q_high = q_keys.astype(BF16)
        q_low = (q_keys - q_high.astype(F32)).astype(BF16)
        qkt[...] = jnp.concatenate([q_high, q_low, jnp.zeros((96, D), BF16)], axis=0)
    with scope("A_y2"):
        A.y_wave(False)
        B = Gather(go, load_wo)
        B.to_y()
    with scope("score0"):
        score(0)
    with scope("score1"):
        score(1)
    with scope("A_opp"):
        A.opposite()
    with scope("pair_stats"):
        lax.fori_loop(0, 4, pair_stats, 0)

    for t, (l0, w, dims) in zip(T, PARTS):
        axis = NAT.index(dims[0])
        t["sc1"] = []
        for o in (1, 2, 3):
            rows = pick(st0, axis, (me[dims[0]] + o) % 4, slice(None), 3)
            t["ts1"][o - 1] = fold(rows)
            t["sc1"].append(cp.remote(t["ts1"].at[o - 1], t["tr1"].at[o - 1], peer(dims[0], o)))

    def stats1():
        for t, (l0, w, dims) in zip(T, PARTS):
            for k in t["sc1"]:
                k.wait_recv()
            own = pick(st0, NAT.index(dims[0]), me[dims[0]], slice(None), 3)
            m, l, scales = merge_stats([own] + [unfold(t["tr1"][o]) for o in range(3)])
            for k, a in enumerate(scales):
                t["ax1"][k] = expand(a, l0, w)
            left = [d for d in NAT if d != dims[0]]
            axis = left.index(dims[1])
            t["st1"] = pack_stats(m, l).reshape(4, 4, 8, 128)
            stats = t["st1"]
            pieces = [(stats[i] if axis == 0 else stats[:, i]).reshape(32, 128) for i in range(4)]
            t["own1"] = choose(pieces, me[dims[1]])
            t["sc2"] = []
            for o in (1, 2, 3):
                t["ts2"][o - 1] = fold(choose(pieces, (me[dims[1]] + o) % 4))
                t["sc2"].append(cp.remote(t["ts2"].at[o - 1], t["tr2"].at[o - 1], peer(dims[1], o)))

    def choose(pieces, index):
        got = pieces[3]
        for i in (2, 1, 0):
            got = jnp.where(index == i, pieces[i], got)
        return got

    def stats2():
        for t, (l0, w, dims) in zip(T, PARTS):
            for k in t["sc2"]:
                k.wait_recv()
            m, l, scales = merge_stats([t["own1"]] + [unfold(t["tr2"][o]) for o in range(3)])
            for k, a in enumerate(scales):
                t["ax2"][k] = expand(a, l0, w)
            stats = pack_stats(m, l)
            pieces = [stats[8 * i : 8 * i + 8] for i in range(4)]
            t["own2"] = choose(pieces, me[dims[2]])
            t["sc3"] = []
            for o in (1, 2, 3):
                t["ts3"][o - 1] = choose(pieces, (me[dims[2]] + o) % 4)
                t["sc3"].append(cp.remote(t["ts3"].at[o - 1], t["tr3"].at[o - 1], peer(dims[2], o)))

    def stats3():
        for t, (l0, w, dims) in zip(T, PARTS):
            for k in t["sc3"]:
                k.wait_recv()
            m, l, scales = merge_stats([t["own2"]] + [t["tr3"][o] for o in range(3)])
            for k, a in enumerate(scales):
                t["ax3"][k] = expand(a / l, l0, w)

    def offsets(o):
        yy = (y + o) % 4
        return pl.multiple_of(yy * 128, 128), pl.multiple_of((4 + yy) * 128, 128)

    def left_rows(start, rows, a, b):
        at = pl.ds(pl.multiple_of(start, rows), rows)
        return jnp.concatenate([mixed[at, pl.ds(a, 128)], mixed[at, pl.ds(b, 128)]], axis=1)

    def group(o, fresh):
        a, b = offsets(o)

        def step(i, carry):
            rhs = jnp.concatenate([gv[pl.ds(a, 128), :], gv[pl.ds(b, 128), :]], axis=0)
            r = jnp.dot(left_rows(i * 256, 256, a, b), rhs, preferred_element_type=F32)
            at = pl.ds(pl.multiple_of(i * 256, 256), 256)
            V[at, :] = r if fresh else V[at, :] + r
            return carry

        lax.fori_loop(0, 4, step, 0)

    def last_rows(o, l0, w, i):
        a, b = offsets(o)
        cols = slice(l0, l0 + w)
        rhs = jnp.concatenate([gv[pl.ds(a, 128), cols], gv[pl.ds(b, 128), cols]], axis=0)
        total = None
        for k in range(2):
            r = jnp.dot(left_rows(k * 512 + i * 128, 128, a, b), rhs, preferred_element_type=F32)
            at = pl.ds(pl.multiple_of(k * 512 + i * 128, 128), 128)
            part = (V[at, cols] + r) * expand(sc[at, :], l0, w)
            total = part if total is None else total + part
        return total

    def last_group(o, l0, w):
        def step(i, carry):
            Pacc[i, :, :, :, l0 : l0 + w] = last_rows(o, l0, w, i).reshape(4, 4, 8, w)
            return carry

        lax.fori_loop(0, 4, step, 0)

    with scope("A_z1"):
        A.z_wave(True)
    with scope("A_z2"):
        A.z_wave(False)
        B.to_z(0, 0)
        B.to_z(0, 1)
        B.to_core(0, None, False)
    with scope("A_c0"):
        A.complete(0)
    with scope("g0"):
        group(0, True)
    with scope("B_y"):
        B.y_wave(True)
        B.y_wave(False)
    with scope("A_c3"):
        A.complete(3)
    with scope("g3"):
        group(3, False)
    with scope("A_zo"):
        A.z_both(2)
    with scope("A_c1"):
        A.complete(1)
    with scope("g1"):
        group(1, False)
    with scope("A_c2"):
        A.complete(2)

    def send1(t, l0, w, dims, o):
        index = (me[dims[0]] + o) % 4
        t["s1"][o - 1] = pick(Pacc, NAT.index(dims[0]), index, slice(l0, l0 + w), 3).astype(BF16)
        t["c1"].append(cp.remote(t["s1"].at[o - 1], t["r1"].at[o - 1], peer(dims[0], o)))

    for t in T:
        t["c1"] = []
    with scope("last1"):
        last_group(2, 512, 512)
        for o in (2, 1, 3):
            send1(T[0], *PARTS[0], o)
    with scope("B_o"):
        B.opposite()
    with scope("last0"):
        for o in (2, 1, 3):
            index = (x + o) % 4
            Pacc[index, :, :, :, 0:512] = last_rows(2, 0, 512, index).reshape(4, 4, 8, 512)
            send1(T[1], *PARTS[1], o)
        Pacc[x, :, :, :, 0:512] = last_rows(2, 0, 512, x).reshape(4, 4, 8, 512)
        for o in (2, 1, 3):
            send1(T[2], *PARTS[2], o)
    with scope("stats1"):
        stats1()
    with scope("B_z"):
        B.z_both(0)
        B.z_wave(True)
        B.z_wave(False)
        B.z_both(2)

    for t, (l0, w, dims) in zip(T, PARTS):
        own = pick(Pacc, NAT.index(dims[0]), me[dims[0]], slice(l0, l0 + w), 3)
        total = t["ax1"][0] * own
        with scope("w_c1"):
            for k in t["c1"]:
                k.wait_recv()
        for o in range(3):
            total = total + t["ax1"][o + 1] * t["r1"][o].astype(F32)
        t["m1"][...] = total.reshape(4, 4, 8, w)
        left = [d for d in NAT if d != dims[0]]
        axis = left.index(dims[1])
        t["c2"] = []
        for o in (2, 1, 3):
            t["s2"][o - 1] = pick(t["m1"], axis, (me[dims[1]] + o) % 4, slice(None), 2).astype(BF16)
            t["c2"].append(cp.remote(t["s2"].at[o - 1], t["r2"].at[o - 1], peer(dims[1], o)))

    with scope("stats2"):
        stats2()

    for t, (l0, w, dims) in zip(T, PARTS):
        left = [d for d in NAT if d != dims[0]]
        own = pick(t["m1"], left.index(dims[1]), me[dims[1]], slice(None), 2)
        total = t["ax2"][0] * own
        with scope("w_c2"):
            for k in t["c2"]:
                k.wait_recv()
        for o in range(3):
            total = total + t["ax2"][o + 1] * t["r2"][o].astype(F32)
        t["m2"][...] = total.reshape(4, 8, w)
        t["c3"] = []
        for o in (2, 1, 3):
            t["s3"][o - 1] = t["m2"][(me[dims[2]] + o) % 4]
            t["c3"].append(cp.remote(t["s3"].at[o - 1], t["r3"].at[o - 1], peer(dims[2], o)))

    with scope("stats3"):
        stats3()
    context = []
    for t, (l0, w, dims) in sorted(zip(T, PARTS), key=lambda tp: tp[1][0]):
        total = t["ax3"][0] * t["m2"][me[dims[2]]]
        with scope("w_c3"):
            for k in t["c3"]:
                k.wait_recv()
        for o in range(3):
            total = total + t["ax3"][o + 1] * t["r3"][o]
        context.append(total)
    with scope("B_c"):
        for o in (0, 3, 1, 2):
            B.complete(o)
    with scope("tail"):
        context = jnp.concatenate(context, axis=1).astype(BF16)
        out[...] = jnp.dot(context, go[...], preferred_element_type=F32).astype(BF16)
    with scope("w_sends"):
        for k in cp.open:
            k.wait_send()


def shards(tokens, var_embed, query, key_weight, value_weight, out_weight, var_slot):
    vm = pl.BlockSpec(memory_space=pltpu.VMEM)
    hbm = pl.BlockSpec(memory_space=pl.ANY)
    V = pltpu.VMEM
    part = []
    for _, w, _ in PARTS:
        part += [
            V((3, 128, w), BF16), V((3, 128, w), BF16),
            V((3, 32, w), BF16), V((3, 32, w), BF16),
            V((3, 8, w), F32), V((3, 8, w), F32),
            V((4, 4, 8, w), F32), V((4, 8, w), F32),
            V((3, 32, 128), F32), V((3, 32, 128), F32),
            V((3, 8, 128), F32), V((3, 8, 128), F32),
            V((3, 8, 128), F32), V((3, 8, 128), F32),
            V((4, 128, w), F32), V((4, 32, w), F32), V((4, 8, w), F32),
        ]
    result = pl.pallas_call(
        kernel,
        out_shape=jax.ShapeDtypeStruct((8, D), BF16),
        in_specs=[hbm, hbm, vm, hbm, hbm, hbm, vm],
        out_specs=vm,
        scratch_shapes=[
            V((91, D), BF16), V((128, D), BF16), V((2, 64, 8, D), BF16), V((1024, D), BF16), V((D, D), BF16), V((D, D), BF16),
            V((1024, D), F32), V((4, 4, 4, 8, D), F32), V((4, 4, 4, 8, 128), F32),
            V((8, 128), F32), V((16, 8, 128), F32), V((128, D), BF16), V((8, D), F32), V((8, 128), F32), V((1024, 128), F32),
            *part,
            pltpu.SemaphoreType.DMA((SEND_SEMS,)), pltpu.SemaphoreType.DMA((SEND_SEMS,)), pltpu.SemaphoreType.DMA((8,)),
        ],
        compiler_params=pltpu.CompilerParams(
            collective_id=0, has_side_effects=True, vmem_limit_bytes=60 * 1024 * 1024
        ),
    )(
        tokens.reshape(64, 2, 8, D), var_embed, query.reshape(8, 128), key_weight, value_weight, out_weight,
        var_slot.reshape(1, -1),
    )
    return result.reshape(1, 8, D)


def solution(mesh):
    placed = (
        P(("vx", "vy"), None, None, None), P(), P(), P("vy", None), P("vy", None), P("vy", None), P(),
    )
    return jax.shard_map(
        shards, mesh=mesh, in_specs=placed, out_specs=P(None, ("vx", "vy"), None), check_vma=False
    )
```

```python
import contextlib
import functools

import jax
import jax.numpy as jnp
from jax import lax
from jax.experimental import pallas as pl
from jax.experimental.pallas import tpu as pltpu
from jax.sharding import PartitionSpec as P

MESH = pl.DeviceIdType.MESH
F32, BF16 = jnp.float32, jnp.bfloat16
HEADS = 16
D = 1024
BIG = -1e30

NAT = ("x", "z", "y")
PARTS = ((0, 512, ("x", "y", "z")), (512, 256, ("y", "z", "x")), (768, 256, ("z", "x", "y")))
BLOCK = 256
SEND_SEMS = 200


def scope(name):
    return contextlib.nullcontext()


def device_of(x, y, z, c):
    return (x * 2 + z // 2, (z % 2) * 8 + y * 2 + c)


class Copies:
    def __init__(self, send, recv, local):
        self.send, self.recv, self.local = send, recv, local
        self.n, self.k, self.open = 0, 0, []

    def remote(self, src, dst, device):
        copy = pltpu.make_async_remote_copy(
            src_ref=src,
            dst_ref=dst,
            send_sem=self.send.at[self.n],
            recv_sem=self.recv.at[self.n],
            device_id=device,
            device_id_type=MESH,
        )
        self.n += 1
        copy.start()
        self.open.append(copy)
        return copy

    def here(self, src, dst):
        copy = pltpu.make_async_copy(src, dst, self.local.at[self.k])
        self.k += 1
        copy.start()
        return copy


def lanes_iota(rows):
    return lax.broadcasted_iota(jnp.int32, (rows, 128), 1)


def expand(a, l0, w):
    half = lanes_iota(a.shape[0]) // 64
    tiles = [jnp.take_along_axis(a, half + 2 * t, axis=1, mode="promise_in_bounds") for t in range(l0 // 128, (l0 + w) // 128)]
    return jnp.concatenate(tiles, axis=1)


def fold(rows):
    lane = lanes_iota(rows.shape[0])
    rows = jnp.where(lane < 32, rows, 0.0)
    q = rows.shape[0] // 4
    out = rows[:q]
    for g in range(1, 4):
        out = out + pltpu.roll(rows[g * q : (g + 1) * q], 32 * g, axis=1)
    return out


def unfold(packed):
    pieces = [packed]
    for g in range(1, 4):
        pieces.append(pltpu.roll(packed, 128 - 32 * g, axis=1))
    return jnp.concatenate(pieces, axis=0)


def pack_stats(m, l):
    lane = lanes_iota(m.shape[0])
    return jnp.where(lane < 16, m, jnp.where(lane < 32, pltpu.roll(l, 16, axis=1), 0.0))


def merge_stats(stats):
    m = functools.reduce(jnp.maximum, stats)
    scales = [jnp.exp(s - m) for s in stats]
    l = sum(a * pltpu.roll(s, 112, axis=1) for a, s in zip(scales, stats))
    return m, l, scales


def pick(ref, axis, index, lanes, ndim):
    where = [slice(None)] * (ndim + 2)
    where[axis] = index
    where[-1] = lanes
    got = ref[tuple(where)]
    return got.reshape(-1, got.shape[-1])


def kernel(tok, emb_h, query, wk, wv, wo, vslot, out, emb, wk_v, tokv, mixed, gv, go, V, Pacc, st0, qk_o, qkg, qkt,
           er, used, sc, *rest):
    ssem, rsem, lsem = rest[-3:]
    per_part = [rest[i * 17 : (i + 1) * 17] for i in range(len(PARTS))]
    names = ("s1", "r1", "s2", "r2", "s3", "r3", "m1", "m2", "ts1", "tr1", "ts2", "tr2", "ts3", "tr3", "ax1", "ax2", "ax3")
    T = [dict(zip(names, p)) for p in per_part]
    cp = Copies(ssem, rsem, lsem)

    vx, vy = lax.axis_index("vx"), lax.axis_index("vy")
    x, z = vx // 2, (vx % 2) * 2 + vy // 8
    y, c = (vy // 2) % 4, vy % 2
    zl = z % 2
    zmate = z + 1 - 2 * zl
    me = {"x": x, "y": y, "z": z}

    def peer(dim, offset):
        at = dict(me)
        at[dim] = (me[dim] + offset) % 4
        return device_of(at["x"], at["y"], at["z"], c)

    other = device_of(x, y, z, 1 - c)
    group_peers = [other, device_of(x, y, zmate, c), device_of(x, y, zmate, 1 - c)]
    for o in (1, 2, 3):
        group_peers += [device_of(x, (y + o) % 4, zz, cc) for zz in (z, zmate) for cc in (c, 1 - c)]

    barrier = pltpu.get_barrier_semaphore()
    partners = group_peers + [peer("x", o) for o in (1, 2, 3)] + [device_of(x, y, (zmate + 2) % 4, c), peer("z", 2)]
    for p in partners:
        pl.semaphore_signal(barrier, inc=1, device_id=p, device_id_type=MESH)
    load_wk = cp.here(wk, wk_v.at[pl.ds(0, 64), :])
    load_emb = cp.here(emb_h, emb)
    load_tok = cp.here(tok.at[:, c], tokv.at[0])

    def row_of(yy, zz, cc):
        return pl.multiple_of(((zz * 4 + yy) * 2 + cc) * 64, 64)

    own_rows = pl.ds(row_of(y, zl, c), 64)
    load_wv = [cp.here(wv.at[:, BLOCK * b : BLOCK * b + BLOCK], gv.at[b, own_rows, :]) for b in range(4)]
    load_wo = cp.here(wo, go.at[own_rows, :])

    head_lane = lax.broadcasted_iota(jnp.int32, (HEADS, D), 1) // 64
    head_row = lax.broadcasted_iota(jnp.int32, (HEADS, D), 0)
    own_head = head_lane == head_row
    wk_v[64:128, :] = jnp.zeros((64, D), BF16)
    q8 = query[...].astype(F32)
    q_row = jnp.concatenate([q8[k : k + 1, :] for k in range(8)], axis=1)
    q_matrix = jnp.where(own_head, q_row, 0.0).astype(BF16)
    with scope("w_wk"):
        load_wk.wait()
    nt = (((1,), (1,)), ((), ()))
    qk = lax.dot_general(q_matrix, wk_v[...], nt, preferred_element_type=F32) * 0.125
    qk_o[...] = qk[:8] + pltpu.roll(qk[8:], 64, axis=1)

    position = vx * 16 + vy
    partner_pos = position + 1 - 2 * c
    n_vars = vslot.shape[1]
    row8 = lax.broadcasted_iota(jnp.int32, (8, n_vars), 0)
    slot_id = jnp.where(row8 == 0, position, jnp.where(row8 == 1, partner_pos, -1))
    match = (vslot[...] == slot_id).astype(F32)
    load_emb.wait()
    er[...] = jnp.dot(match.astype(BF16), emb[...], preferred_element_type=F32)
    used[...] = jnp.broadcast_to(jnp.sum(match, axis=1, keepdims=True), (8, 128))

    with scope("w_barrier"):
        pl.semaphore_wait(barrier, len(partners))

    mine = (zl * 4 + y) * 2 + c
    qk_copies = [cp.remote(qk_o, qkg.at[mine], p) for p in group_peers]

    class Gather:
        def __init__(self, g, local):
            self.g = g
            local.wait()
            self.y, self.z, self.core = {}, {}, {}

        def put(self, o, half, zz, device):
            rows = 64 if half is None else 32
            start = row_of((y + o) % 4, zz, c) + (half or 0) * 32
            ref = self.g.at[pl.ds(pl.multiple_of(start, 32), rows), :]
            return cp.remote(ref, ref, device)

        def to_y(self):
            for o in (1, 3, 2):
                self.y[4 - o] = self.put(0, None, zl, peer("y", o))

        def to_z(self, o):
            self.z[o] = [self.put(o, half, zl, peer("z", 1 + 2 * half)) for half in (0, 1)]

        def to_core(self, o, far):
            self.core.setdefault(o, []).append(self.put(o, None, 1 - zl if far else zl, other))

        def start(self):
            self.to_y()
            self.to_z(0)
            self.to_core(0, False)

        def from_y(self, *order):
            for o in order:
                self.y[o].wait_recv()
                self.to_z(o)
                self.to_core(o, False)

        def from_z(self, *order):
            for o in order:
                for k in self.z[o]:
                    k.wait_recv()
                self.to_core(o, True)

        def complete(self, *order):
            for o in order:
                for k in self.core[o]:
                    k.wait_recv()

    with scope("gatherA"):
        A = [Gather(gv.at[b], load_wv[b]) for b in range(4)]
        A[0].start()
        tok_copy = cp.remote(tok.at[:, 1 - c], tokv.at[1], other)
        for b in range(1, 4):
            A[b].start()

    def mix(k):
        def step(i, carry):
            t = tokv[k, pl.ds(i * 8, 8)].astype(F32).reshape(64, D)
            mixed[pl.ds(pl.multiple_of(k * 512 + i * 64, 64), 64), :] = (t + er[k : k + 1, :]).astype(BF16)
            return carry

        lax.fori_loop(0, 8, step, 0)

    def score(k):
        rows = slice(k * 512, k * 512 + 512)
        d = lax.dot_general(mixed[rows, :], qkt[...], nt, preferred_element_type=F32)
        d = d + pltpu.roll(d, 112, axis=1)
        sc[rows, :] = jnp.where(used[k : k + 1, :] > 0, d, BIG)

    def pair_stats(i, carry):
        low, high = pl.ds(pl.multiple_of(i * 128, 128), 128), pl.ds(pl.multiple_of(512 + i * 128, 128), 128)
        s0, s1 = sc[low, :], sc[high, :]
        m = jnp.maximum(s0, s1)
        w0 = used[0:1, :] * jnp.exp(s0 - m)
        w1 = used[1:2, :] * jnp.exp(s1 - m)
        st0[i] = pack_stats(m, w0 + w1).reshape(4, 4, 8, 128)
        sc[low, :] = w0
        sc[high, :] = w1
        return carry

    with scope("mix0"):
        load_tok.wait()
        mix(0)
    with scope("y0"):
        A[0].from_y(3, 1)
    with scope("z00"):
        A[0].from_z(0)
    with scope("w_tok"):
        tok_copy.wait_recv()
    with scope("mix1"):
        mix(1)
    with scope("o0"):
        A[0].from_y(2)
    with scope("z01"):
        A[1].from_z(0)
    with scope("y1"):
        A[1].from_y(3, 1)
    with scope("w_qk"):
        for k in qk_copies:
            k.wait_recv()
    with scope("qkt"):
        qkg[mine] = qk_o[...]
        left = lax.broadcasted_iota(jnp.int32, (8, 128), 1) < 64
        columns = []
        for k in range(8):
            a, b = qkg[2 * k], qkg[2 * k + 1]
            top = jnp.where(left, a, pltpu.roll(b, 64, axis=1))
            bottom = jnp.where(left, pltpu.roll(a, 64, axis=1), b)
            columns.append(jnp.concatenate([top, bottom], axis=0))
        q_keys = jnp.concatenate(columns, axis=1)
        q_high = q_keys.astype(BF16)
        q_low = (q_keys - q_high.astype(F32)).astype(BF16)
        qkt[...] = jnp.concatenate([q_high, q_low, jnp.zeros((96, D), BF16)], axis=0)
    with scope("score0"):
        score(0)
    with scope("o1"):
        A[1].from_y(2)
    with scope("y2"):
        A[2].from_z(0)
        A[2].from_y(3, 1)
    with scope("zy0"):
        A[0].from_z(3, 1)
    with scope("score1"):
        score(1)
    with scope("o2"):
        A[2].from_y(2)
    with scope("y3"):
        A[3].from_z(0)
        A[3].from_y(3, 1)
    with scope("pair_stats"):
        lax.fori_loop(0, 4, pair_stats, 0)
    with scope("zo0"):
        A[0].from_z(2)
    with scope("o3"):
        A[3].from_y(2)
    with scope("gatherB"):
        B = Gather(go, load_wo)
        B.to_y()

    for t, (l0, w, dims) in zip(T, PARTS):
        axis = NAT.index(dims[0])
        t["sc1"] = []
        for o in (1, 2, 3):
            rows = pick(st0, axis, (me[dims[0]] + o) % 4, slice(None), 3)
            t["ts1"][o - 1] = fold(rows)
            t["sc1"].append(cp.remote(t["ts1"].at[o - 1], t["tr1"].at[o - 1], peer(dims[0], o)))

    def stats1():
        for t, (l0, w, dims) in zip(T, PARTS):
            for k in t["sc1"]:
                k.wait_recv()
            own = pick(st0, NAT.index(dims[0]), me[dims[0]], slice(None), 3)
            m, l, scales = merge_stats([own] + [unfold(t["tr1"][o]) for o in range(3)])
            for k, a in enumerate(scales):
                t["ax1"][k] = expand(a, l0, w)
            left = [d for d in NAT if d != dims[0]]
            axis = left.index(dims[1])
            t["st1"] = pack_stats(m, l).reshape(4, 4, 8, 128)
            stats = t["st1"]
            pieces = [(stats[i] if axis == 0 else stats[:, i]).reshape(32, 128) for i in range(4)]
            t["own1"] = choose(pieces, me[dims[1]])
            t["sc2"] = []
            for o in (1, 2, 3):
                t["ts2"][o - 1] = fold(choose(pieces, (me[dims[1]] + o) % 4))
                t["sc2"].append(cp.remote(t["ts2"].at[o - 1], t["tr2"].at[o - 1], peer(dims[1], o)))

    def choose(pieces, index):
        got = pieces[3]
        for i in (2, 1, 0):
            got = jnp.where(index == i, pieces[i], got)
        return got

    def stats2():
        for t, (l0, w, dims) in zip(T, PARTS):
            for k in t["sc2"]:
                k.wait_recv()
            m, l, scales = merge_stats([t["own1"]] + [unfold(t["tr2"][o]) for o in range(3)])
            for k, a in enumerate(scales):
                t["ax2"][k] = expand(a, l0, w)
            stats = pack_stats(m, l)
            pieces = [stats[8 * i : 8 * i + 8] for i in range(4)]
            t["own2"] = choose(pieces, me[dims[2]])
            t["sc3"] = []
            for o in (1, 2, 3):
                t["ts3"][o - 1] = choose(pieces, (me[dims[2]] + o) % 4)
                t["sc3"].append(cp.remote(t["ts3"].at[o - 1], t["tr3"].at[o - 1], peer(dims[2], o)))

    def stats3():
        for t, (l0, w, dims) in zip(T, PARTS):
            for k in t["sc3"]:
                k.wait_recv()
            m, l, scales = merge_stats([t["own2"]] + [t["tr3"][o] for o in range(3)])
            for k, a in enumerate(scales):
                t["ax3"][k] = expand(a / l, l0, w)

    def offsets(o):
        yy = (y + o) % 4
        return pl.multiple_of(yy * 128, 128), pl.multiple_of((4 + yy) * 128, 128)

    def left_cols(start, rows, groups):
        at = pl.ds(pl.multiple_of(start, rows), rows)
        return jnp.concatenate([mixed[at, pl.ds(a, 128)] for o in groups for a in offsets(o)], axis=1)

    def right_rows(b, groups):
        return jnp.concatenate([gv[b, pl.ds(a, 128), :] for o in groups for a in offsets(o)], axis=0)

    def early(b, groups):
        cols = slice(BLOCK * b, BLOCK * b + BLOCK)

        def step(i, carry):
            at = pl.ds(pl.multiple_of(i * 256, 256), 256)
            V[at, cols] = jnp.dot(left_cols(i * 256, 256, groups), right_rows(b, groups), preferred_element_type=F32)
            return carry

        lax.fori_loop(0, 4, step, 0)

    def late_rows(b, groups, i):
        cols = slice(BLOCK * b, BLOCK * b + BLOCK)
        total = None
        for k in range(2):
            start = k * 512 + i * 128
            at = pl.ds(pl.multiple_of(start, 128), 128)
            r = jnp.dot(left_cols(start, 128, groups), right_rows(b, groups), preferred_element_type=F32)
            if len(groups) < 4:
                r = r + V[at, cols]
            part = r * expand(sc[at, :], BLOCK * b, BLOCK)
            total = part if total is None else total + part
        Pacc[i, :, :, :, cols] = total.reshape(4, 4, 8, BLOCK)

    def late(b, groups):
        def step(i, carry):
            late_rows(b, groups, i)
            return carry

        lax.fori_loop(0, 4, step, 0)

    ALL = (0, 3, 1, 2)

    def send1(b, o):
        p = 0 if b < 2 else b - 1
        t, (l0, w, dims) = T[p], PARTS[p]
        index = (me[dims[0]] + o) % 4
        s = b % 2 * 3 + o - 1 if p == 0 else o - 1
        t["s1"][s] = pick(Pacc, NAT.index(dims[0]), index, slice(BLOCK * b, BLOCK * b + BLOCK), 3).astype(BF16)
        t["c1"].append(cp.remote(t["s1"].at[s], t["r1"].at[s], peer(dims[0], o)))

    for t in T:
        t["c1"] = []
    with scope("zy1"):
        A[1].from_z(3, 1)
    with scope("c00"):
        A[0].complete(0, 3, 1)
    with scope("early0"):
        early(0, ALL[:3])
    with scope("zo1"):
        A[1].from_z(2)
    with scope("zy2"):
        A[2].from_z(3, 1)
    with scope("c0"):
        A[0].complete(2)
    with scope("late0"):
        for o in (2, 1, 3):
            late_rows(0, ALL[3:], (x + o) % 4)
            send1(0, o)
        late_rows(0, ALL[3:], x)
    with scope("B_z0"):
        B.to_z(0)
        B.to_core(0, False)
        B.from_y(3, 1)
    with scope("zo2"):
        A[2].from_z(2)
    with scope("c1"):
        A[1].complete(0, 3, 1, 2)
    with scope("late1"):
        for o in (2, 1, 3):
            late_rows(1, ALL, (x + o) % 4)
            send1(1, o)
        late_rows(1, ALL, x)
    with scope("zy3"):
        A[3].from_z(3, 1)
    with scope("zo3"):
        A[3].from_z(2)
    with scope("c2"):
        A[2].complete(0, 3, 1, 2)
    with scope("late2"):
        late(2, ALL)
        for o in (2, 1, 3):
            send1(2, o)
    with scope("c3"):
        A[3].complete(0, 3, 1, 2)
    with scope("late3"):
        late(3, ALL)
        for o in (2, 1, 3):
            send1(3, o)
    with scope("B_o"):
        B.from_y(2)
    with scope("stats1"):
        stats1()
    with scope("B_z"):
        B.from_z(0, 3, 1, 2)

    for t, (l0, w, dims) in zip(T, PARTS):
        for s in range(w // BLOCK):
            with scope("w_c1"):
                for k in t["c1"][3 * s : 3 * s + 3]:
                    k.wait_recv()
            cols = slice(BLOCK * s, BLOCK * s + BLOCK)
            own = pick(Pacc, NAT.index(dims[0]), me[dims[0]], slice(l0 + BLOCK * s, l0 + BLOCK * s + BLOCK), 3)
            total = t["ax1"][0, :, cols] * own
            for o in range(3):
                total = total + t["ax1"][o + 1, :, cols] * t["r1"][3 * s + o].astype(F32)
            t["m1"][:, :, :, cols] = total.reshape(4, 4, 8, BLOCK)
        left = [d for d in NAT if d != dims[0]]
        axis = left.index(dims[1])
        t["c2"] = []
        for o in (2, 1, 3):
            t["s2"][o - 1] = pick(t["m1"], axis, (me[dims[1]] + o) % 4, slice(None), 2).astype(BF16)
            t["c2"].append(cp.remote(t["s2"].at[o - 1], t["r2"].at[o - 1], peer(dims[1], o)))
    with scope("stats2"):
        stats2()

    for t, (l0, w, dims) in zip(T, PARTS):
        left = [d for d in NAT if d != dims[0]]
        own = pick(t["m1"], left.index(dims[1]), me[dims[1]], slice(None), 2)
        total = t["ax2"][0] * own
        with scope("w_c2"):
            for k in t["c2"]:
                k.wait_recv()
        for o in range(3):
            total = total + t["ax2"][o + 1] * t["r2"][o].astype(F32)
        t["m2"][...] = total.reshape(4, 8, w)
        t["c3"] = []
        for o in (2, 1, 3):
            t["s3"][o - 1] = t["m2"][(me[dims[2]] + o) % 4]
            t["c3"].append(cp.remote(t["s3"].at[o - 1], t["r3"].at[o - 1], peer(dims[2], o)))

    with scope("stats3"):
        stats3()
    context = []
    for t, (l0, w, dims) in sorted(zip(T, PARTS), key=lambda tp: tp[1][0]):
        total = t["ax3"][0] * t["m2"][me[dims[2]]]
        with scope("w_c3"):
            for k in t["c3"]:
                k.wait_recv()
        for o in range(3):
            total = total + t["ax3"][o + 1] * t["r3"][o]
        context.append(total)
    with scope("B_c"):
        for o in (0, 3, 1, 2):
            B.complete(o)
    with scope("tail"):
        context = jnp.concatenate(context, axis=1).astype(BF16)
        out[...] = jnp.dot(context, go[...], preferred_element_type=F32).astype(BF16)
    with scope("w_sends"):
        for k in cp.open:
            k.wait_send()


def shards(tokens, var_embed, query, key_weight, value_weight, out_weight, var_slot):
    vm = pl.BlockSpec(memory_space=pltpu.VMEM)
    hbm = pl.BlockSpec(memory_space=pl.ANY)
    V = pltpu.VMEM
    part = []
    for _, w, _ in PARTS:
        part += [
            V((w // BLOCK * 3, 128, BLOCK), BF16), V((w // BLOCK * 3, 128, BLOCK), BF16),
            V((3, 32, w), BF16), V((3, 32, w), BF16),
            V((3, 8, w), F32), V((3, 8, w), F32),
            V((4, 4, 8, w), F32), V((4, 8, w), F32),
            V((3, 32, 128), F32), V((3, 32, 128), F32),
            V((3, 8, 128), F32), V((3, 8, 128), F32),
            V((3, 8, 128), F32), V((3, 8, 128), F32),
            V((4, 128, w), F32), V((4, 32, w), F32), V((4, 8, w), F32),
        ]
    result = pl.pallas_call(
        kernel,
        out_shape=jax.ShapeDtypeStruct((8, D), BF16),
        in_specs=[hbm, hbm, vm, hbm, hbm, hbm, vm],
        out_specs=vm,
        scratch_shapes=[
            V((91, D), BF16), V((128, D), BF16), V((2, 64, 8, D), BF16), V((1024, D), BF16),
            V((4, D, BLOCK), BF16), V((D, D), BF16),
            V((1024, D), F32), V((4, 4, 4, 8, D), F32), V((4, 4, 4, 8, 128), F32),
            V((8, 128), F32), V((16, 8, 128), F32), V((128, D), BF16), V((8, D), F32), V((8, 128), F32), V((1024, 128), F32),
            *part,
            pltpu.SemaphoreType.DMA((SEND_SEMS,)), pltpu.SemaphoreType.DMA((SEND_SEMS,)), pltpu.SemaphoreType.DMA((10,)),
        ],
        compiler_params=pltpu.CompilerParams(
            collective_id=0, has_side_effects=True, vmem_limit_bytes=60 * 1024 * 1024
        ),
    )(
        tokens.reshape(64, 2, 8, D), var_embed, query.reshape(8, 128), key_weight, value_weight, out_weight,
        var_slot.reshape(1, -1),
    )
    return result.reshape(1, 8, D)


def solution(mesh):
    placed = (
        P(("vx", "vy"), None, None, None), P(), P(), P("vy", None), P("vy", None), P("vy", None), P(),
    )
    return jax.shard_map(
        shards, mesh=mesh, in_specs=placed, out_specs=P(None, ("vx", "vy"), None), check_vma=False
    )
```

```python
import contextlib
import functools

import jax
import jax.numpy as jnp
from jax import lax
from jax.experimental import pallas as pl
from jax.experimental.pallas import tpu as pltpu
from jax.sharding import PartitionSpec as P

MESH = pl.DeviceIdType.MESH
F32, BF16 = jnp.float32, jnp.bfloat16
HEADS = 16
D = 1024
BIG = -1e30

NAT = ("x", "z", "y")
PARTS = ((0, 512, ("x", "y", "z")), (512, 256, ("y", "z", "x")), (768, 256, ("z", "x", "y")))
BLOCK = 256
SEND_SEMS = 200


def scope(name):
    return contextlib.nullcontext()


def device_of(x, y, z, c):
    return (x * 2 + z // 2, (z % 2) * 8 + y * 2 + c)


class Copies:
    def __init__(self, send, recv, local):
        self.send, self.recv, self.local = send, recv, local
        self.n, self.k, self.open = 0, 0, []

    def remote(self, src, dst, device):
        copy = pltpu.make_async_remote_copy(
            src_ref=src,
            dst_ref=dst,
            send_sem=self.send.at[self.n],
            recv_sem=self.recv.at[self.n],
            device_id=device,
            device_id_type=MESH,
        )
        self.n += 1
        copy.start()
        self.open.append(copy)
        return copy

    def here(self, src, dst):
        copy = pltpu.make_async_copy(src, dst, self.local.at[self.k])
        self.k += 1
        copy.start()
        return copy


def lanes_iota(rows):
    return lax.broadcasted_iota(jnp.int32, (rows, 128), 1)


def expand(a, l0, w):
    half = lanes_iota(a.shape[0]) // 64
    tiles = [jnp.take_along_axis(a, half + 2 * t, axis=1, mode="promise_in_bounds") for t in range(l0 // 128, (l0 + w) // 128)]
    return jnp.concatenate(tiles, axis=1)


def fold(rows):
    lane = lanes_iota(rows.shape[0])
    rows = jnp.where(lane < 32, rows, 0.0)
    q = rows.shape[0] // 4
    out = rows[:q]
    for g in range(1, 4):
        out = out + pltpu.roll(rows[g * q : (g + 1) * q], 32 * g, axis=1)
    return out


def unfold(packed):
    pieces = [packed]
    for g in range(1, 4):
        pieces.append(pltpu.roll(packed, 128 - 32 * g, axis=1))
    return jnp.concatenate(pieces, axis=0)


def pack_stats(m, l):
    lane = lanes_iota(m.shape[0])
    return jnp.where(lane < 16, m, jnp.where(lane < 32, pltpu.roll(l, 16, axis=1), 0.0))


def merge_stats(stats):
    m = functools.reduce(jnp.maximum, stats)
    scales = [jnp.exp(s - m) for s in stats]
    l = sum(a * pltpu.roll(s, 112, axis=1) for a, s in zip(scales, stats))
    return m, l, scales


def pick(ref, axis, index, lanes, ndim):
    where = [slice(None)] * (ndim + 2)
    where[axis] = index
    where[-1] = lanes
    got = ref[tuple(where)]
    return got.reshape(-1, got.shape[-1])


def kernel(tok, emb_h, query_h, wk, wv, wo, vslot_h, out, emb, query, vslot, wk_v, tokv, mixed, gv, go, V, Pacc, st0, qk_o, qkg, qkt,
           er, used, sc, *rest):
    ssem, rsem, lsem = rest[-3:]
    per_part = [rest[i * 17 : (i + 1) * 17] for i in range(len(PARTS))]
    names = ("s1", "r1", "s2", "r2", "s3", "r3", "m1", "m2", "ts1", "tr1", "ts2", "tr2", "ts3", "tr3", "ax1", "ax2", "ax3")
    T = [dict(zip(names, p)) for p in per_part]
    cp = Copies(ssem, rsem, lsem)

    vx, vy = lax.axis_index("vx"), lax.axis_index("vy")
    x, z = vx // 2, (vx % 2) * 2 + vy // 8
    y, c = (vy // 2) % 4, vy % 2
    zl = z % 2
    zmate = z + 1 - 2 * zl
    me = {"x": x, "y": y, "z": z}

    def peer(dim, offset):
        at = dict(me)
        at[dim] = (me[dim] + offset) % 4
        return device_of(at["x"], at["y"], at["z"], c)

    other = device_of(x, y, z, 1 - c)
    group_peers = [other, device_of(x, y, zmate, c), device_of(x, y, zmate, 1 - c)]
    for o in (1, 2, 3):
        group_peers += [device_of(x, (y + o) % 4, zz, cc) for zz in (z, zmate) for cc in (c, 1 - c)]

    barrier = pltpu.get_barrier_semaphore()
    partners = group_peers + [peer("x", o) for o in (1, 2, 3)] + [device_of(x, y, (zmate + 2) % 4, c), peer("z", 2)]
    for p in partners:
        pl.semaphore_signal(barrier, inc=1, device_id=p, device_id_type=MESH)
    load_wk = cp.here(wk, wk_v.at[pl.ds(0, 64), :])
    load_query = cp.here(query_h, query)
    load_slot = cp.here(vslot_h, vslot)
    load_emb = cp.here(emb_h, emb)
    load_tok = cp.here(tok.at[:, c], tokv.at[0])

    def row_of(yy, zz, cc):
        return pl.multiple_of(((zz * 4 + yy) * 2 + cc) * 64, 64)

    own_rows = pl.ds(row_of(y, zl, c), 64)
    load_wv = [cp.here(wv.at[:, BLOCK * b : BLOCK * b + BLOCK], gv.at[b, own_rows, :]) for b in range(4)]
    load_wo = cp.here(wo, go.at[own_rows, :])

    head_lane = lax.broadcasted_iota(jnp.int32, (HEADS, D), 1) // 64
    head_row = lax.broadcasted_iota(jnp.int32, (HEADS, D), 0)
    own_head = head_lane == head_row
    wk_v[64:128, :] = jnp.zeros((64, D), BF16)
    load_query.wait()
    q8 = query[...].astype(F32)
    q_row = jnp.concatenate([q8[k : k + 1, :] for k in range(8)], axis=1)
    q_matrix = jnp.where(own_head, q_row, 0.0).astype(BF16)
    with scope("w_wk"):
        load_wk.wait()
    nt = (((1,), (1,)), ((), ()))
    qk = lax.dot_general(q_matrix, wk_v[...], nt, preferred_element_type=F32) * 0.125
    qk_o[...] = qk[:8] + pltpu.roll(qk[8:], 64, axis=1)

    position = vx * 16 + vy
    partner_pos = position + 1 - 2 * c
    load_slot.wait()
    n_vars = vslot.shape[1]
    row8 = lax.broadcasted_iota(jnp.int32, (8, n_vars), 0)
    slot_id = jnp.where(row8 == 0, position, jnp.where(row8 == 1, partner_pos, -1))
    match = (vslot[...] == slot_id).astype(F32)
    load_emb.wait()
    er[...] = jnp.dot(match.astype(BF16), emb[...], preferred_element_type=F32)
    used[...] = jnp.broadcast_to(jnp.sum(match, axis=1, keepdims=True), (8, 128))

    with scope("w_barrier"):
        pl.semaphore_wait(barrier, len(partners))

    mine = (zl * 4 + y) * 2 + c
    qk_copies = [cp.remote(qk_o, qkg.at[mine], p) for p in group_peers]

    class Gather:
        def __init__(self, g, local):
            self.g = g
            local.wait()
            self.y, self.z, self.core = {}, {}, {}

        def put(self, o, half, zz, device):
            rows = 64 if half is None else 32
            start = row_of((y + o) % 4, zz, c) + (half or 0) * 32
            ref = self.g.at[pl.ds(pl.multiple_of(start, 32), rows), :]
            return cp.remote(ref, ref, device)

        def to_y(self):
            for o in (1, 3, 2):
                self.y[4 - o] = self.put(0, None, zl, peer("y", o))

        def to_z(self, o):
            self.z[o] = [self.put(o, half, zl, peer("z", 1 + 2 * half)) for half in (0, 1)]

        def to_core(self, o, far):
            self.core.setdefault(o, []).append(self.put(o, None, 1 - zl if far else zl, other))

        def start(self):
            self.to_y()
            self.to_z(0)
            self.to_core(0, False)

        def from_y(self, *order):
            for o in order:
                self.y[o].wait_recv()
                self.to_z(o)
                self.to_core(o, False)

        def from_z(self, *order):
            for o in order:
                for k in self.z[o]:
                    k.wait_recv()
                self.to_core(o, True)

        def complete(self, *order):
            for o in order:
                for k in self.core[o]:
                    k.wait_recv()

    with scope("gatherA"):
        A = [Gather(gv.at[b], load_wv[b]) for b in range(4)]
        A[0].start()
        tok_copy = cp.remote(tok.at[:, 1 - c], tokv.at[1], other)
        for b in range(1, 4):
            A[b].start()
        B = Gather(go, load_wo)
        B.start()

    def mix(k):
        def step(i, carry):
            t = tokv[k, pl.ds(i * 8, 8)].astype(F32).reshape(64, D)
            mixed[pl.ds(pl.multiple_of(k * 512 + i * 64, 64), 64), :] = (t + er[k : k + 1, :]).astype(BF16)
            return carry

        lax.fori_loop(0, 8, step, 0)

    def score(k):
        rows = slice(k * 512, k * 512 + 512)
        d = lax.dot_general(mixed[rows, :], qkt[...], nt, preferred_element_type=F32)
        d = d + pltpu.roll(d, 112, axis=1)
        sc[rows, :] = jnp.where(used[k : k + 1, :] > 0, d, BIG)

    def pair_stats(i, carry):
        low, high = pl.ds(pl.multiple_of(i * 128, 128), 128), pl.ds(pl.multiple_of(512 + i * 128, 128), 128)
        s0, s1 = sc[low, :], sc[high, :]
        m = jnp.maximum(s0, s1)
        w0 = used[0:1, :] * jnp.exp(s0 - m)
        w1 = used[1:2, :] * jnp.exp(s1 - m)
        st0[i] = pack_stats(m, w0 + w1).reshape(4, 4, 8, 128)
        sc[low, :] = w0
        sc[high, :] = w1
        return carry

    with scope("mix0"):
        load_tok.wait()
        mix(0)
    with scope("y0"):
        A[0].from_y(3, 1)
    with scope("z00"):
        A[0].from_z(0)
    with scope("w_tok"):
        tok_copy.wait_recv()
    with scope("mix1"):
        mix(1)
    with scope("o0"):
        A[0].from_y(2)
    with scope("z01"):
        A[1].from_z(0)
    with scope("y1"):
        A[1].from_y(3, 1)
    with scope("w_qk"):
        for k in qk_copies:
            k.wait_recv()
    with scope("qkt"):
        qkg[mine] = qk_o[...]
        left = lax.broadcasted_iota(jnp.int32, (8, 128), 1) < 64
        columns = []
        for k in range(8):
            a, b = qkg[2 * k], qkg[2 * k + 1]
            top = jnp.where(left, a, pltpu.roll(b, 64, axis=1))
            bottom = jnp.where(left, pltpu.roll(a, 64, axis=1), b)
            columns.append(jnp.concatenate([top, bottom], axis=0))
        q_keys = jnp.concatenate(columns, axis=1)
        q_high = q_keys.astype(BF16)
        q_low = (q_keys - q_high.astype(F32)).astype(BF16)
        qkt[...] = jnp.concatenate([q_high, q_low, jnp.zeros((96, D), BF16)], axis=0)
    with scope("score0"):
        score(0)
    with scope("o1"):
        A[1].from_y(2)
    with scope("y2"):
        A[2].from_z(0)
        A[2].from_y(3, 1)
    with scope("zy0"):
        A[0].from_z(3, 1)
    with scope("score1"):
        score(1)
    with scope("o2"):
        A[2].from_y(2)
    with scope("y3"):
        A[3].from_z(0)
        A[3].from_y(3, 1)
    with scope("pair_stats"):
        lax.fori_loop(0, 4, pair_stats, 0)
    with scope("zo0"):
        A[0].from_z(2)
    with scope("o3"):
        A[3].from_y(2)

    def stats0():
        for t, (l0, w, dims) in zip(T, PARTS):
            axis = NAT.index(dims[0])
            t["sc1"] = []
            for o in (1, 2, 3):
                rows = pick(st0, axis, (me[dims[0]] + o) % 4, slice(None), 3)
                t["ts1"][o - 1] = fold(rows)
        for t, (l0, w, dims) in zip(T, PARTS):
            for o in (1, 2, 3):
                t["sc1"].append(cp.remote(t["ts1"].at[o - 1], t["tr1"].at[o - 1], peer(dims[0], o)))

    def stats1():
        for t, (l0, w, dims) in zip(T, PARTS):
            for k in t["sc1"]:
                k.wait_recv()
            own = pick(st0, NAT.index(dims[0]), me[dims[0]], slice(None), 3)
            m, l, scales = merge_stats([own] + [unfold(t["tr1"][o]) for o in range(3)])
            for k, a in enumerate(scales):
                t["ax1"][k] = expand(a, l0, w)
            left = [d for d in NAT if d != dims[0]]
            axis = left.index(dims[1])
            t["st1"] = pack_stats(m, l).reshape(4, 4, 8, 128)
            stats = t["st1"]
            pieces = [(stats[i] if axis == 0 else stats[:, i]).reshape(32, 128) for i in range(4)]
            t["own1"] = choose(pieces, me[dims[1]])
            t["sc2"] = []
            for o in (1, 2, 3):
                t["ts2"][o - 1] = fold(choose(pieces, (me[dims[1]] + o) % 4))
                t["sc2"].append(cp.remote(t["ts2"].at[o - 1], t["tr2"].at[o - 1], peer(dims[1], o)))

    def choose(pieces, index):
        got = pieces[3]
        for i in (2, 1, 0):
            got = jnp.where(index == i, pieces[i], got)
        return got

    def stats2():
        for t, (l0, w, dims) in zip(T, PARTS):
            for k in t["sc2"]:
                k.wait_recv()
            m, l, scales = merge_stats([t["own1"]] + [unfold(t["tr2"][o]) for o in range(3)])
            for k, a in enumerate(scales):
                t["ax2"][k] = expand(a, l0, w)
            stats = pack_stats(m, l)
            pieces = [stats[8 * i : 8 * i + 8] for i in range(4)]
            t["own2"] = choose(pieces, me[dims[2]])
            t["sc3"] = []
            for o in (1, 2, 3):
                t["ts3"][o - 1] = choose(pieces, (me[dims[2]] + o) % 4)
                t["sc3"].append(cp.remote(t["ts3"].at[o - 1], t["tr3"].at[o - 1], peer(dims[2], o)))

    def stats3():
        for t, (l0, w, dims) in zip(T, PARTS):
            for k in t["sc3"]:
                k.wait_recv()
            m, l, scales = merge_stats([t["own2"]] + [t["tr3"][o] for o in range(3)])
            for k, a in enumerate(scales):
                t["ax3"][k] = expand(a / l, l0, w)

    def offsets(o):
        yy = (y + o) % 4
        return pl.multiple_of(yy * 128, 128), pl.multiple_of((4 + yy) * 128, 128)

    def left_cols(start, rows, groups):
        at = pl.ds(pl.multiple_of(start, rows), rows)
        return jnp.concatenate([mixed[at, pl.ds(a, 128)] for o in groups for a in offsets(o)], axis=1)

    def right_rows(b, groups):
        return jnp.concatenate([gv[b, pl.ds(a, 128), :] for o in groups for a in offsets(o)], axis=0)

    def early(b, groups):
        cols = slice(BLOCK * b, BLOCK * b + BLOCK)

        def step(i, carry):
            at = pl.ds(pl.multiple_of(i * 256, 256), 256)
            V[at, cols] = jnp.dot(left_cols(i * 256, 256, groups), right_rows(b, groups), preferred_element_type=F32)
            return carry

        lax.fori_loop(0, 4, step, 0)

    def weighted(b, groups, starts, rows):
        cols = slice(BLOCK * b, BLOCK * b + BLOCK)
        spans = [pl.ds(pl.multiple_of(k * 512 + start, rows), rows) for k in range(2) for start in starts]
        lhs = jnp.concatenate(
            [jnp.concatenate([mixed[at, pl.ds(a, 128)] for o in groups for a in offsets(o)], axis=1) for at in spans], axis=0
        )
        r = jnp.dot(lhs, right_rows(b, groups), preferred_element_type=F32)
        if len(groups) < 4:
            r = r + jnp.concatenate([V[at, cols] for at in spans], axis=0)
        r = r * expand(jnp.concatenate([sc[at, :] for at in spans], axis=0), BLOCK * b, BLOCK)
        return r[:128] + r[128:]

    def late_rows(b, groups, i):
        Pacc[i, :, :, :, BLOCK * b : BLOCK * b + BLOCK] = weighted(b, groups, [i * 128], 128).reshape(4, 4, 8, BLOCK)

    def late_by_z(b, groups, i):
        return weighted(b, groups, [k * 128 + i * 32 for k in range(4)], 32)

    def late(b, groups):
        def step(i, carry):
            late_rows(b, groups, i)
            return carry

        lax.fori_loop(0, 4, step, 0)

    ALL = (0, 3, 1, 2)

    def send1(b, o):
        p = 0 if b < 2 else b - 1
        t, (l0, w, dims) = T[p], PARTS[p]
        index = (me[dims[0]] + o) % 4
        s = b % 2 * 3 + o - 1 if p == 0 else o - 1
        t["s1"][s] = pick(Pacc, NAT.index(dims[0]), index, slice(BLOCK * b, BLOCK * b + BLOCK), 3).astype(BF16)
        t["c1"].append(cp.remote(t["s1"].at[s], t["r1"].at[s], peer(dims[0], o)))

    for t in T:
        t["c1"] = []
    with scope("zy1"):
        A[1].from_z(3, 1)
    with scope("c00"):
        A[0].complete(0, 3, 1)
    with scope("early0"):
        early(0, ALL[:3])
    with scope("zo1"):
        A[1].from_z(2)
    with scope("zy2"):
        A[2].from_z(3, 1)
    with scope("c0"):
        A[0].complete(2)
    with scope("late0"):
        for o in (2, 1, 3):
            late_rows(0, ALL[3:], (x + o) % 4)
            send1(0, o)
        late_rows(0, ALL[3:], x)
    with scope("stats0"):
        stats0()
    with scope("B_z0"):
        B.from_z(0)
    with scope("zo2"):
        A[2].from_z(2)
    with scope("c1"):
        A[1].complete(0, 3, 1, 2)
    with scope("late1"):
        for o in (2, 1, 3):
            late_rows(1, ALL, (x + o) % 4)
            send1(1, o)
        late_rows(1, ALL, x)
    with scope("zy3"):
        A[3].from_z(3, 1)
    with scope("zo3"):
        A[3].from_z(2)
    with scope("c2"):
        A[2].complete(0, 3, 1, 2)
    with scope("late2"):
        late(2, ALL)
        for o in (2, 1, 3):
            send1(2, o)
    with scope("B_y"):
        B.from_y(3, 1, 2)
    with scope("c3"):
        A[3].complete(0, 3, 1, 2)
    with scope("late3"):
        for o in (2, 1, 3):
            T[2]["s1"][o - 1] = late_by_z(3, ALL, (z + o) % 4).astype(BF16)
            T[2]["c1"].append(cp.remote(T[2]["s1"].at[o - 1], T[2]["r1"].at[o - 1], peer("z", o)))
        own_z = late_by_z(3, ALL, z).reshape(4, 4, 8, BLOCK)
        for i in range(4):
            Pacc[i, z, :, :, 768:1024] = own_z[i]
    with scope("stats1"):
        stats1()

    for t, (l0, w, dims) in zip(T, PARTS):
        if t is T[2]:
            with scope("stats2"):
                stats2()
        for s in range(w // BLOCK):
            with scope("w_c1"):
                for k in t["c1"][3 * s : 3 * s + 3]:
                    k.wait_recv()
            cols = slice(BLOCK * s, BLOCK * s + BLOCK)
            own = pick(Pacc, NAT.index(dims[0]), me[dims[0]], slice(l0 + BLOCK * s, l0 + BLOCK * s + BLOCK), 3)
            total = t["ax1"][0, :, cols] * own
            for o in range(3):
                total = total + t["ax1"][o + 1, :, cols] * t["r1"][3 * s + o].astype(F32)
            t["m1"][:, :, :, cols] = total.reshape(4, 4, 8, BLOCK)
        left = [d for d in NAT if d != dims[0]]
        axis = left.index(dims[1])
        t["c2"] = []
        for o in (2, 1, 3):
            t["s2"][o - 1] = pick(t["m1"], axis, (me[dims[1]] + o) % 4, slice(None), 2).astype(BF16)
            t["c2"].append(cp.remote(t["s2"].at[o - 1], t["r2"].at[o - 1], peer(dims[1], o)))
    with scope("B_z"):
        B.from_z(3, 1, 2)

    for t, (l0, w, dims) in zip(T, PARTS):
        left = [d for d in NAT if d != dims[0]]
        own = pick(t["m1"], left.index(dims[1]), me[dims[1]], slice(None), 2)
        total = t["ax2"][0] * own
        with scope("w_c2"):
            for k in t["c2"]:
                k.wait_recv()
        for o in range(3):
            total = total + t["ax2"][o + 1] * t["r2"][o].astype(F32)
        t["m2"][...] = total.reshape(4, 8, w)
        t["c3"] = []
        for o in (2, 1, 3):
            t["s3"][o - 1] = t["m2"][(me[dims[2]] + o) % 4].astype(BF16)
            t["c3"].append(cp.remote(t["s3"].at[o - 1], t["r3"].at[o - 1], peer(dims[2], o)))

    with scope("w_sends0"):
        early_sends, cp.open = cp.open[:-40], cp.open[-40:]
        for k in early_sends:
            k.wait_send()
    with scope("stats3"):
        stats3()
    context = []
    for t, (l0, w, dims) in sorted(zip(T, PARTS), key=lambda tp: tp[1][0]):
        total = t["ax3"][0] * t["m2"][me[dims[2]]]
        with scope("w_c3"):
            for k in t["c3"]:
                k.wait_recv()
        for o in range(3):
            total = total + t["ax3"][o + 1] * t["r3"][o].astype(F32)
        context.append(total)
    with scope("B_c"):
        for o in (0, 3, 1, 2):
            B.complete(o)
    with scope("tail"):
        context = jnp.concatenate(context, axis=1).astype(BF16)
        out[...] = jnp.dot(context, go[...], preferred_element_type=F32).astype(BF16)
    with scope("w_sends"):
        for k in cp.open:
            k.wait_send()


def shards(tokens, var_embed, query, key_weight, value_weight, out_weight, var_slot):
    vm = pl.BlockSpec(memory_space=pltpu.VMEM)
    hbm = pl.BlockSpec(memory_space=pl.ANY)
    V = pltpu.VMEM
    part = []
    for _, w, _ in PARTS:
        part += [
            V((w // BLOCK * 3, 128, BLOCK), BF16), V((w // BLOCK * 3, 128, BLOCK), BF16),
            V((3, 32, w), BF16), V((3, 32, w), BF16),
            V((3, 8, w), BF16), V((3, 8, w), BF16),
            V((4, 4, 8, w), F32), V((4, 8, w), F32),
            V((3, 32, 128), F32), V((3, 32, 128), F32),
            V((3, 8, 128), F32), V((3, 8, 128), F32),
            V((3, 8, 128), F32), V((3, 8, 128), F32),
            V((4, 128, w), F32), V((4, 32, w), F32), V((4, 8, w), F32),
        ]
    result = pl.pallas_call(
        kernel,
        out_shape=jax.ShapeDtypeStruct((8, D), BF16),
        in_specs=[hbm] * 7,
        out_specs=vm,
        scratch_shapes=[
            V((91, D), BF16), V((8, 128), BF16), V((1, 91), jnp.int32), V((128, D), BF16), V((2, 64, 8, D), BF16), V((1024, D), BF16),
            V((4, D, BLOCK), BF16), V((D, D), BF16),
            V((1024, D), F32), V((4, 4, 4, 8, D), F32), V((4, 4, 4, 8, 128), F32),
            V((8, 128), F32), V((16, 8, 128), F32), V((128, D), BF16), V((8, D), F32), V((8, 128), F32), V((1024, 128), F32),
            *part,
            pltpu.SemaphoreType.DMA((SEND_SEMS,)), pltpu.SemaphoreType.DMA((SEND_SEMS,)), pltpu.SemaphoreType.DMA((12,)),
        ],
        compiler_params=pltpu.CompilerParams(
            collective_id=0, has_side_effects=True, vmem_limit_bytes=60 * 1024 * 1024
        ),
    )(
        tokens.reshape(64, 2, 8, D), var_embed, query.reshape(8, 128), key_weight, value_weight, out_weight,
        var_slot.reshape(1, -1),
    )
    return result.reshape(1, 8, D)


def solution(mesh):
    placed = (
        P(("vx", "vy"), None, None, None), P(), P(), P("vy", None), P("vy", None), P("vy", None), P(),
    )
    return jax.shard_map(
        shards, mesh=mesh, in_specs=placed, out_specs=P(None, ("vx", "vy"), None), check_vma=False
    )
```

```python
import contextlib
import functools

import jax
import jax.numpy as jnp
from jax import lax
from jax.experimental import pallas as pl
from jax.experimental.pallas import tpu as pltpu
from jax.sharding import PartitionSpec as P

MESH = pl.DeviceIdType.MESH
F32, BF16 = jnp.float32, jnp.bfloat16
HEADS = 16
D = 1024
BIG = -1e30

NAT = ("x", "z", "y")
PARTS = ((0, 512, ("x", "y", "z")), (512, 512, ("y", "x", "z")))
SEQUENCE = (0, 2, 1, 3)
BLOCK = 256
SEND_SEMS = 200


def scope(name):
    return contextlib.nullcontext()


def device_of(x, y, z, c):
    return (x * 2 + z // 2, (z % 2) * 8 + y * 2 + c)


class Copies:
    def __init__(self, send, recv, local):
        self.send, self.recv, self.local = send, recv, local
        self.n, self.k, self.open = 0, 0, []

    def remote(self, src, dst, device):
        copy = pltpu.make_async_remote_copy(
            src_ref=src,
            dst_ref=dst,
            send_sem=self.send.at[self.n],
            recv_sem=self.recv.at[self.n],
            device_id=device,
            device_id_type=MESH,
        )
        self.n += 1
        copy.start()
        self.open.append(copy)
        return copy

    def here(self, src, dst):
        copy = pltpu.make_async_copy(src, dst, self.local.at[self.k])
        self.k += 1
        copy.start()
        return copy


def lanes_iota(rows):
    return lax.broadcasted_iota(jnp.int32, (rows, 128), 1)


def expand(a, l0, w):
    half = lanes_iota(a.shape[0]) // 64
    tiles = [jnp.take_along_axis(a, half + 2 * t, axis=1, mode="promise_in_bounds") for t in range(l0 // 128, (l0 + w) // 128)]
    return jnp.concatenate(tiles, axis=1)


def fold(rows):
    lane = lanes_iota(rows.shape[0])
    rows = jnp.where(lane < 32, rows, 0.0)
    q = rows.shape[0] // 4
    out = rows[:q]
    for g in range(1, 4):
        out = out + pltpu.roll(rows[g * q : (g + 1) * q], 32 * g, axis=1)
    return out


def unfold(packed):
    pieces = [packed]
    for g in range(1, 4):
        pieces.append(pltpu.roll(packed, 128 - 32 * g, axis=1))
    return jnp.concatenate(pieces, axis=0)


def pack_stats(m, l):
    lane = lanes_iota(m.shape[0])
    return jnp.where(lane < 16, m, jnp.where(lane < 32, pltpu.roll(l, 16, axis=1), 0.0))


def merge_stats(stats):
    m = functools.reduce(jnp.maximum, stats)
    scales = [jnp.exp(s - m) for s in stats]
    l = sum(a * pltpu.roll(s, 112, axis=1) for a, s in zip(scales, stats))
    return m, l, scales


def pick(ref, axis, index, lanes, ndim):
    where = [slice(None)] * (ndim + 2)
    where[axis] = index
    where[-1] = lanes
    got = ref[tuple(where)]
    return got.reshape(-1, got.shape[-1])


def kernel(tok, emb_h, query_h, wk, wv, wo, vslot_h, out, emb, query, vslot, wk_v, tokv, mixed, mixed_y,
           gv, go, V, own1, st0, qk_o, qkg, qkt, er, used, sc, s1, r1, s2, r2, s3, r3, m1, m2, *rest):
    ssem, rsem, lsem = rest[-3:]
    names = ("ts1", "tr1", "ts2", "tr2", "ts3", "tr3", "ax1", "ax2", "ax3")
    T = [dict(zip(names, rest[i * 9 : (i + 1) * 9])) for i in range(len(PARTS))]
    cp = Copies(ssem, rsem, lsem)

    vx, vy = lax.axis_index("vx"), lax.axis_index("vy")
    x, z = vx // 2, (vx % 2) * 2 + vy // 8
    y, c = (vy // 2) % 4, vy % 2
    zl = z % 2
    zmate = z + 1 - 2 * zl
    me = {"x": x, "y": y, "z": z}

    def peer(dim, offset):
        at = dict(me)
        at[dim] = (me[dim] + offset) % 4
        return device_of(at["x"], at["y"], at["z"], c)

    other = device_of(x, y, z, 1 - c)
    group_peers = [other, device_of(x, y, zmate, c), device_of(x, y, zmate, 1 - c)]
    for o in (1, 2, 3):
        group_peers += [device_of(x, (y + o) % 4, zz, cc) for zz in (z, zmate) for cc in (c, 1 - c)]

    barrier = pltpu.get_barrier_semaphore()
    partners = group_peers + [peer("x", o) for o in (1, 2, 3)] + [device_of(x, y, (zmate + 2) % 4, c), peer("z", 2)]
    for p in partners:
        pl.semaphore_signal(barrier, inc=1, device_id=p, device_id_type=MESH)
    load_wk = cp.here(wk, wk_v.at[pl.ds(0, 64), :])
    load_query = cp.here(query_h, query)
    load_slot = cp.here(vslot_h, vslot)
    load_emb = cp.here(emb_h, emb)
    load_tok = cp.here(tok.at[:, :, :, c], tokv.at[0])

    def row_of(yy, zz, cc):
        return pl.multiple_of(((zz * 4 + yy) * 2 + cc) * 64, 64)

    own_rows = pl.ds(row_of(y, zl, c), 64)
    load_wv = [cp.here(wv.at[:, BLOCK * b : BLOCK * b + BLOCK], gv.at[j, own_rows, :]) for j, b in enumerate(SEQUENCE)]
    load_wo = cp.here(wo, go.at[own_rows, :])

    head_lane = lax.broadcasted_iota(jnp.int32, (HEADS, D), 1) // 64
    head_row = lax.broadcasted_iota(jnp.int32, (HEADS, D), 0)
    own_head = head_lane == head_row
    wk_v[64:128, :] = jnp.zeros((64, D), BF16)
    load_query.wait()
    q8 = query[...].astype(F32)
    q_row = jnp.concatenate([q8[k : k + 1, :] for k in range(8)], axis=1)
    q_matrix = jnp.where(own_head, q_row, 0.0).astype(BF16)
    with scope("w_wk"):
        load_wk.wait()
    nt = (((1,), (1,)), ((), ()))
    qk = lax.dot_general(q_matrix, wk_v[...], nt, preferred_element_type=F32) * 0.125
    qk_o[...] = qk[:8] + pltpu.roll(qk[8:], 64, axis=1)

    position = vx * 16 + vy
    partner_pos = position + 1 - 2 * c
    load_slot.wait()
    n_vars = vslot.shape[1]
    row8 = lax.broadcasted_iota(jnp.int32, (8, n_vars), 0)
    slot_id = jnp.where(row8 == 0, position, jnp.where(row8 == 1, partner_pos, -1))
    match = (vslot[...] == slot_id).astype(F32)
    load_emb.wait()
    er[...] = jnp.dot(match.astype(BF16), emb[...], preferred_element_type=F32)
    used[...] = jnp.broadcast_to(jnp.sum(match, axis=1, keepdims=True), (8, 128))

    with scope("w_barrier"):
        pl.semaphore_wait(barrier, len(partners))

    mine = (zl * 4 + y) * 2 + c
    qk_copies = [cp.remote(qk_o, qkg.at[mine], p) for p in group_peers]

    class Gather:
        def __init__(self, g, local):
            self.g = g
            local.wait()
            self.y, self.z, self.core = {}, {}, {}

        def put(self, o, half, zz, device):
            rows = 64 if half is None else 32
            start = row_of((y + o) % 4, zz, c) + (half or 0) * 32
            ref = self.g.at[pl.ds(pl.multiple_of(start, 32), rows), :]
            return cp.remote(ref, ref, device)

        def to_y(self):
            for o in (1, 3, 2):
                self.y[4 - o] = self.put(0, None, zl, peer("y", o))

        def to_z(self, o):
            self.z[o] = [self.put(o, half, zl, peer("z", 1 + 2 * half)) for half in (0, 1)]

        def to_core(self, o, far):
            self.core.setdefault(o, []).append(self.put(o, None, 1 - zl if far else zl, other))

        def start(self):
            self.to_y()
            self.to_z(0)
            self.to_core(0, False)

        def from_y(self, *order):
            for o in order:
                self.y[o].wait_recv()
                self.to_z(o)
                self.to_core(o, False)

        def from_z(self, *order):
            for o in order:
                for k in self.z[o]:
                    k.wait_recv()
                self.to_core(o, True)

        def complete(self, *order):
            for o in order:
                for k in self.core[o]:
                    k.wait_recv()

    with scope("gatherA"):
        A = [Gather(gv.at[b], load_wv[b]) for b in range(4)]
        A[0].start()
        tok_copy = cp.remote(tok.at[:, :, :, 1 - c], tokv.at[1], other)
        for b in range(1, 4):
            A[b].start()
        B = Gather(go, load_wo)
        B.start()

    def mix(k):
        def step(i, carry):
            at = pl.ds(pl.multiple_of(k * 512 + i * 64, 64), 64)
            half = pl.ds(2 * (i % 2), 2)
            t = tokv[k, i // 2, half].astype(F32).reshape(64, D)
            mixed[at, :] = (t + er[k : k + 1, :]).astype(BF16)
            t = tokv[k, half, :, i // 2].astype(F32).reshape(64, D)
            mixed_y[at, :] = (t + er[k : k + 1, :]).astype(BF16)
            return carry

        lax.fori_loop(0, 8, step, 0)

    def score(k):
        d = lax.dot_general(mixed[k * 512 : k * 512 + 512, :], qkt[...], nt, preferred_element_type=F32)
        d = d + pltpu.roll(d, 112, axis=1)
        sc[k] = jnp.where(used[k : k + 1, :] > 0, d, BIG).reshape(4, 4, 4, 8, 128)

    def pair_stats(i, carry):
        s0, s1_ = sc[0, i].reshape(128, 128), sc[1, i].reshape(128, 128)
        m = jnp.maximum(s0, s1_)
        w0 = used[0:1, :] * jnp.exp(s0 - m)
        w1 = used[1:2, :] * jnp.exp(s1_ - m)
        st0[i] = pack_stats(m, w0 + w1).reshape(4, 4, 8, 128)
        sc[0, i] = w0.reshape(4, 4, 8, 128)
        sc[1, i] = w1.reshape(4, 4, 8, 128)
        return carry

    with scope("mix0"):
        load_tok.wait()
        mix(0)
    with scope("y0"):
        A[0].from_y(3, 1)
    with scope("z00"):
        A[0].from_z(0)
    with scope("w_tok"):
        tok_copy.wait_recv()
    with scope("mix1"):
        mix(1)
    with scope("o0"):
        A[0].from_y(2)
    with scope("z01"):
        A[1].from_z(0)
    with scope("y1"):
        A[1].from_y(3, 1)
    with scope("w_qk"):
        for k in qk_copies:
            k.wait_recv()
    with scope("qkt"):
        qkg[mine] = qk_o[...]
        left = lax.broadcasted_iota(jnp.int32, (8, 128), 1) < 64
        columns = []
        for k in range(8):
            a, b = qkg[2 * k], qkg[2 * k + 1]
            top = jnp.where(left, a, pltpu.roll(b, 64, axis=1))
            bottom = jnp.where(left, pltpu.roll(a, 64, axis=1), b)
            columns.append(jnp.concatenate([top, bottom], axis=0))
        q_keys = jnp.concatenate(columns, axis=1)
        q_high = q_keys.astype(BF16)
        q_low = (q_keys - q_high.astype(F32)).astype(BF16)
        qkt[...] = jnp.concatenate([q_high, q_low, jnp.zeros((96, D), BF16)], axis=0)
    with scope("score0"):
        score(0)
    with scope("o1"):
        A[1].from_y(2)
    with scope("y2"):
        A[2].from_z(0)
        A[2].from_y(3, 1)
    with scope("zy0"):
        A[0].from_z(3, 1)
    with scope("score1"):
        score(1)
    with scope("o2"):
        A[2].from_y(2)
    with scope("y3"):
        A[3].from_z(0)
        A[3].from_y(3, 1)
    with scope("pair_stats"):
        lax.fori_loop(0, 4, pair_stats, 0)
    with scope("zo0"):
        A[0].from_z(2)
    with scope("o3"):
        A[3].from_y(2)

    def stats0():
        for t, (l0, w, dims) in zip(T, PARTS):
            axis = NAT.index(dims[0])
            t["sc1"] = []
            for o in (1, 2, 3):
                rows = pick(st0, axis, (me[dims[0]] + o) % 4, slice(None), 3)
                t["ts1"][o - 1] = fold(rows)
        for t, (l0, w, dims) in zip(T, PARTS):
            for o in (1, 2, 3):
                t["sc1"].append(cp.remote(t["ts1"].at[o - 1], t["tr1"].at[o - 1], peer(dims[0], o)))

    def stats1():
        for t, (l0, w, dims) in zip(T, PARTS):
            for k in t["sc1"]:
                k.wait_recv()
            own = pick(st0, NAT.index(dims[0]), me[dims[0]], slice(None), 3)
            m, l, scales = merge_stats([own] + [unfold(t["tr1"][o]) for o in range(3)])
            for k, a in enumerate(scales):
                t["ax1"][k] = expand(a, l0, w)
            left = [d for d in NAT if d != dims[0]]
            axis = left.index(dims[1])
            t["st1"] = pack_stats(m, l).reshape(4, 4, 8, 128)
            stats = t["st1"]
            pieces = [(stats[i] if axis == 0 else stats[:, i]).reshape(32, 128) for i in range(4)]
            t["own1"] = choose(pieces, me[dims[1]])
            t["sc2"] = []
            for o in (1, 2, 3):
                t["ts2"][o - 1] = fold(choose(pieces, (me[dims[1]] + o) % 4))
                t["sc2"].append(cp.remote(t["ts2"].at[o - 1], t["tr2"].at[o - 1], peer(dims[1], o)))

    def choose(pieces, index):
        got = pieces[3]
        for i in (2, 1, 0):
            got = jnp.where(index == i, pieces[i], got)
        return got

    def stats2():
        for t, (l0, w, dims) in zip(T, PARTS):
            for k in t["sc2"]:
                k.wait_recv()
            m, l, scales = merge_stats([t["own1"]] + [unfold(t["tr2"][o]) for o in range(3)])
            for k, a in enumerate(scales):
                t["ax2"][k] = expand(a, l0, w)
            stats = pack_stats(m, l)
            pieces = [stats[8 * i : 8 * i + 8] for i in range(4)]
            t["own2"] = choose(pieces, me[dims[2]])
            t["sc3"] = []
            for o in (1, 2, 3):
                t["ts3"][o - 1] = choose(pieces, (me[dims[2]] + o) % 4)
                t["sc3"].append(cp.remote(t["ts3"].at[o - 1], t["tr3"].at[o - 1], peer(dims[2], o)))

    def stats3():
        for t, (l0, w, dims) in zip(T, PARTS):
            for k in t["sc3"]:
                k.wait_recv()
            m, l, scales = merge_stats([t["own2"]] + [t["tr3"][o] for o in range(3)])
            for k, a in enumerate(scales):
                t["ax3"][k] = expand(a / l, l0, w)

    def offsets(o):
        yy = (y + o) % 4
        return pl.multiple_of(yy * 128, 128), pl.multiple_of((4 + yy) * 128, 128)

    def product(j, groups, source, start, rows):
        at = pl.ds(pl.multiple_of(start, rows), rows)
        lhs = jnp.concatenate([source[at, pl.ds(a, 128)] for o in groups for a in offsets(o)], axis=1)
        rhs = jnp.concatenate([gv[j, pl.ds(a, 128), :] for o in groups for a in offsets(o)], axis=0)
        return jnp.dot(lhs, rhs, preferred_element_type=F32)

    def early(j, groups):
        def step(i, carry):
            V[pl.ds(pl.multiple_of(i * 256, 256), 256), :] = product(j, groups, mixed, i * 256, 256)
            return carry

        lax.fori_loop(0, 4, step, 0)

    def weighted(j, groups, dim, index):
        total = None
        for k in range(2):
            start = k * 512 + index * 128
            r = product(j, groups, mixed if dim == "x" else mixed_y, start, 128)
            if len(groups) < 4:
                r = r + V[pl.ds(pl.multiple_of(start, 128), 128), :]
            w = (sc[k, index] if dim == "x" else sc[k, :, :, index]).reshape(128, 128)
            r = r * expand(w, BLOCK * SEQUENCE[j], BLOCK)
            total = r if total is None else total + r
        return total

    c1 = [[] for _ in range(4)]

    def reduce1(j, groups):
        dim = PARTS[SEQUENCE[j] // 2][2][0]
        for o in (2, 1, 3):
            s1[j, o - 1] = weighted(j, groups, dim, (me[dim] + o) % 4).astype(BF16)
            c1[j].append(cp.remote(s1.at[j, o - 1], r1.at[j, o - 1], peer(dim, o)))
        own1[j] = weighted(j, groups, dim, me[dim])

    ALL = (0, 3, 1, 2)

    with scope("zy1"):
        A[1].from_z(3, 1)
    with scope("c00"):
        A[0].complete(0, 3, 1)
    with scope("early0"):
        early(0, ALL[:3])
    with scope("zo1"):
        A[1].from_z(2)
    with scope("zy2"):
        A[2].from_z(3, 1)
    with scope("c0"):
        A[0].complete(2)
    with scope("late0"):
        reduce1(0, ALL[3:])
    with scope("stats0"):
        stats0()
    with scope("B_z0"):
        B.from_z(0)
    with scope("zo2"):
        A[2].from_z(2)
    with scope("c1"):
        A[1].complete(0, 3, 1, 2)
    with scope("late1"):
        reduce1(1, ALL)
    with scope("zy3"):
        A[3].from_z(3, 1)
    with scope("zo3"):
        A[3].from_z(2)
    with scope("c2"):
        A[2].complete(0, 3, 1, 2)
    with scope("late2"):
        reduce1(2, ALL)
    with scope("B_y"):
        B.from_y(3, 1, 2)
    with scope("c3"):
        A[3].complete(0, 3, 1, 2)
    with scope("late3"):
        reduce1(3, ALL)
    with scope("stats1"):
        stats1()

    c2, c3 = [[] for _ in range(4)], [[] for _ in range(4)]

    def part_of(j):
        b = SEQUENCE[j]
        t, (l0, _, dims) = T[b // 2], PARTS[b // 2]
        return t, dims, slice(BLOCK * b - l0, BLOCK * b - l0 + BLOCK)

    def reduce2(j):
        t, dims, cols = part_of(j)
        axis = [d for d in NAT if d != dims[0]].index(dims[1])
        with scope("w_c1"):
            for k in c1[j]:
                k.wait_recv()
        total = t["ax1"][0, :, cols] * own1[j]
        for o in range(3):
            total = total + t["ax1"][o + 1, :, cols] * r1[j, o].astype(F32)
        m1[j] = total.reshape(4, 4, 8, BLOCK)
        for o in (2, 1, 3):
            s2[j, o - 1] = pick(m1.at[j], axis, (me[dims[1]] + o) % 4, slice(None), 2).astype(BF16)
        for o in (2, 1, 3):
            c2[j].append(cp.remote(s2.at[j, o - 1], r2.at[j, o - 1], peer(dims[1], o)))

    def reduce3(j):
        t, dims, cols = part_of(j)
        axis = [d for d in NAT if d != dims[0]].index(dims[1])
        with scope("w_c2"):
            for k in c2[j]:
                k.wait_recv()
        total = t["ax2"][0, :, cols] * pick(m1.at[j], axis, me[dims[1]], slice(None), 2)
        for o in range(3):
            total = total + t["ax2"][o + 1, :, cols] * r2[j, o].astype(F32)
        m2[j] = total.reshape(4, 8, BLOCK)
        for o in (2, 1, 3):
            s3[j, o - 1] = m2[j, (me[dims[2]] + o) % 4].astype(BF16)
        for o in (2, 1, 3):
            c3[j].append(cp.remote(s3.at[j, o - 1], r3.at[j, o - 1], peer(dims[2], o)))

    def result(j):
        t, dims, cols = part_of(j)
        with scope("w_c3"):
            for k in c3[j]:
                k.wait_recv()
        total = t["ax3"][0, :, cols] * m2[j, me[dims[2]]]
        for o in range(3):
            total = total + t["ax3"][o + 1, :, cols] * r3[j, o].astype(F32)
        return total

    for j in (0, 1, 2):
        reduce2(j)
    with scope("stats2"):
        stats2()
    reduce2(3)
    with scope("B_z"):
        B.from_z(3, 1, 2)
    for j in (0, 1, 2):
        reduce3(j)
    with scope("stats3"):
        stats3()
    reduce3(3)
    context = [result(j) for j in (0, 1, 2)]
    with scope("B_c"):
        B.complete(0, 3, 1, 2)
    with scope("w_sends0"):
        early_sends, cp.open = cp.open[:-6], cp.open[-6:]
        for k in early_sends:
            k.wait_send()
    context.append(result(3))
    with scope("tail"):
        context = jnp.concatenate([context[SEQUENCE.index(b)] for b in range(4)], axis=1).astype(BF16)
        out[...] = jnp.dot(context, go[...], preferred_element_type=F32).astype(BF16)
    with scope("w_sends"):
        for k in cp.open:
            k.wait_send()


def shards(tokens, var_embed, query, key_weight, value_weight, out_weight, var_slot):
    vm = pl.BlockSpec(memory_space=pltpu.VMEM)
    hbm = pl.BlockSpec(memory_space=pl.ANY)
    V = pltpu.VMEM
    part = []
    for _, w, _ in PARTS:
        part += [
            V((3, 32, 128), F32), V((3, 32, 128), F32),
            V((3, 8, 128), F32), V((3, 8, 128), F32),
            V((3, 8, 128), F32), V((3, 8, 128), F32),
            V((4, 128, w), F32), V((4, 32, w), F32), V((4, 8, w), F32),
        ]
    result = pl.pallas_call(
        kernel,
        out_shape=jax.ShapeDtypeStruct((8, D), BF16),
        in_specs=[hbm] * 7,
        out_specs=vm,
        scratch_shapes=[
            V((91, D), BF16), V((8, 128), BF16), V((1, 91), jnp.int32), V((128, D), BF16), V((2, 4, 4, 4, 8, D), BF16),
            V((1024, D), BF16), V((1024, D), BF16), V((4, D, BLOCK), BF16), V((D, D), BF16),
            V((1024, BLOCK), F32), V((4, 128, BLOCK), F32), V((4, 4, 4, 8, 128), F32),
            V((8, 128), F32), V((16, 8, 128), F32), V((128, D), BF16), V((8, D), F32), V((8, 128), F32),
            V((2, 4, 4, 4, 8, 128), F32),
            V((4, 3, 128, BLOCK), BF16), V((4, 3, 128, BLOCK), BF16),
            V((4, 3, 32, BLOCK), BF16), V((4, 3, 32, BLOCK), BF16),
            V((4, 3, 8, BLOCK), BF16), V((4, 3, 8, BLOCK), BF16),
            V((4, 4, 4, 8, BLOCK), F32), V((4, 4, 8, BLOCK), F32),
            *part,
            pltpu.SemaphoreType.DMA((SEND_SEMS,)), pltpu.SemaphoreType.DMA((SEND_SEMS,)), pltpu.SemaphoreType.DMA((12,)),
        ],
        compiler_params=pltpu.CompilerParams(
            collective_id=0, has_side_effects=True, vmem_limit_bytes=60 * 1024 * 1024
        ),
    )(
        tokens.reshape(4, 4, 4, 2, 8, D), var_embed, query.reshape(8, 128), key_weight, value_weight, out_weight,
        var_slot.reshape(1, -1),
    )
    return result.reshape(1, 8, D)


def solution(mesh):
    placed = (
        P(("vx", "vy"), None, None, None), P(), P(), P("vy", None), P("vy", None), P("vy", None), P(),
    )
    return jax.shard_map(
        shards, mesh=mesh, in_specs=placed, out_specs=P(None, ("vx", "vy"), None), check_vma=False
    )
```

```python
import contextlib
import functools

import jax
import jax.numpy as jnp
from jax import lax
from jax.experimental import pallas as pl
from jax.experimental.pallas import tpu as pltpu
from jax.sharding import PartitionSpec as P

MESH = pl.DeviceIdType.MESH
F32, BF16 = jnp.float32, jnp.bfloat16
HEADS = 16
D = 1024
BIG = -1e30

NAT = ("x", "z", "y")
PARTS = ((0, 512, ("x", "y", "z")), (512, 512, ("y", "x", "z")))
SEQUENCE = (0, 2, 1, 3)
BLOCK = 256
SEND_SEMS = 264


def scope(name):
    return contextlib.nullcontext()


def device_of(x, y, z, c):
    return (x * 2 + z // 2, (z % 2) * 8 + y * 2 + c)


class Copies:
    def __init__(self, send, recv, local):
        self.send, self.recv, self.local = send, recv, local
        self.n, self.k, self.open = 0, 0, []

    def remote(self, src, dst, device):
        copy = pltpu.make_async_remote_copy(
            src_ref=src,
            dst_ref=dst,
            send_sem=self.send.at[self.n],
            recv_sem=self.recv.at[self.n],
            device_id=device,
            device_id_type=MESH,
        )
        self.n += 1
        copy.start()
        self.open.append(copy)
        return copy

    def here(self, src, dst):
        copy = pltpu.make_async_copy(src, dst, self.local.at[self.k])
        self.k += 1
        copy.start()
        return copy


def lanes_iota(rows):
    return lax.broadcasted_iota(jnp.int32, (rows, 128), 1)


def expand(a, l0, w):
    half = lanes_iota(a.shape[0]) // 64
    tiles = [jnp.take_along_axis(a, half + 2 * t, axis=1, mode="promise_in_bounds") for t in range(l0 // 128, (l0 + w) // 128)]
    return jnp.concatenate(tiles, axis=1)


def fold(rows):
    lane = lanes_iota(rows.shape[0])
    rows = jnp.where(lane < 32, rows, 0.0)
    q = rows.shape[0] // 4
    out = rows[:q]
    for g in range(1, 4):
        out = out + pltpu.roll(rows[g * q : (g + 1) * q], 32 * g, axis=1)
    return out


def unfold(packed):
    pieces = [packed]
    for g in range(1, 4):
        pieces.append(pltpu.roll(packed, 128 - 32 * g, axis=1))
    return jnp.concatenate(pieces, axis=0)


def pack_stats(m, l):
    lane = lanes_iota(m.shape[0])
    return jnp.where(lane < 16, m, jnp.where(lane < 32, pltpu.roll(l, 16, axis=1), 0.0))


def merge_stats(stats):
    m = functools.reduce(jnp.maximum, stats)
    scales = [jnp.exp(s - m) for s in stats]
    l = sum(a * pltpu.roll(s, 112, axis=1) for a, s in zip(scales, stats))
    return m, l, scales


def pick(ref, axis, index, lanes, ndim):
    where = [slice(None)] * (ndim + 2)
    where[axis] = index
    where[-1] = lanes
    got = ref[tuple(where)]
    return got.reshape(-1, got.shape[-1])


def kernel(tok, emb_h, query_h, wk, wv, wo, vslot_h, out, emb, query, vslot, wk_v, tokv, mixed, mixed_y,
           gv, go, V, own1, st0, qk_o, qkg, qkt, er, used, sc, s1, r1, s2, r2, m1, *rest):
    ssem, rsem, lsem = rest[-3:]
    names = ("ts1", "tr1", "tr2", "ax1", "ax2", "st1")
    T = [dict(zip(names, rest[i * 6 : (i + 1) * 6])) for i in range(len(PARTS))]
    cp = Copies(ssem, rsem, lsem)

    vx, vy = lax.axis_index("vx"), lax.axis_index("vy")
    x, z = vx // 2, (vx % 2) * 2 + vy // 8
    y, c = (vy // 2) % 4, vy % 2
    zl = z % 2
    zmate = z + 1 - 2 * zl
    me = {"x": x, "y": y, "z": z}

    def peer(dim, offset):
        at = dict(me)
        at[dim] = (me[dim] + offset) % 4
        return device_of(at["x"], at["y"], at["z"], c)

    other = device_of(x, y, z, 1 - c)
    group_peers = [other, device_of(x, y, zmate, c), device_of(x, y, zmate, 1 - c)]
    for o in (1, 2, 3):
        group_peers += [device_of(x, (y + o) % 4, zz, cc) for zz in (z, zmate) for cc in (c, 1 - c)]

    def row_of(yy, zz, cc):
        return pl.multiple_of(((zz * 4 + yy) * 2 + cc) * 64, 64)

    class Gather:
        def __init__(self, g, local):
            self.g = g
            local.wait()
            self.y, self.z, self.core = {}, {}, {}

        def put(self, o, half, zz, device):
            rows = 64 if half is None else 32
            start = row_of((y + o) % 4, zz, c) + (half or 0) * 32
            ref = self.g.at[pl.ds(pl.multiple_of(start, 32), rows), :]
            return cp.remote(ref, ref, device)

        def to_y(self):
            for o in (1, 3, 2):
                self.y[4 - o] = self.put(0, None, zl, peer("y", o))

        def to_z(self, o):
            self.z[o] = [self.put(o, half, zl, peer("z", 1 + 2 * half)) for half in (0, 1)]

        def to_core(self, o, far):
            self.core.setdefault(o, []).append(self.put(o, None, 1 - zl if far else zl, other))

        def start(self):
            self.to_y()
            self.to_z(0)
            self.to_core(0, False)

        def from_y(self, *order):
            for o in order:
                self.y[o].wait_recv()
                self.to_z(o)
                self.to_core(o, False)

        def from_z(self, *order):
            for o in order:
                for k in self.z[o]:
                    k.wait_recv()
                self.to_core(o, True)

        def complete(self, *order):
            for o in order:
                for k in self.core[o]:
                    k.wait_recv()

    with scope("signals"):
        barrier = pltpu.get_barrier_semaphore()
        partners = group_peers + [peer("x", o) for o in (1, 2, 3)] + [device_of(x, y, (zmate + 2) % 4, c), peer("z", 2)]
        for p in partners:
            pl.semaphore_signal(barrier, inc=1, device_id=p, device_id_type=MESH)
    own_rows = pl.ds(row_of(y, zl, c), 64)
    load_wv = [cp.here(wv.at[:, BLOCK * b : BLOCK * b + BLOCK], gv.at[j, own_rows, :]) for j, b in enumerate(SEQUENCE)]
    load_wo = cp.here(wo, go.at[own_rows, :])
    load_wk = cp.here(wk, wk_v.at[pl.ds(0, 64), :])
    load_query = cp.here(query_h, query)
    load_slot = cp.here(vslot_h, vslot)
    load_emb = cp.here(emb_h, emb)
    load_tok = cp.here(tok.at[:, :, :, c], tokv.at[0])

    with scope("w_barrier"):
        pl.semaphore_wait(barrier, len(partners))

    with scope("gatherA"):
        A = [Gather(gv.at[0], load_wv[0])]
        A[0].start()

    head_lane = lax.broadcasted_iota(jnp.int32, (HEADS, D), 1) // 64
    head_row = lax.broadcasted_iota(jnp.int32, (HEADS, D), 0)
    own_head = head_lane == head_row
    wk_v[64:128, :] = jnp.zeros((64, D), BF16)
    load_query.wait()
    q8 = query[...].astype(F32)
    q_row = jnp.concatenate([q8[k : k + 1, :] for k in range(8)], axis=1)
    q_matrix = jnp.where(own_head, q_row, 0.0).astype(BF16)
    with scope("w_wk"):
        load_wk.wait()
    nt = (((1,), (1,)), ((), ()))
    qk = lax.dot_general(q_matrix, wk_v[...], nt, preferred_element_type=F32) * 0.125
    qk_o[...] = qk[:8] + pltpu.roll(qk[8:], 64, axis=1)

    mine = (zl * 4 + y) * 2 + c
    qk_copies = [cp.remote(qk_o, qkg.at[mine], p) for p in group_peers]
    with scope("gatherA2"):
        tok_copy = cp.remote(tok.at[:, :, :, 1 - c], tokv.at[1], other)
        for b in range(1, 4):
            A.append(Gather(gv.at[b], load_wv[b]))
            A[b].start()
        B = Gather(go, load_wo)
        B.start()

    position = vx * 16 + vy
    partner_pos = position + 1 - 2 * c
    load_slot.wait()
    n_vars = vslot.shape[1]
    row8 = lax.broadcasted_iota(jnp.int32, (8, n_vars), 0)
    slot_id = jnp.where(row8 == 0, position, jnp.where(row8 == 1, partner_pos, -1))
    match = (vslot[...] == slot_id).astype(F32)
    load_emb.wait()
    er[...] = jnp.dot(match.astype(BF16), emb[...], preferred_element_type=F32)
    used[...] = jnp.broadcast_to(jnp.sum(match, axis=1, keepdims=True), (8, 128))

    def mix(k):
        def step(i, carry):
            at = pl.ds(pl.multiple_of(k * 512 + i * 64, 64), 64)
            half = pl.ds(2 * (i % 2), 2)
            t = tokv[k, i // 2, half].astype(F32).reshape(64, D)
            mixed[at, :] = (t + er[k : k + 1, :]).astype(BF16)
            t = tokv[k, half, :, i // 2].astype(F32).reshape(64, D)
            mixed_y[at, :] = (t + er[k : k + 1, :]).astype(BF16)
            return carry

        lax.fori_loop(0, 8, step, 0)

    def score(k):
        d = lax.dot_general(mixed[k * 512 : k * 512 + 512, :], qkt[...], nt, preferred_element_type=F32)
        d = d + pltpu.roll(d, 112, axis=1)
        sc[k] = jnp.where(used[k : k + 1, :] > 0, d, BIG).reshape(4, 4, 4, 8, 128)

    def pair_stats(i, carry):
        s0, s1_ = sc[0, i].reshape(128, 128), sc[1, i].reshape(128, 128)
        m = jnp.maximum(s0, s1_)
        w0 = used[0:1, :] * jnp.exp(s0 - m)
        w1 = used[1:2, :] * jnp.exp(s1_ - m)
        st0[i] = pack_stats(m, w0 + w1).reshape(4, 4, 8, 128)
        sc[0, i] = w0.reshape(4, 4, 8, 128)
        sc[1, i] = w1.reshape(4, 4, 8, 128)
        return carry

    with scope("mix0"):
        load_tok.wait()
        mix(0)
    with scope("y0"):
        A[0].from_y(3, 1)
    with scope("z00"):
        A[0].from_z(0)
    with scope("w_tok"):
        tok_copy.wait_recv()
    with scope("mix1"):
        mix(1)
    with scope("o0"):
        A[0].from_y(2)
    with scope("z01"):
        A[1].from_z(0)
    with scope("y1"):
        A[1].from_y(3, 1)
    with scope("w_qk"):
        for k in qk_copies:
            k.wait_recv()
    with scope("qkt"):
        qkg[mine] = qk_o[...]
        left = lax.broadcasted_iota(jnp.int32, (8, 128), 1) < 64
        columns = []
        for k in range(8):
            a, b = qkg[2 * k], qkg[2 * k + 1]
            top = jnp.where(left, a, pltpu.roll(b, 64, axis=1))
            bottom = jnp.where(left, pltpu.roll(a, 64, axis=1), b)
            columns.append(jnp.concatenate([top, bottom], axis=0))
        q_keys = jnp.concatenate(columns, axis=1)
        q_high = q_keys.astype(BF16)
        q_low = (q_keys - q_high.astype(F32)).astype(BF16)
        qkt[...] = jnp.concatenate([q_high, q_low, jnp.zeros((96, D), BF16)], axis=0)
    with scope("score0"):
        score(0)
    with scope("o1"):
        A[1].from_y(2)
    with scope("y2"):
        A[2].from_z(0)
        A[2].from_y(3, 1)
    with scope("zy0"):
        A[0].from_z(3, 1)
    with scope("score1"):
        score(1)
    with scope("o2"):
        A[2].from_y(2)
    with scope("y3"):
        A[3].from_z(0)
        A[3].from_y(3, 1)
    with scope("pair_stats"):
        lax.fori_loop(0, 4, pair_stats, 0)
    with scope("zo0"):
        A[0].from_z(2)
    with scope("o3"):
        A[3].from_y(2)

    def stats0():
        for t, (l0, w, dims) in zip(T, PARTS):
            axis = NAT.index(dims[0])
            t["sc1"] = []
            for o in (1, 2, 3):
                rows = pick(st0, axis, (me[dims[0]] + o) % 4, slice(None), 3)
                t["ts1"][o - 1] = fold(rows)
        for t, (l0, w, dims) in zip(T, PARTS):
            for o in (1, 2, 3):
                t["sc1"].append(cp.remote(t["ts1"].at[o - 1], t["tr1"].at[o - 1], peer(dims[0], o)))

    plane = [(o, p) for o in range(4) for p in range(4) if o or p]

    def rest_of(dims):
        return [d for d in NAT if d != dims[0]]

    def plane_peer(dims, o, p):
        at = dict(me)
        first, second = rest_of(dims)
        at[first], at[second] = (me[first] + o) % 4, (me[second] + p) % 4
        return at[first], at[second], device_of(at["x"], at["y"], at["z"], c)

    def stats1():
        for t, (l0, w, dims) in zip(T, PARTS):
            for k in t["sc1"]:
                k.wait_recv()
            own = pick(st0, NAT.index(dims[0]), me[dims[0]], slice(None), 3)
            m, l, scales = merge_stats([own] + [unfold(t["tr1"][o]) for o in range(3)])
            t["st1"][...] = pack_stats(m, l).reshape(4, 4, 8, 128)
            for k, a in enumerate(scales):
                t["ax1"][k] = expand(a, l0, w)
        for t, (l0, w, dims) in zip(T, PARTS):
            t["sc2"] = []
            for n, (o, p) in enumerate(plane):
                i, k, device = plane_peer(dims, o, p)
                t["sc2"].append(cp.remote(t["st1"].at[i, k], t["tr2"].at[n], device))

    def stats2():
        for t, (l0, w, dims) in zip(T, PARTS):
            for k in t["sc2"]:
                k.wait_recv()
            first, second = rest_of(dims)
            m, l, scales = merge_stats([t["st1"][me[first], me[second]]] + [t["tr2"][n] for n in range(15)])
            for k, a in enumerate(scales):
                t["ax2"][k] = expand(a / l, l0, w)

    def offsets(o):
        yy = (y + o) % 4
        return pl.multiple_of(yy * 128, 128), pl.multiple_of((4 + yy) * 128, 128)

    def product(j, groups, source, start, rows):
        at = pl.ds(pl.multiple_of(start, rows), rows)
        lhs = jnp.concatenate([source[at, pl.ds(a, 128)] for o in groups for a in offsets(o)], axis=1)
        rhs = jnp.concatenate([gv[j, pl.ds(a, 128), :] for o in groups for a in offsets(o)], axis=0)
        return jnp.dot(lhs, rhs, preferred_element_type=F32)

    def early(j, groups):
        def step(i, carry):
            V[pl.ds(pl.multiple_of(i * 256, 256), 256), :] = product(j, groups, mixed, i * 256, 256)
            return carry

        lax.fori_loop(0, 4, step, 0)

    def weighted(j, groups, dim, index):
        total = None
        for k in range(2):
            start = k * 512 + index * 128
            r = product(j, groups, mixed if dim == "x" else mixed_y, start, 128)
            if len(groups) < 4:
                r = r + V[pl.ds(pl.multiple_of(start, 128), 128), :]
            w = (sc[k, index] if dim == "x" else sc[k, :, :, index]).reshape(128, 128)
            r = r * expand(w, BLOCK * SEQUENCE[j], BLOCK)
            total = r if total is None else total + r
        return total

    c1 = [[] for _ in range(4)]

    def reduce1(j, groups):
        dim = PARTS[SEQUENCE[j] // 2][2][0]
        for o in (2, 1, 3):
            s1[j, o - 1] = weighted(j, groups, dim, (me[dim] + o) % 4).astype(BF16)
            c1[j].append(cp.remote(s1.at[j, o - 1], r1.at[j, o - 1], peer(dim, o)))
        own1[j] = weighted(j, groups, dim, me[dim])

    ALL = (0, 3, 1, 2)

    with scope("zy1"):
        A[1].from_z(3, 1)
    with scope("c00"):
        A[0].complete(0, 3, 1)
    with scope("early0"):
        early(0, ALL[:3])
    with scope("zo1"):
        A[1].from_z(2)
    with scope("zy2"):
        A[2].from_z(3, 1)
    with scope("c0"):
        A[0].complete(2)
    with scope("late0"):
        reduce1(0, ALL[3:])
    with scope("stats0"):
        stats0()
    with scope("B_z0"):
        B.from_z(0)
    with scope("zo2"):
        A[2].from_z(2)
    with scope("c1"):
        A[1].complete(0, 3, 1, 2)
    with scope("late1"):
        reduce1(1, ALL)
    with scope("zy3"):
        A[3].from_z(3, 1)
    with scope("zo3"):
        A[3].from_z(2)
    with scope("c2"):
        A[2].complete(0, 3, 1, 2)
    with scope("late2"):
        reduce1(2, ALL)
    with scope("B_y"):
        B.from_y(3, 1, 2)
    with scope("c3"):
        A[3].complete(0, 3, 1, 2)
    with scope("late3"):
        reduce1(3, ALL)
    with scope("stats1"):
        stats1()

    c2 = [[] for _ in range(4)]

    def part_of(j):
        b = SEQUENCE[j]
        t, (l0, _, dims) = T[b // 2], PARTS[b // 2]
        return t, dims, slice(BLOCK * b - l0, BLOCK * b - l0 + BLOCK)

    def reduce2(j):
        t, dims, cols = part_of(j)
        with scope("w_c1"):
            for k in c1[j]:
                k.wait_recv()
        total = t["ax1"][0, :, cols] * own1[j]
        for o in range(3):
            total = total + t["ax1"][o + 1, :, cols] * r1[j, o].astype(F32)
        total = total.reshape(4, 4, 8, BLOCK)
        m1[j] = total
        s2[j] = total.astype(BF16)
        for n, (o, p) in enumerate(plane):
            i, k, device = plane_peer(dims, o, p)
            c2[j].append(cp.remote(s2.at[j, i, k], r2.at[j, n], device))

    def result(j):
        t, dims, cols = part_of(j)
        first, second = rest_of(dims)
        with scope("w_c2"):
            for k in c2[j]:
                k.wait_recv()
        total = t["ax2"][0, :, cols] * m1[j, me[first], me[second]]
        for n in range(15):
            total = total + t["ax2"][n + 1, :, cols] * r2[j, n].astype(F32)
        return total

    for j in range(4):
        reduce2(j)
    with scope("B_z"):
        B.from_z(3, 1, 2)
    with scope("stats2"):
        stats2()
    context = [result(j) for j in (0, 1, 2)]
    with scope("B_c"):
        B.complete(0, 3, 1, 2)
    with scope("w_sends0"):
        early_sends, cp.open = cp.open[:-15], cp.open[-15:]
        for k in early_sends:
            k.wait_send()
    context.append(result(3))
    with scope("tail"):
        context = jnp.concatenate([context[SEQUENCE.index(b)] for b in range(4)], axis=1).astype(BF16)
        out[...] = jnp.dot(context, go[...], preferred_element_type=F32).astype(BF16)
    with scope("w_sends"):
        for k in cp.open:
            k.wait_send()


def shards(tokens, var_embed, query, key_weight, value_weight, out_weight, var_slot):
    vm = pl.BlockSpec(memory_space=pltpu.VMEM)
    hbm = pl.BlockSpec(memory_space=pl.ANY)
    V = pltpu.VMEM
    part = []
    for _, w, _ in PARTS:
        part += [
            V((3, 32, 128), F32), V((3, 32, 128), F32), V((15, 8, 128), F32),
            V((4, 128, w), F32), V((16, 8, w), F32), V((4, 4, 8, 128), F32),
        ]
    result = pl.pallas_call(
        kernel,
        out_shape=jax.ShapeDtypeStruct((8, D), BF16),
        in_specs=[hbm] * 7,
        out_specs=vm,
        scratch_shapes=[
            V((91, D), BF16), V((8, 128), BF16), V((1, 91), jnp.int32), V((128, D), BF16), V((2, 4, 4, 4, 8, D), BF16),
            V((1024, D), BF16), V((1024, D), BF16), V((4, D, BLOCK), BF16), V((D, D), BF16),
            V((1024, BLOCK), F32), V((4, 128, BLOCK), F32), V((4, 4, 4, 8, 128), F32),
            V((8, 128), F32), V((16, 8, 128), F32), V((128, D), BF16), V((8, D), F32), V((8, 128), F32),
            V((2, 4, 4, 4, 8, 128), F32),
            V((4, 3, 128, BLOCK), BF16), V((4, 3, 128, BLOCK), BF16),
            V((4, 4, 4, 8, BLOCK), BF16), V((4, 15, 8, BLOCK), BF16), V((4, 4, 4, 8, BLOCK), F32),
            *part,
            pltpu.SemaphoreType.DMA((SEND_SEMS,)), pltpu.SemaphoreType.DMA((SEND_SEMS,)), pltpu.SemaphoreType.DMA((12,)),
        ],
        compiler_params=pltpu.CompilerParams(
            collective_id=0, has_side_effects=True, vmem_limit_bytes=60 * 1024 * 1024
        ),
    )(
        tokens.reshape(4, 4, 4, 2, 8, D), var_embed, query.reshape(8, 128), key_weight, value_weight, out_weight,
        var_slot.reshape(1, -1),
    )
    return result.reshape(1, 8, D)


def solution(mesh):
    placed = (
        P(("vx", "vy"), None, None, None), P(), P(), P("vy", None), P("vy", None), P("vy", None), P(),
    )
    return jax.shard_map(
        shards, mesh=mesh, in_specs=placed, out_specs=P(None, ("vx", "vy"), None), check_vma=False
    )
```

```python
import contextlib
import functools

import jax
import jax.numpy as jnp
from jax import lax
from jax.experimental import pallas as pl
from jax.experimental.pallas import tpu as pltpu
from jax.sharding import PartitionSpec as P

MESH = pl.DeviceIdType.MESH
F32, BF16 = jnp.float32, jnp.bfloat16
HEADS = 16
D = 1024
BIG = -1e30

NAT = ("x", "z", "y")
PARTS = ((0, 512, ("x", "y", "z")), (512, 512, ("y", "x", "z")))
SEQUENCE = (0, 2, 1, 3)
BLOCK = 256
SENDS, RECVS = 13, 54


def scope(name):
    return contextlib.nullcontext()


def device_of(x, y, z, c):
    return (x * 2 + z // 2, (z % 2) * 8 + y * 2 + c)


class Copies:
    def __init__(self, send, recv, local):
        self.sems = {"send": send, "recv": recv}
        self.local, self.k, self.used = local, 0, {"send": 0, "recv": 0}

    def new(self, side):
        self.used[side] += 1
        return self.sems[side].at[self.used[side] - 1]

    def remote(self, src, dst, device, send, recv):
        pltpu.make_async_remote_copy(
            src_ref=src, dst_ref=dst, send_sem=send, recv_sem=recv, device_id=device, device_id_type=MESH
        ).start()

    def here(self, src, dst):
        copy = pltpu.make_async_copy(src, dst, self.local.at[self.k])
        self.k += 1
        copy.start()
        return copy

    def wait(self, like, sem):
        pltpu.make_async_copy(like, like, sem).wait()


def lanes_iota(rows):
    return lax.broadcasted_iota(jnp.int32, (rows, 128), 1)


def expand(a, l0, w):
    half = lanes_iota(a.shape[0]) // 64
    tiles = [jnp.take_along_axis(a, half + 2 * t, axis=1, mode="promise_in_bounds") for t in range(l0 // 128, (l0 + w) // 128)]
    return jnp.concatenate(tiles, axis=1)


def fold(rows):
    lane = lanes_iota(rows.shape[0])
    rows = jnp.where(lane < 32, rows, 0.0)
    q = rows.shape[0] // 4
    out = rows[:q]
    for g in range(1, 4):
        out = out + pltpu.roll(rows[g * q : (g + 1) * q], 32 * g, axis=1)
    return out


def unfold(packed):
    pieces = [packed]
    for g in range(1, 4):
        pieces.append(pltpu.roll(packed, 128 - 32 * g, axis=1))
    return jnp.concatenate(pieces, axis=0)


def pack_stats(m, l):
    lane = lanes_iota(m.shape[0])
    return jnp.where(lane < 16, m, jnp.where(lane < 32, pltpu.roll(l, 16, axis=1), 0.0))


def merge_stats(stats):
    m = functools.reduce(jnp.maximum, stats)
    scales = [jnp.exp(s - m) for s in stats]
    l = sum(a * pltpu.roll(s, 112, axis=1) for a, s in zip(scales, stats))
    return m, l, scales


def pick(ref, axis, index, lanes, ndim):
    where = [slice(None)] * (ndim + 2)
    where[axis] = index
    where[-1] = lanes
    got = ref[tuple(where)]
    return got.reshape(-1, got.shape[-1])


def kernel(tok, emb_h, query_h, wk, wv, wo, vslot_h, out, emb, query, vslot, wk_v, tokv, mixed, mixed_y,
           gv, go, V, own1, st0, qk_o, qkg, qkt, er, used, sc, s1, r1, s2, r2, m1, *rest):
    ssem, rsem, lsem = rest[-3:]
    names = ("ts1", "tr1", "tr2", "ax1", "ax2", "st1", "a1")
    T = [dict(zip(names, rest[i * 7 : (i + 1) * 7])) for i in range(len(PARTS))]
    cp = Copies(ssem, rsem, lsem)

    vx, vy = lax.axis_index("vx"), lax.axis_index("vy")
    x, z = vx // 2, (vx % 2) * 2 + vy // 8
    y, c = (vy // 2) % 4, vy % 2
    zl = z % 2
    zmate = z + 1 - 2 * zl
    me = {"x": x, "y": y, "z": z}

    def peer(dim, offset):
        at = dict(me)
        at[dim] = (me[dim] + offset) % 4
        return device_of(at["x"], at["y"], at["z"], c)

    other = device_of(x, y, z, 1 - c)
    group_peers = [other, device_of(x, y, zmate, c), device_of(x, y, zmate, 1 - c)]
    for o in (1, 2, 3):
        group_peers += [device_of(x, (y + o) % 4, zz, cc) for zz in (z, zmate) for cc in (c, 1 - c)]

    def row_of(yy, zz, cc):
        return pl.multiple_of(((zz * 4 + yy) * 2 + cc) * 64, 64)

    kinds = {"own": (0,), "near": (3, 1), "far": (2,)}
    kind_of = {0: "own", 1: "near", 2: "far", 3: "near"}

    class Gather:
        def __init__(self, g, local):
            self.g = g
            local.wait()
            self.send = cp.new("send")
            self.recv = {way + kind: cp.new("recv") for way in "yzc" for kind in kinds if way + kind != "yown"}

        def put(self, o, half, zz, device, recv):
            rows = 64 if half is None else 32
            start = row_of((y + o) % 4, zz, c) + (half or 0) * 32
            ref = self.g.at[pl.ds(pl.multiple_of(start, 32), rows), :]
            cp.remote(ref, ref, device, self.send, self.recv[recv])

        def to_z(self, o):
            for half in (0, 1):
                self.put(o, half, zl, peer("z", 1 + 2 * half), "z" + kind_of[o])

        def to_core(self, o, far):
            self.put(o, None, 1 - zl if far else zl, other, "c" + kind_of[o])

        def start(self):
            for o in (1, 3, 2):
                self.put(0, None, zl, peer("y", o), "y" + kind_of[o])
            self.to_z(0)
            self.to_core(0, False)

        def wait(self, way, kind, rows):
            cp.wait(self.g.at[pl.ds(0, rows * len(kinds[kind])), :], self.recv[way + kind])

        def from_y(self, kind):
            self.wait("y", kind, 64)
            for o in kinds[kind]:
                self.to_z(o)
                self.to_core(o, False)

        def from_z(self, kind):
            self.wait("z", kind, 64)
            for o in kinds[kind]:
                self.to_core(o, True)

        def complete(self, kind):
            self.wait("c", kind, 128)

        def finish(self):
            cp.wait(self.g.at[pl.ds(0, 960), :], self.send)

    with scope("signals"):
        barrier = pltpu.get_barrier_semaphore()
        partners = group_peers + [peer("x", o) for o in (1, 2, 3)] + [device_of(x, y, (zmate + 2) % 4, c), peer("z", 2)]
        for p in partners:
            pl.semaphore_signal(barrier, inc=1, device_id=p, device_id_type=MESH)
    own_rows = pl.ds(row_of(y, zl, c), 64)
    load_wv = [cp.here(wv.at[:, BLOCK * b : BLOCK * b + BLOCK], gv.at[j, own_rows, :]) for j, b in enumerate(SEQUENCE)]
    load_wo = cp.here(wo, go.at[own_rows, :])
    load_wk = cp.here(wk, wk_v.at[pl.ds(0, 64), :])
    load_query = cp.here(query_h, query)
    load_slot = cp.here(vslot_h, vslot)
    load_emb = cp.here(emb_h, emb)
    load_tok = cp.here(tok.at[:, :, :, c], tokv.at[0])

    with scope("w_barrier"):
        pl.semaphore_wait(barrier, len(partners))

    with scope("gatherA"):
        A = [Gather(gv.at[0], load_wv[0])]
        A[0].start()

    head_lane = lax.broadcasted_iota(jnp.int32, (HEADS, D), 1) // 64
    head_row = lax.broadcasted_iota(jnp.int32, (HEADS, D), 0)
    own_head = head_lane == head_row
    wk_v[64:128, :] = jnp.zeros((64, D), BF16)
    load_query.wait()
    q8 = query[...].astype(F32)
    q_row = jnp.concatenate([q8[k : k + 1, :] for k in range(8)], axis=1)
    q_matrix = jnp.where(own_head, q_row, 0.0).astype(BF16)
    with scope("w_wk"):
        load_wk.wait()
    nt = (((1,), (1,)), ((), ()))
    qk = lax.dot_general(q_matrix, wk_v[...], nt, preferred_element_type=F32) * 0.125
    qk_o[...] = qk[:8] + pltpu.roll(qk[8:], 64, axis=1)

    mine = (zl * 4 + y) * 2 + c
    qk_send, qk_recv = cp.new("send"), cp.new("recv")
    for p in group_peers:
        cp.remote(qk_o, qkg.at[mine], p, qk_send, qk_recv)
    with scope("gatherA2"):
        tok_send, tok_recv = cp.new("send"), cp.new("recv")
        cp.remote(tok.at[:, :, :, 1 - c], tokv.at[1], other, tok_send, tok_recv)
        for b in range(1, 4):
            A.append(Gather(gv.at[b], load_wv[b]))
            A[b].start()
        B = Gather(go, load_wo)
        B.start()

    position = vx * 16 + vy
    partner_pos = position + 1 - 2 * c
    load_slot.wait()
    n_vars = vslot.shape[1]
    row8 = lax.broadcasted_iota(jnp.int32, (8, n_vars), 0)
    slot_id = jnp.where(row8 == 0, position, jnp.where(row8 == 1, partner_pos, -1))
    match = (vslot[...] == slot_id).astype(F32)
    load_emb.wait()
    er[...] = jnp.dot(match.astype(BF16), emb[...], preferred_element_type=F32)
    used[...] = jnp.broadcast_to(jnp.sum(match, axis=1, keepdims=True), (8, 128))

    def mix(k):
        def step(i, carry):
            at = pl.ds(pl.multiple_of(k * 512 + i * 64, 64), 64)
            half = pl.ds(2 * (i % 2), 2)
            t = tokv[k, i // 2, half].astype(F32).reshape(64, D)
            mixed[at, :] = (t + er[k : k + 1, :]).astype(BF16)
            t = tokv[k, half, :, i // 2].astype(F32).reshape(64, D)
            mixed_y[at, :] = (t + er[k : k + 1, :]).astype(BF16)
            return carry

        lax.fori_loop(0, 8, step, 0)

    def score(k):
        d = lax.dot_general(mixed[k * 512 : k * 512 + 512, :], qkt[...], nt, preferred_element_type=F32)
        d = d + pltpu.roll(d, 112, axis=1)
        sc[k] = jnp.where(used[k : k + 1, :] > 0, d, BIG).reshape(4, 4, 4, 8, 128)

    def pair_stats(i, carry):
        s0, s1_ = sc[0, i].reshape(128, 128), sc[1, i].reshape(128, 128)
        m = jnp.maximum(s0, s1_)
        w0 = used[0:1, :] * jnp.exp(s0 - m)
        w1 = used[1:2, :] * jnp.exp(s1_ - m)
        st0[i] = pack_stats(m, w0 + w1).reshape(4, 4, 8, 128)
        sc[0, i] = w0.reshape(4, 4, 8, 128)
        sc[1, i] = w1.reshape(4, 4, 8, 128)
        return carry

    def offsets(o):
        yy = (y + o) % 4
        return pl.multiple_of(yy * 128, 128), pl.multiple_of((4 + yy) * 128, 128)

    def product(j, groups, source, start, rows):
        at = pl.ds(pl.multiple_of(start, rows), rows)
        lhs = jnp.concatenate([source[at, pl.ds(a, 128)] for o in groups for a in offsets(o)], axis=1)
        rhs = jnp.concatenate([gv[j, pl.ds(a, 128), :] for o in groups for a in offsets(o)], axis=0)
        return jnp.dot(lhs, rhs, preferred_element_type=F32)

    def early(j, groups, fresh):
        def step(i, carry):
            at = pl.ds(pl.multiple_of(i * 256, 256), 256)
            r = product(j, groups, mixed if SEQUENCE[j] < 2 else mixed_y, i * 256, 256)
            V[j, at, :] = r if fresh else V[j, at, :] + r
            return carry

        lax.fori_loop(0, 4, step, 0)

    def first_products():
        a, b = offsets(0)

        def step(i, carry):
            at = pl.ds(pl.multiple_of(i * 512, 512), 512)
            for source, blocks in ((mixed, (0, 2)), (mixed_y, (1, 3))):
                lhs = jnp.concatenate([source[at, pl.ds(a, 128)], source[at, pl.ds(b, 128)]], axis=1)
                rhs = jnp.concatenate(
                    [jnp.concatenate([gv[j, pl.ds(a, 128), :], gv[j, pl.ds(b, 128), :]], axis=0) for j in blocks], axis=1
                )
                r = jnp.dot(lhs, rhs, preferred_element_type=F32)
                for n, j in enumerate(blocks):
                    V[j, at, :] = r[:, BLOCK * n : BLOCK * n + BLOCK]
            return carry

        lax.fori_loop(0, 2, step, 0)

    def weighted(j, groups, dim, index):
        total = None
        for k in range(2):
            start = k * 512 + index * 128
            r = product(j, groups, mixed if dim == "x" else mixed_y, start, 128)
            r = r + V[j, pl.ds(pl.multiple_of(start, 128), 128), :]
            w = (sc[k, index] if dim == "x" else sc[k, :, :, index]).reshape(128, 128)
            r = r * expand(w, BLOCK * SEQUENCE[j], BLOCK)
            total = r if total is None else total + r
        return total

    with scope("mix0"):
        load_tok.wait()
        mix(0)
    with scope("y0"):
        A[0].from_y("near")
    with scope("z00"):
        for b in range(4):
            A[b].from_z("own")
    with scope("w_tok"):
        cp.wait(tokv.at[1], tok_recv)
    with scope("mix1"):
        mix(1)
    with scope("o0"):
        A[0].from_y("far")
    with scope("g00"):
        for b in range(4):
            A[b].complete("own")
        first_products()
    with scope("y1"):
        A[1].from_y("near")
    with scope("w_qk"):
        cp.wait(qkg.at[0:15], qk_recv)
    with scope("qkt"):
        qkg[mine] = qk_o[...]
        left = lax.broadcasted_iota(jnp.int32, (8, 128), 1) < 64
        columns = []
        for k in range(8):
            a, b = qkg[2 * k], qkg[2 * k + 1]
            top = jnp.where(left, a, pltpu.roll(b, 64, axis=1))
            bottom = jnp.where(left, pltpu.roll(a, 64, axis=1), b)
            columns.append(jnp.concatenate([top, bottom], axis=0))
        q_keys = jnp.concatenate(columns, axis=1)
        q_high = q_keys.astype(BF16)
        q_low = (q_keys - q_high.astype(F32)).astype(BF16)
        qkt[...] = jnp.concatenate([q_high, q_low, jnp.zeros((96, D), BF16)], axis=0)
    with scope("score0"):
        score(0)
    with scope("o1"):
        A[1].from_y("far")
    with scope("y2"):
        A[2].from_y("near")
    with scope("score1"):
        score(1)
    with scope("o2"):
        A[2].from_y("far")
    with scope("pair_stats"):
        lax.fori_loop(0, 4, pair_stats, 0)
    with scope("y3"):
        A[3].from_y("near")
    with scope("zy0"):
        A[0].from_z("near")
    with scope("zo0"):
        A[0].from_z("far")

    def stats0():
        for t, (l0, w, dims) in zip(T, PARTS):
            axis = NAT.index(dims[0])
            for o in (1, 2, 3):
                rows = pick(st0, axis, (me[dims[0]] + o) % 4, slice(None), 3)
                t["ts1"][o - 1] = fold(rows)
        for t, (l0, w, dims) in zip(T, PARTS):
            t["send1"], t["recv1"] = cp.new("send"), cp.new("recv")
            for o in (1, 2, 3):
                cp.remote(t["ts1"].at[o - 1], t["tr1"].at[o - 1], peer(dims[0], o), t["send1"], t["recv1"])

    plane = [(o, p) for o in range(4) for p in range(4) if o or p]

    def rest_of(dims):
        return [d for d in NAT if d != dims[0]]

    def plane_peer(dims, o, p):
        at = dict(me)
        first, second = rest_of(dims)
        at[first], at[second] = (me[first] + o) % 4, (me[second] + p) % 4
        return at[first], at[second], device_of(at["x"], at["y"], at["z"], c)

    def stats1():
        for t, (l0, w, dims) in zip(T, PARTS):
            cp.wait(t["tr1"], t["recv1"])
            own = pick(st0, NAT.index(dims[0]), me[dims[0]], slice(None), 3)
            m, l, scales = merge_stats([own] + [unfold(t["tr1"][o]) for o in range(3)])
            t["st1"][...] = pack_stats(m, l).reshape(4, 4, 8, 128)
            for k, a in enumerate(scales):
                t["a1"][k] = a
        for t, (l0, w, dims) in zip(T, PARTS):
            t["send2"], t["recv2"] = cp.new("send"), cp.new("recv")
            for n, (o, p) in enumerate(plane):
                i, k, device = plane_peer(dims, o, p)
                cp.remote(t["st1"].at[i, k], t["tr2"].at[n], device, t["send2"], t["recv2"])

    def expand1():
        for t, (l0, w, dims) in zip(T, PARTS):
            for k in range(4):
                t["ax1"][k] = expand(t["a1"][k], l0, w)

    def stats2():
        for t, (l0, w, dims) in zip(T, PARTS):
            cp.wait(t["tr2"], t["recv2"])
            first, second = rest_of(dims)
            m, l, scales = merge_stats([t["st1"][me[first], me[second]]] + [t["tr2"][n] for n in range(15)])
            inverse = 1.0 / l
            for k, a in enumerate(scales):
                t["ax2"][k] = expand(a * inverse, l0, w)

    send1, recv1 = cp.new("send"), [cp.new("recv") for _ in range(4)]

    def reduce1(j, groups):
        dim = PARTS[SEQUENCE[j] // 2][2][0]
        for o in (2, 1, 3):
            s1[j, o - 1] = weighted(j, groups, dim, (me[dim] + o) % 4).astype(BF16)
            cp.remote(s1.at[j, o - 1], r1.at[j, o - 1], peer(dim, o), send1, recv1[j])
        own1[j] = weighted(j, groups, dim, me[dim])

    ALL = (0, 3, 1, 2)

    with scope("stats0"):
        stats0()
    with scope("o3"):
        A[3].from_y("far")
    with scope("zy1"):
        A[1].from_z("near")
    with scope("c00"):
        A[0].complete("near")
    with scope("early0"):
        early(0, (3, 1), False)
    with scope("zo1"):
        A[1].from_z("far")
    with scope("zy2"):
        A[2].from_z("near")
    with scope("c0"):
        A[0].complete("far")
    with scope("late0"):
        reduce1(0, (2,))
    with scope("B_z0"):
        B.from_z("own")
    with scope("zo2"):
        A[2].from_z("far")
    with scope("B_y"):
        B.from_y("near")
    with scope("c1"):
        A[1].complete("near")
        A[1].complete("far")
    with scope("late1"):
        reduce1(1, ALL[1:])
    with scope("zy3"):
        A[3].from_z("near")
    with scope("zo3"):
        A[3].from_z("far")
    with scope("c2"):
        A[2].complete("near")
        A[2].complete("far")
    with scope("late2"):
        reduce1(2, ALL[1:])
    with scope("B_o"):
        B.from_y("far")
    with scope("stats1"):
        stats1()
    with scope("c3"):
        A[3].complete("near")
        A[3].complete("far")
    with scope("late3"):
        reduce1(3, ALL[1:])
    with scope("expand1"):
        expand1()

    send2, recv2 = cp.new("send"), [cp.new("recv") for _ in range(4)]

    def part_of(j):
        b = SEQUENCE[j]
        t, (l0, _, dims) = T[b // 2], PARTS[b // 2]
        return t, dims, slice(BLOCK * b - l0, BLOCK * b - l0 + BLOCK)

    def reduce2(j):
        t, dims, cols = part_of(j)
        with scope("w_c1"):
            cp.wait(r1.at[j], recv1[j])
        total = t["ax1"][0, :, cols] * own1[j]
        for o in range(3):
            total = total + t["ax1"][o + 1, :, cols] * r1[j, o].astype(F32)
        total = total.reshape(4, 4, 8, BLOCK)
        m1[j] = total
        s2[j] = total.astype(BF16)
        for n, (o, p) in enumerate(plane):
            i, k, device = plane_peer(dims, o, p)
            cp.remote(s2.at[j, i, k], r2.at[j, n], device, send2, recv2[j])

    def result(j):
        t, dims, cols = part_of(j)
        first, second = rest_of(dims)
        with scope("w_c2"):
            cp.wait(r2.at[j], recv2[j])
        total = t["ax2"][0, :, cols] * m1[j, me[first], me[second]]
        for n in range(15):
            total = total + t["ax2"][n + 1, :, cols] * r2[j, n].astype(F32)
        return total

    for j in range(3):
        reduce2(j)
    with scope("B_z"):
        B.from_z("near")
    reduce2(3)
    with scope("stats2"):
        stats2()
    with scope("B_z2"):
        B.from_z("far")
    context = [result(j) for j in (0, 1, 2)]
    with scope("B_c"):
        for kind in kinds:
            B.complete(kind)
    with scope("w_sends0"):
        for gather in A + [B]:
            gather.finish()
        cp.wait(qkg.at[0:15], qk_send)
        cp.wait(tokv.at[1], tok_send)
        cp.wait(s1, send1)
        for t in T:
            cp.wait(t["ts1"], t["send1"])
            cp.wait(t["tr2"], t["send2"])
    context.append(result(3))
    with scope("tail"):
        context = jnp.concatenate([context[SEQUENCE.index(b)] for b in range(4)], axis=1).astype(BF16)
        out[...] = jnp.dot(context, go[...], preferred_element_type=F32).astype(BF16)
    with scope("w_sends"):
        cp.wait(r2, send2)


def shards(tokens, var_embed, query, key_weight, value_weight, out_weight, var_slot):
    vm = pl.BlockSpec(memory_space=pltpu.VMEM)
    hbm = pl.BlockSpec(memory_space=pl.ANY)
    V = pltpu.VMEM
    part = []
    for _, w, _ in PARTS:
        part += [
            V((3, 32, 128), F32), V((3, 32, 128), F32), V((15, 8, 128), F32),
            V((4, 128, w), F32), V((16, 8, w), F32), V((4, 4, 8, 128), F32), V((4, 128, 128), F32),
        ]
    result = pl.pallas_call(
        kernel,
        out_shape=jax.ShapeDtypeStruct((8, D), BF16),
        in_specs=[hbm] * 7,
        out_specs=vm,
        scratch_shapes=[
            V((91, D), BF16), V((8, 128), BF16), V((1, 91), jnp.int32), V((128, D), BF16), V((2, 4, 4, 4, 8, D), BF16),
            V((1024, D), BF16), V((1024, D), BF16), V((4, D, BLOCK), BF16), V((D, D), BF16),
            V((4, 1024, BLOCK), F32), V((4, 128, BLOCK), F32), V((4, 4, 4, 8, 128), F32),
            V((8, 128), F32), V((16, 8, 128), F32), V((128, D), BF16), V((8, D), F32), V((8, 128), F32),
            V((2, 4, 4, 4, 8, 128), F32),
            V((4, 3, 128, BLOCK), BF16), V((4, 3, 128, BLOCK), BF16),
            V((4, 4, 4, 8, BLOCK), BF16), V((4, 15, 8, BLOCK), BF16), V((4, 4, 4, 8, BLOCK), F32),
            *part,
            pltpu.SemaphoreType.DMA((SENDS,)), pltpu.SemaphoreType.DMA((RECVS,)), pltpu.SemaphoreType.DMA((10,)),
        ],
        compiler_params=pltpu.CompilerParams(
            collective_id=0, has_side_effects=True, vmem_limit_bytes=60 * 1024 * 1024
        ),
    )(
        tokens.reshape(4, 4, 4, 2, 8, D), var_embed, query.reshape(8, 128), key_weight, value_weight, out_weight,
        var_slot.reshape(1, -1),
    )
    return result.reshape(1, 8, D)


def solution(mesh):
    placed = (
        P(("vx", "vy"), None, None, None), P(), P(), P("vy", None), P("vy", None), P("vy", None), P(),
    )
    return jax.shard_map(
        shards, mesh=mesh, in_specs=placed, out_specs=P(None, ("vx", "vy"), None), check_vma=False
    )
```

```python
import contextlib
import functools

import jax
import jax.numpy as jnp
from jax import lax
from jax.experimental import pallas as pl
from jax.experimental.pallas import tpu as pltpu
from jax.sharding import PartitionSpec as P

MESH = pl.DeviceIdType.MESH
F32, BF16 = jnp.float32, jnp.bfloat16
HEADS = 16
D = 1024
BIG = -1e30

NAT = ("x", "z", "y")
PARTS = ((0, 512, ("x", "y", "z")), (512, 512, ("y", "x", "z")))
SEQUENCE = (0, 2, 1, 3)
BLOCK = 256
SENDS, RECVS = 13, 49


def scope(name):
    return contextlib.nullcontext()


def device_of(x, y, z, c):
    return (x * 2 + z // 2, (z % 2) * 8 + y * 2 + c)


class Copies:
    def __init__(self, send, recv, local):
        self.sems = {"send": send, "recv": recv}
        self.local, self.k, self.used = local, 0, {"send": 0, "recv": 0}

    def new(self, side):
        self.used[side] += 1
        return self.sems[side].at[self.used[side] - 1]

    def remote(self, src, dst, device, send, recv):
        pltpu.make_async_remote_copy(
            src_ref=src, dst_ref=dst, send_sem=send, recv_sem=recv, device_id=device, device_id_type=MESH
        ).start()

    def here(self, src, dst):
        copy = pltpu.make_async_copy(src, dst, self.local.at[self.k])
        self.k += 1
        copy.start()
        return copy

    def wait(self, like, sem):
        pltpu.make_async_copy(like, like, sem).wait()


def lanes_iota(rows):
    return lax.broadcasted_iota(jnp.int32, (rows, 128), 1)


def expand(a, l0, w):
    half = lanes_iota(a.shape[0]) // 64
    tiles = [jnp.take_along_axis(a, half + 2 * t, axis=1, mode="promise_in_bounds") for t in range(l0 // 128, (l0 + w) // 128)]
    return jnp.concatenate(tiles, axis=1)


def fold(rows):
    lane = lanes_iota(rows.shape[0])
    rows = jnp.where(lane < 32, rows, 0.0)
    q = rows.shape[0] // 4
    out = rows[:q]
    for g in range(1, 4):
        out = out + pltpu.roll(rows[g * q : (g + 1) * q], 32 * g, axis=1)
    return out


def unfold(packed):
    pieces = [packed]
    for g in range(1, 4):
        pieces.append(pltpu.roll(packed, 128 - 32 * g, axis=1))
    return jnp.concatenate(pieces, axis=0)


def pack_stats(m, l):
    lane = lanes_iota(m.shape[0])
    return jnp.where(lane < 16, m, jnp.where(lane < 32, pltpu.roll(l, 16, axis=1), 0.0))


def merge_stats(stats):
    m = functools.reduce(jnp.maximum, stats)
    scales = [jnp.exp(s - m) for s in stats]
    l = sum(a * pltpu.roll(s, 112, axis=1) for a, s in zip(scales, stats))
    return m, l, scales


def pick(ref, axis, index, lanes, ndim):
    where = [slice(None)] * (ndim + 2)
    where[axis] = index
    where[-1] = lanes
    got = ref[tuple(where)]
    return got.reshape(-1, got.shape[-1])


def kernel(tok, emb_h, query_h, wk, wv, wo, vslot_h, out, emb, query, vslot, wk_v, tokv, mixed, mixed_y,
           gv, go, V, own1, st0, qk_o, qkg, qkt, er, used, sc, s1, r1, s2, r2, m1, *rest):
    ssem, rsem, lsem = rest[-3:]
    names = ("ts1", "tr1", "tr2", "ax1", "ax2", "st1", "a1")
    T = [dict(zip(names, rest[i * 7 : (i + 1) * 7])) for i in range(len(PARTS))]
    cp = Copies(ssem, rsem, lsem)

    vx, vy = lax.axis_index("vx"), lax.axis_index("vy")
    x, z = vx // 2, (vx % 2) * 2 + vy // 8
    y, c = (vy // 2) % 4, vy % 2
    zl = z % 2
    zmate = z + 1 - 2 * zl
    me = {"x": x, "y": y, "z": z}

    def peer(dim, offset):
        at = dict(me)
        at[dim] = (me[dim] + offset) % 4
        return device_of(at["x"], at["y"], at["z"], c)

    other = device_of(x, y, z, 1 - c)
    group_peers = [other, device_of(x, y, zmate, c), device_of(x, y, zmate, 1 - c)]
    for o in (1, 2, 3):
        group_peers += [device_of(x, (y + o) % 4, zz, cc) for zz in (z, zmate) for cc in (c, 1 - c)]

    def row_of(yy, zz, cc):
        return pl.multiple_of(((zz * 4 + yy) * 2 + cc) * 64, 64)

    kinds = {"own": (0,), "near": (3, 1), "far": (2,)}
    kind_of = {0: "own", 1: "near", 2: "far", 3: "near"}

    class Gather:
        def __init__(self, g, local):
            self.g = g
            local.wait()
            self.send = cp.new("send")
            self.recv = {name: cp.new("recv") for name in ("ynear", "yfar", "zown", "znear", "zfar", "same", "cross")}

        def put(self, o, half, zz, device, recv):
            rows = 64 if half is None else 32
            start = row_of((y + o) % 4, zz, c) + (half or 0) * 32
            ref = self.g.at[pl.ds(pl.multiple_of(start, 32), rows), :]
            cp.remote(ref, ref, device, self.send, self.recv[recv])

        def to_z(self, o):
            for half in (0, 1):
                self.put(o, half, zl, peer("z", 1 + 2 * half), "z" + kind_of[o])

        def to_core(self, o, far):
            self.put(o, None, 1 - zl if far else zl, other, "cross" if far else "same")

        def to_y(self, *order):
            for o in order:
                self.put(0, None, zl, peer("y", o), "y" + kind_of[o])

        def start(self, *order):
            self.to_y(*order)
            self.to_z(0)
            self.to_core(0, False)

        def wait(self, way, kind, rows):
            cp.wait(self.g.at[pl.ds(0, rows * len(kinds[kind])), :], self.recv[way + kind])

        def from_y(self, kind):
            self.wait("y", kind, 64)
            for o in kinds[kind]:
                self.to_z(o)
                self.to_core(o, False)

        def from_z(self, kind):
            self.wait("z", kind, 64)
            for o in kinds[kind]:
                self.to_core(o, True)

        def complete(self, half):
            cp.wait(self.g.at[0:256, :], self.recv[half])

        def finish(self):
            cp.wait(self.g.at[pl.ds(0, 960), :], self.send)

    with scope("signals"):
        barrier = pltpu.get_barrier_semaphore()
        partners = group_peers + [peer("x", o) for o in (1, 2, 3)] + [device_of(x, y, (zmate + 2) % 4, c), peer("z", 2)]
        for p in partners:
            pl.semaphore_signal(barrier, inc=1, device_id=p, device_id_type=MESH)
    own_rows = pl.ds(row_of(y, zl, c), 64)
    load_wv = [cp.here(wv.at[:, BLOCK * b : BLOCK * b + BLOCK], gv.at[j, own_rows, :]) for j, b in enumerate(SEQUENCE)]
    load_wo = cp.here(wo, go.at[own_rows, :])
    load_wk = cp.here(wk, wk_v.at[pl.ds(0, 64), :])
    load_query = cp.here(query_h, query)
    load_slot = cp.here(vslot_h, vslot)
    load_emb = cp.here(emb_h, emb)
    load_tok = cp.here(tok.at[:, :, :, c], tokv.at[0])

    with scope("w_barrier"):
        pl.semaphore_wait(barrier, len(partners))

    with scope("gatherA"):
        A = [Gather(gv.at[0], load_wv[0])]
        A[0].start(1, 3, 2)

    head_lane = lax.broadcasted_iota(jnp.int32, (HEADS, D), 1) // 64
    head_row = lax.broadcasted_iota(jnp.int32, (HEADS, D), 0)
    own_head = head_lane == head_row
    wk_v[64:128, :] = jnp.zeros((64, D), BF16)
    load_query.wait()
    q8 = query[...].astype(F32)
    q_row = jnp.concatenate([q8[k : k + 1, :] for k in range(8)], axis=1)
    q_matrix = jnp.where(own_head, q_row, 0.0).astype(BF16)
    with scope("w_wk"):
        load_wk.wait()
    nt = (((1,), (1,)), ((), ()))
    qk = lax.dot_general(q_matrix, wk_v[...], nt, preferred_element_type=F32) * 0.125
    qk_o[...] = qk[:8] + pltpu.roll(qk[8:], 64, axis=1)

    mine = (zl * 4 + y) * 2 + c
    qk_send, qk_recv = cp.new("send"), cp.new("recv")
    for p in group_peers:
        cp.remote(qk_o, qkg.at[mine], p, qk_send, qk_recv)
    with scope("gatherA2"):
        tok_send, tok_recv = cp.new("send"), cp.new("recv")
        cp.remote(tok.at[:, :, :, 1 - c], tokv.at[1], other, tok_send, tok_recv)
        for b in range(1, 4):
            A.append(Gather(gv.at[b], load_wv[b]))
            A[b].start(1, 3, 2)
        B = Gather(go, load_wo)
        B.start(1, 3)

    position = vx * 16 + vy
    partner_pos = position + 1 - 2 * c
    load_slot.wait()
    n_vars = vslot.shape[1]
    row8 = lax.broadcasted_iota(jnp.int32, (8, n_vars), 0)
    slot_id = jnp.where(row8 == 0, position, jnp.where(row8 == 1, partner_pos, -1))
    match = (vslot[...] == slot_id).astype(F32)
    load_emb.wait()
    er[...] = jnp.dot(match.astype(BF16), emb[...], preferred_element_type=F32)
    used[...] = jnp.broadcast_to(jnp.sum(match, axis=1, keepdims=True), (8, 128))

    def mix(k):
        def step(i, carry):
            at = pl.ds(pl.multiple_of(k * 512 + i * 64, 64), 64)
            half = pl.ds(2 * (i % 2), 2)
            t = tokv[k, i // 2, half].astype(F32).reshape(64, D)
            mixed[at, :] = (t + er[k : k + 1, :]).astype(BF16)
            t = tokv[k, half, :, i // 2].astype(F32).reshape(64, D)
            mixed_y[at, :] = (t + er[k : k + 1, :]).astype(BF16)
            return carry

        lax.fori_loop(0, 8, step, 0)

    def score(k):
        d = lax.dot_general(mixed[k * 512 : k * 512 + 512, :], qkt[...], nt, preferred_element_type=F32)
        d = d + pltpu.roll(d, 112, axis=1)
        sc[k] = jnp.where(used[k : k + 1, :] > 0, d, BIG).reshape(4, 4, 4, 8, 128)

    def pair_stats(i, carry):
        s0, s1_ = sc[0, i].reshape(128, 128), sc[1, i].reshape(128, 128)
        m = jnp.maximum(s0, s1_)
        w0 = used[0:1, :] * jnp.exp(s0 - m)
        w1 = used[1:2, :] * jnp.exp(s1_ - m)
        st0[i] = pack_stats(m, w0 + w1).reshape(4, 4, 8, 128)
        sc[0, i] = w0.reshape(4, 4, 8, 128)
        sc[1, i] = w1.reshape(4, 4, 8, 128)
        return carry

    def product(j, half, source, start, rows):
        at = pl.ds(pl.multiple_of(start, rows), rows)
        features = pl.ds(pl.multiple_of(half * 512, 512), 512)
        return jnp.dot(source[at, features], gv[j, features, :], preferred_element_type=F32)

    def early(j):
        def step(i, carry):
            at = pl.ds(pl.multiple_of(i * 512, 512), 512)
            V[j, at, :] = product(j, zl, mixed if SEQUENCE[j] < 2 else mixed_y, i * 512, 512)
            return carry

        lax.fori_loop(0, 2, step, 0)

    def weighted(j, dim, index):
        total = None
        for k in range(2):
            start = k * 512 + index * 128
            r = product(j, 1 - zl, mixed if dim == "x" else mixed_y, start, 128)
            r = r + V[j, pl.ds(pl.multiple_of(start, 128), 128), :]
            w = (sc[k, index] if dim == "x" else sc[k, :, :, index]).reshape(128, 128)
            r = r * expand(w, BLOCK * SEQUENCE[j], BLOCK)
            total = r if total is None else total + r
        return total

    with scope("mix0"):
        load_tok.wait()
        mix(0)
    with scope("y0"):
        A[0].from_y("near")
    with scope("w_tok"):
        cp.wait(tokv.at[1], tok_recv)
    with scope("mix1"):
        mix(1)
    with scope("o0"):
        A[0].from_y("far")
    with scope("z00"):
        A[0].from_z("own")
    with scope("y1"):
        A[1].from_y("near")
        A[1].from_z("own")
    with scope("w_qk"):
        cp.wait(qkg.at[0:15], qk_recv)
    with scope("qkt"):
        qkg[mine] = qk_o[...]
        left = lax.broadcasted_iota(jnp.int32, (8, 128), 1) < 64
        columns = []
        for k in range(8):
            a, b = qkg[2 * k], qkg[2 * k + 1]
            top = jnp.where(left, a, pltpu.roll(b, 64, axis=1))
            bottom = jnp.where(left, pltpu.roll(a, 64, axis=1), b)
            columns.append(jnp.concatenate([top, bottom], axis=0))
        q_keys = jnp.concatenate(columns, axis=1)
        q_high = q_keys.astype(BF16)
        q_low = (q_keys - q_high.astype(F32)).astype(BF16)
        qkt[...] = jnp.concatenate([q_high, q_low, jnp.zeros((96, D), BF16)], axis=0)
    with scope("score0"):
        score(0)
    with scope("o1"):
        A[1].from_y("far")
    with scope("s0"):
        A[0].complete("same")
    with scope("early0"):
        early(0)
    with scope("y2"):
        A[2].from_y("near")
        A[2].from_z("own")
    with scope("score1"):
        score(1)
    with scope("o2"):
        A[2].from_y("far")
    with scope("pair_stats"):
        lax.fori_loop(0, 4, pair_stats, 0)
    with scope("y3"):
        A[3].from_y("near")
        A[3].from_z("own")
    with scope("zy0"):
        A[0].from_z("near")
    with scope("zo0"):
        A[0].from_z("far")

    def stats0():
        for t, (l0, w, dims) in zip(T, PARTS):
            axis = NAT.index(dims[0])
            for o in (1, 2, 3):
                rows = pick(st0, axis, (me[dims[0]] + o) % 4, slice(None), 3)
                t["ts1"][o - 1] = fold(rows)
        for t, (l0, w, dims) in zip(T, PARTS):
            t["send1"], t["recv1"] = cp.new("send"), cp.new("recv")
            for o in (1, 2, 3):
                cp.remote(t["ts1"].at[o - 1], t["tr1"].at[o - 1], peer(dims[0], o), t["send1"], t["recv1"])

    plane = [(o, p) for o in range(4) for p in range(4) if o or p]

    def rest_of(dims):
        return [d for d in NAT if d != dims[0]]

    def plane_peer(dims, o, p):
        at = dict(me)
        first, second = rest_of(dims)
        at[first], at[second] = (me[first] + o) % 4, (me[second] + p) % 4
        return at[first], at[second], device_of(at["x"], at["y"], at["z"], c)

    def stats1():
        for t, (l0, w, dims) in zip(T, PARTS):
            cp.wait(t["tr1"], t["recv1"])
            own = pick(st0, NAT.index(dims[0]), me[dims[0]], slice(None), 3)
            m, l, scales = merge_stats([own] + [unfold(t["tr1"][o]) for o in range(3)])
            t["st1"][...] = pack_stats(m, l).reshape(4, 4, 8, 128)
            for k, a in enumerate(scales):
                t["a1"][k] = a
        for t, (l0, w, dims) in zip(T, PARTS):
            t["send2"], t["recv2"] = cp.new("send"), cp.new("recv")
            for n, (o, p) in enumerate(plane):
                i, k, device = plane_peer(dims, o, p)
                cp.remote(t["st1"].at[i, k], t["tr2"].at[n], device, t["send2"], t["recv2"])

    def expand1():
        for t, (l0, w, dims) in zip(T, PARTS):
            for k in range(4):
                t["ax1"][k] = expand(t["a1"][k], l0, w)

    def stats2():
        for t, (l0, w, dims) in zip(T, PARTS):
            cp.wait(t["tr2"], t["recv2"])
            first, second = rest_of(dims)
            m, l, scales = merge_stats([t["st1"][me[first], me[second]]] + [t["tr2"][n] for n in range(15)])
            inverse = 1.0 / l
            for k, a in enumerate(scales):
                t["ax2"][k] = expand(a * inverse, l0, w)

    send1, recv1 = cp.new("send"), [cp.new("recv") for _ in range(4)]

    def reduce1(j):
        dim = PARTS[SEQUENCE[j] // 2][2][0]

        def send(*offsets):
            for o in offsets:
                cp.remote(s1.at[j, o - 1], r1.at[j, o - 1], peer(dim, o), send1, recv1[j])

        for o in (2, 1):
            s1[j, o - 1] = weighted(j, dim, (me[dim] + o) % 4).astype(BF16)
        if j == 3:
            send(2, 1)
        s1[j, 2] = weighted(j, dim, (me[dim] + 3) % 4).astype(BF16)
        own1[j] = weighted(j, dim, me[dim])
        if j == 3:
            send(3)
        else:
            send(2, 1, 3)

    with scope("stats0"):
        stats0()
        B.to_y(2)
    with scope("s1"):
        A[1].complete("same")
    with scope("early1"):
        early(1)
    with scope("o3"):
        A[3].from_y("far")
    with scope("zy1"):
        A[1].from_z("near")
    with scope("s2"):
        A[2].complete("same")
    with scope("early2"):
        early(2)
    with scope("zo1"):
        A[1].from_z("far")
    with scope("c0"):
        A[0].complete("cross")
    with scope("late0"):
        reduce1(0)
    with scope("zy2"):
        A[2].from_z("near")
    with scope("s3"):
        A[3].complete("same")
    with scope("early3"):
        early(3)
    with scope("zo2"):
        A[2].from_z("far")
    with scope("c1"):
        A[1].complete("cross")
    with scope("late1"):
        reduce1(1)
    with scope("zy3"):
        A[3].from_z("near")
    with scope("B_y"):
        B.from_z("own")
        B.from_y("near")
    with scope("c2"):
        A[2].complete("cross")
    with scope("late2"):
        reduce1(2)
    with scope("zo3"):
        A[3].from_z("far")
    with scope("stats1"):
        stats1()
    with scope("c3"):
        A[3].complete("cross")
    with scope("late3"):
        reduce1(3)
    with scope("B_o"):
        B.from_y("far")
    with scope("expand1"):
        expand1()

    send2, recv2 = cp.new("send"), [cp.new("recv") for _ in range(4)]

    def part_of(j):
        b = SEQUENCE[j]
        t, (l0, _, dims) = T[b // 2], PARTS[b // 2]
        return t, dims, slice(BLOCK * b - l0, BLOCK * b - l0 + BLOCK)

    def reduce2(j):
        t, dims, cols = part_of(j)
        with scope("w_c1"):
            cp.wait(r1.at[j], recv1[j])
        total = t["ax1"][0, :, cols] * own1[j]
        for o in range(3):
            total = total + t["ax1"][o + 1, :, cols] * r1[j, o].astype(F32)
        total = total.reshape(4, 4, 8, BLOCK)
        m1[j] = total
        s2[j] = total.astype(BF16)
        for n, (o, p) in enumerate(plane):
            i, k, device = plane_peer(dims, o, p)
            cp.remote(s2.at[j, i, k], r2.at[j, n], device, send2, recv2[j])

    def result(j):
        t, dims, cols = part_of(j)
        first, second = rest_of(dims)
        with scope("w_c2"):
            cp.wait(r2.at[j], recv2[j])
        total = t["ax2"][0, :, cols] * m1[j, me[first], me[second]]
        for n in range(15):
            total = total + t["ax2"][n + 1, :, cols] * r2[j, n].astype(F32)
        return total

    for j in range(3):
        reduce2(j)
    with scope("B_z"):
        B.from_z("near")
    reduce2(3)
    with scope("stats2"):
        stats2()
    with scope("B_z2"):
        B.from_z("far")
    context = [result(j) for j in (0, 1, 2)]
    with scope("B_c"):
        B.complete("same")
        B.complete("cross")
    with scope("w_sends0"):
        for gather in A + [B]:
            gather.finish()
        cp.wait(qkg.at[0:15], qk_send)
        cp.wait(tokv.at[1], tok_send)
        cp.wait(s1, send1)
        for t in T:
            cp.wait(t["ts1"], t["send1"])
            cp.wait(t["tr2"], t["send2"])
    context.append(result(3))
    with scope("tail"):
        context = jnp.concatenate([context[SEQUENCE.index(b)] for b in range(4)], axis=1).astype(BF16)
        out[...] = jnp.dot(context, go[...], preferred_element_type=F32).astype(BF16)
    with scope("w_sends"):
        cp.wait(r2, send2)


def shards(tokens, var_embed, query, key_weight, value_weight, out_weight, var_slot):
    vm = pl.BlockSpec(memory_space=pltpu.VMEM)
    hbm = pl.BlockSpec(memory_space=pl.ANY)
    V = pltpu.VMEM
    part = []
    for _, w, _ in PARTS:
        part += [
            V((3, 32, 128), F32), V((3, 32, 128), F32), V((15, 8, 128), F32),
            V((4, 128, w), F32), V((16, 8, w), F32), V((4, 4, 8, 128), F32), V((4, 128, 128), F32),
        ]
    result = pl.pallas_call(
        kernel,
        out_shape=jax.ShapeDtypeStruct((8, D), BF16),
        in_specs=[hbm] * 7,
        out_specs=vm,
        scratch_shapes=[
            V((91, D), BF16), V((8, 128), BF16), V((1, 91), jnp.int32), V((128, D), BF16), V((2, 4, 4, 4, 8, D), BF16),
            V((1024, D), BF16), V((1024, D), BF16), V((4, D, BLOCK), BF16), V((D, D), BF16),
            V((4, 1024, BLOCK), F32), V((4, 128, BLOCK), F32), V((4, 4, 4, 8, 128), F32),
            V((8, 128), F32), V((16, 8, 128), F32), V((128, D), BF16), V((8, D), F32), V((8, 128), F32),
            V((2, 4, 4, 4, 8, 128), F32),
            V((4, 3, 128, BLOCK), BF16), V((4, 3, 128, BLOCK), BF16),
            V((4, 4, 4, 8, BLOCK), BF16), V((4, 15, 8, BLOCK), BF16), V((4, 4, 4, 8, BLOCK), F32),
            *part,
            pltpu.SemaphoreType.DMA((SENDS,)), pltpu.SemaphoreType.DMA((RECVS,)), pltpu.SemaphoreType.DMA((10,)),
        ],
        compiler_params=pltpu.CompilerParams(
            collective_id=0, has_side_effects=True, vmem_limit_bytes=60 * 1024 * 1024
        ),
    )(
        tokens.reshape(4, 4, 4, 2, 8, D), var_embed, query.reshape(8, 128), key_weight, value_weight, out_weight,
        var_slot.reshape(1, -1),
    )
    return result.reshape(1, 8, D)


def solution(mesh):
    placed = (
        P(("vx", "vy"), None, None, None), P(), P(), P("vy", None), P("vy", None), P("vy", None), P(),
    )
    return jax.shard_map(
        shards, mesh=mesh, in_specs=placed, out_specs=P(None, ("vx", "vy"), None), check_vma=False
    )
```

```python
import contextlib
import functools

import jax
import jax.numpy as jnp
from jax import lax
from jax.experimental import pallas as pl
from jax.experimental.pallas import tpu as pltpu
from jax.sharding import PartitionSpec as P

MESH = pl.DeviceIdType.MESH
F32, BF16 = jnp.float32, jnp.bfloat16
HEADS = 16
D = 1024
BIG = -1e30

NAT = ("x", "z", "y")
PARTS = ((0, 512, ("x", "y", "z")), (512, 512, ("y", "x", "z")))
SEQUENCE = (0, 2, 1, 3)
BLOCK = 256
SENDS, RECVS = 13, 49


def scope(name):
    return contextlib.nullcontext()


def device_of(x, y, z, c):
    return (x * 2 + z // 2, (z % 2) * 8 + y * 2 + c)


class Copies:
    def __init__(self, send, recv, local):
        self.sems = {"send": send, "recv": recv}
        self.local, self.k, self.used = local, 0, {"send": 0, "recv": 0}

    def new(self, side):
        self.used[side] += 1
        return self.sems[side].at[self.used[side] - 1]

    def remote(self, src, dst, device, send, recv):
        pltpu.make_async_remote_copy(
            src_ref=src, dst_ref=dst, send_sem=send, recv_sem=recv, device_id=device, device_id_type=MESH
        ).start()

    def here(self, src, dst):
        copy = pltpu.make_async_copy(src, dst, self.local.at[self.k])
        self.k += 1
        copy.start()
        return copy

    def wait(self, like, sem):
        pltpu.make_async_copy(like, like, sem).wait()


def lanes_iota(rows):
    return lax.broadcasted_iota(jnp.int32, (rows, 128), 1)


def expand(a, l0, w):
    half = lanes_iota(a.shape[0]) // 64
    tiles = [jnp.take_along_axis(a, half + 2 * t, axis=1, mode="promise_in_bounds") for t in range(l0 // 128, (l0 + w) // 128)]
    return jnp.concatenate(tiles, axis=1)


def fold(rows):
    lane = lanes_iota(rows.shape[0])
    rows = jnp.where(lane < 32, rows, 0.0)
    q = rows.shape[0] // 4
    out = rows[:q]
    for g in range(1, 4):
        out = out + pltpu.roll(rows[g * q : (g + 1) * q], 32 * g, axis=1)
    return out


def unfold(packed):
    pieces = [packed]
    for g in range(1, 4):
        pieces.append(pltpu.roll(packed, 128 - 32 * g, axis=1))
    return jnp.concatenate(pieces, axis=0)


def pack_stats(m, l):
    lane = lanes_iota(m.shape[0])
    return jnp.where(lane < 16, m, jnp.where(lane < 32, pltpu.roll(l, 16, axis=1), 0.0))


def merge_stats(stats):
    m = functools.reduce(jnp.maximum, stats)
    scales = [jnp.exp(s - m) for s in stats]
    l = sum(a * pltpu.roll(s, 112, axis=1) for a, s in zip(scales, stats))
    return m, l, scales


def pick(ref, axis, index, lanes, ndim):
    where = [slice(None)] * (ndim + 2)
    where[axis] = index
    where[-1] = lanes
    got = ref[tuple(where)]
    return got.reshape(-1, got.shape[-1])


def kernel(tok, emb_h, query_h, wk, wv, wo, vslot_h, out, emb, query, vslot, wk_v, tokv, mixed, mixed_y,
           gv, go, V, own1, st0, qk_o, qkg, qkt, er, used, sc, s1, r1, s2, r2, m1, *rest):
    ssem, rsem, lsem = rest[-3:]
    names = ("ts1", "tr1", "tr2", "ax1", "ax2", "st1", "a1")
    T = [dict(zip(names, rest[i * 7 : (i + 1) * 7])) for i in range(len(PARTS))]
    cp = Copies(ssem, rsem, lsem)

    vx, vy = lax.axis_index("vx"), lax.axis_index("vy")
    x, z = vx // 2, (vx % 2) * 2 + vy // 8
    y, c = (vy // 2) % 4, vy % 2
    zl = z % 2
    zmate = z + 1 - 2 * zl
    me = {"x": x, "y": y, "z": z}

    def peer(dim, offset):
        at = dict(me)
        at[dim] = (me[dim] + offset) % 4
        return device_of(at["x"], at["y"], at["z"], c)

    other = device_of(x, y, z, 1 - c)
    group_peers = [other, device_of(x, y, zmate, c), device_of(x, y, zmate, 1 - c)]
    for o in (1, 2, 3):
        group_peers += [device_of(x, (y + o) % 4, zz, cc) for zz in (z, zmate) for cc in (c, 1 - c)]

    def row_of(yy, zz, cc):
        return pl.multiple_of(((zz * 4 + yy) * 2 + cc) * 64, 64)

    kinds = {"own": (0,), "near": (3, 1), "far": (2,)}
    kind_of = {0: "own", 1: "near", 2: "far", 3: "near"}

    class Gather:
        def __init__(self, g, local):
            self.g = g
            local.wait()
            self.send = cp.new("send")
            self.recv = {name: cp.new("recv") for name in ("ynear", "yfar", "zown", "znear", "zfar", "same", "cross")}

        def put(self, o, half, zz, device, recv):
            rows = 64 if half is None else 32
            start = row_of((y + o) % 4, zz, c) + (half or 0) * 32
            ref = self.g.at[pl.ds(pl.multiple_of(start, 32), rows), :]
            cp.remote(ref, ref, device, self.send, self.recv[recv])

        def to_z(self, o):
            for half in (0, 1):
                self.put(o, half, zl, peer("z", 1 + 2 * half), "z" + kind_of[o])

        def to_core(self, o, far):
            self.put(o, None, 1 - zl if far else zl, other, "cross" if far else "same")

        def to_y(self, *order):
            for o in order:
                self.put(0, None, zl, peer("y", o), "y" + kind_of[o])

        def start(self, *order):
            self.to_y(*order)
            self.to_z(0)
            self.to_core(0, False)

        def wait(self, way, kind, rows):
            cp.wait(self.g.at[pl.ds(0, rows * len(kinds[kind])), :], self.recv[way + kind])

        def from_y(self, kind):
            self.wait("y", kind, 64)
            for o in kinds[kind]:
                self.to_z(o)
                self.to_core(o, False)

        def from_z(self, kind):
            self.wait("z", kind, 64)
            for o in kinds[kind]:
                self.to_core(o, True)

        def complete(self, half):
            cp.wait(self.g.at[0:256, :], self.recv[half])

        def finish(self):
            cp.wait(self.g.at[pl.ds(0, 960), :], self.send)

    with scope("signals"):
        barrier = pltpu.get_barrier_semaphore()
        partners = group_peers + [peer("x", o) for o in (1, 2, 3)] + [device_of(x, y, (zmate + 2) % 4, c), peer("z", 2)]
        for p in partners:
            pl.semaphore_signal(barrier, inc=1, device_id=p, device_id_type=MESH)
    own_rows = pl.ds(row_of(y, zl, c), 64)
    load_wv = [cp.here(wv.at[:, BLOCK * b : BLOCK * b + BLOCK], gv.at[j, own_rows, :]) for j, b in enumerate(SEQUENCE)]
    load_wo = cp.here(wo, go.at[own_rows, :])
    load_wk = cp.here(wk, wk_v.at[pl.ds(0, 64), :])
    load_query = cp.here(query_h, query)
    load_slot = cp.here(vslot_h, vslot)
    load_emb = cp.here(emb_h, emb)
    load_tok = cp.here(tok.at[:, :, :, c], tokv.at[0])

    with scope("w_barrier"):
        pl.semaphore_wait(barrier, len(partners))

    with scope("gatherA"):
        A = [Gather(gv.at[0], load_wv[0])]
        A[0].start(2, 1, 3)

    head_lane = lax.broadcasted_iota(jnp.int32, (HEADS, D), 1) // 64
    head_row = lax.broadcasted_iota(jnp.int32, (HEADS, D), 0)
    own_head = head_lane == head_row
    wk_v[64:128, :] = jnp.zeros((64, D), BF16)
    load_query.wait()
    q8 = query[...].astype(F32)
    q_row = jnp.concatenate([q8[k : k + 1, :] for k in range(8)], axis=1)
    q_matrix = jnp.where(own_head, q_row, 0.0).astype(BF16)
    with scope("w_wk"):
        load_wk.wait()
    nt = (((1,), (1,)), ((), ()))
    qk = lax.dot_general(q_matrix, wk_v[...], nt, preferred_element_type=F32) * 0.125
    qk_o[...] = qk[:8] + pltpu.roll(qk[8:], 64, axis=1)

    mine = (zl * 4 + y) * 2 + c
    qk_send, qk_recv = cp.new("send"), cp.new("recv")
    for p in group_peers:
        cp.remote(qk_o, qkg.at[mine], p, qk_send, qk_recv)
    with scope("gatherA2"):
        tok_send, tok_recv = cp.new("send"), cp.new("recv")
        cp.remote(tok.at[:, :, :, 1 - c], tokv.at[1], other, tok_send, tok_recv)
        for b in range(1, 4):
            A.append(Gather(gv.at[b], load_wv[b]))
            A[b].start(2, 1, 3)
        B = Gather(go, load_wo)
        B.start(1, 3)

    position = vx * 16 + vy
    partner_pos = position + 1 - 2 * c
    load_slot.wait()
    n_vars = vslot.shape[1]
    row8 = lax.broadcasted_iota(jnp.int32, (8, n_vars), 0)
    slot_id = jnp.where(row8 == 0, position, jnp.where(row8 == 1, partner_pos, -1))
    match = (vslot[...] == slot_id).astype(F32)
    load_emb.wait()
    er[...] = jnp.dot(match.astype(BF16), emb[...], preferred_element_type=F32)
    used[...] = jnp.broadcast_to(jnp.sum(match, axis=1, keepdims=True), (8, 128))

    def mix(k):
        def step(i, carry):
            at = pl.ds(pl.multiple_of(k * 512 + i * 64, 64), 64)
            half = pl.ds(2 * (i % 2), 2)
            t = tokv[k, i // 2, half].astype(F32).reshape(64, D)
            mixed[at, :] = (t + er[k : k + 1, :]).astype(BF16)
            t = tokv[k, half, :, i // 2].astype(F32).reshape(64, D)
            mixed_y[at, :] = (t + er[k : k + 1, :]).astype(BF16)
            return carry

        lax.fori_loop(0, 8, step, 0)

    def score(k):
        d = lax.dot_general(mixed[k * 512 : k * 512 + 512, :], qkt[...], nt, preferred_element_type=F32)
        d = d + pltpu.roll(d, 112, axis=1)
        sc[k] = jnp.where(used[k : k + 1, :] > 0, d, BIG).reshape(4, 4, 4, 8, 128)

    def pair_stats(i, carry):
        s0, s1_ = sc[0, i].reshape(128, 128), sc[1, i].reshape(128, 128)
        m = jnp.maximum(s0, s1_)
        w0 = used[0:1, :] * jnp.exp(s0 - m)
        w1 = used[1:2, :] * jnp.exp(s1_ - m)
        st0[i] = pack_stats(m, w0 + w1).reshape(4, 4, 8, 128)
        sc[0, i] = w0.reshape(4, 4, 8, 128)
        sc[1, i] = w1.reshape(4, 4, 8, 128)
        return carry

    def product(j, half, source, start, rows):
        at = pl.ds(pl.multiple_of(start, rows), rows)
        features = pl.ds(pl.multiple_of(half * 512, 512), 512)
        return jnp.dot(source[at, features], gv[j, features, :], preferred_element_type=F32)

    def early(j):
        def step(i, carry):
            at = pl.ds(pl.multiple_of(i * 512, 512), 512)
            V[j, at, :] = product(j, zl, mixed if SEQUENCE[j] < 2 else mixed_y, i * 512, 512)
            return carry

        lax.fori_loop(0, 2, step, 0)

    def weighted(j, dim, index):
        total = None
        for k in range(2):
            start = k * 512 + index * 128
            r = product(j, 1 - zl, mixed if dim == "x" else mixed_y, start, 128)
            r = r + V[j, pl.ds(pl.multiple_of(start, 128), 128), :]
            w = (sc[k, index] if dim == "x" else sc[k, :, :, index]).reshape(128, 128)
            r = r * expand(w, BLOCK * SEQUENCE[j], BLOCK)
            total = r if total is None else total + r
        return total

    with scope("mix0"):
        load_tok.wait()
        mix(0)
    with scope("y0"):
        A[0].from_y("near")
    with scope("w_tok"):
        cp.wait(tokv.at[1], tok_recv)
    with scope("mix1"):
        mix(1)
    with scope("o0"):
        A[0].from_y("far")
    with scope("z00"):
        A[0].from_z("own")
    with scope("y1"):
        A[1].from_y("near")
        A[1].from_z("own")
    with scope("o1"):
        A[1].from_y("far")
    with scope("s0"):
        A[0].complete("same")
    with scope("early0"):
        early(0)
    with scope("w_qk"):
        cp.wait(qkg.at[0:15], qk_recv)
    with scope("qkt"):
        qkg[mine] = qk_o[...]
        left = lax.broadcasted_iota(jnp.int32, (8, 128), 1) < 64
        columns = []
        for k in range(8):
            a, b = qkg[2 * k], qkg[2 * k + 1]
            top = jnp.where(left, a, pltpu.roll(b, 64, axis=1))
            bottom = jnp.where(left, pltpu.roll(a, 64, axis=1), b)
            columns.append(jnp.concatenate([top, bottom], axis=0))
        q_keys = jnp.concatenate(columns, axis=1)
        q_high = q_keys.astype(BF16)
        q_low = (q_keys - q_high.astype(F32)).astype(BF16)
        qkt[...] = jnp.concatenate([q_high, q_low, jnp.zeros((96, D), BF16)], axis=0)
    with scope("score0"):
        score(0)
    with scope("y2"):
        A[2].from_y("near")
        A[2].from_z("own")
    with scope("o2"):
        A[2].from_y("far")
    with scope("zy0"):
        A[0].from_z("near")
    with scope("score1"):
        score(1)
    with scope("zo0"):
        A[0].from_z("far")
    with scope("pair_stats"):
        lax.fori_loop(0, 4, pair_stats, 0)
    with scope("y3"):
        A[3].from_y("near")
        A[3].from_z("own")
    with scope("o3"):
        A[3].from_y("far")

    def stats0():
        for t, (l0, w, dims) in zip(T, PARTS):
            axis = NAT.index(dims[0])
            for o in (1, 2, 3):
                rows = pick(st0, axis, (me[dims[0]] + o) % 4, slice(None), 3)
                t["ts1"][o - 1] = fold(rows)
        for t, (l0, w, dims) in zip(T, PARTS):
            t["send1"], t["recv1"] = cp.new("send"), cp.new("recv")
            for o in (1, 2, 3):
                cp.remote(t["ts1"].at[o - 1], t["tr1"].at[o - 1], peer(dims[0], o), t["send1"], t["recv1"])

    plane = [(o, p) for o in range(4) for p in range(4) if o or p]

    def rest_of(dims):
        return [d for d in NAT if d != dims[0]]

    def plane_peer(dims, o, p):
        at = dict(me)
        first, second = rest_of(dims)
        at[first], at[second] = (me[first] + o) % 4, (me[second] + p) % 4
        return at[first], at[second], device_of(at["x"], at["y"], at["z"], c)

    def stats1():
        for t, (l0, w, dims) in zip(T, PARTS):
            cp.wait(t["tr1"], t["recv1"])
            own = pick(st0, NAT.index(dims[0]), me[dims[0]], slice(None), 3)
            m, l, scales = merge_stats([own] + [unfold(t["tr1"][o]) for o in range(3)])
            t["st1"][...] = pack_stats(m, l).reshape(4, 4, 8, 128)
            for k, a in enumerate(scales):
                t["a1"][k] = a
        for t, (l0, w, dims) in zip(T, PARTS):
            t["send2"], t["recv2"] = cp.new("send"), cp.new("recv")
            for n, (o, p) in enumerate(plane):
                i, k, device = plane_peer(dims, o, p)
                cp.remote(t["st1"].at[i, k], t["tr2"].at[n], device, t["send2"], t["recv2"])

    def expand1():
        for t, (l0, w, dims) in zip(T, PARTS):
            for k in range(4):
                t["ax1"][k] = expand(t["a1"][k], l0, w)

    def stats2():
        for t, (l0, w, dims) in zip(T, PARTS):
            cp.wait(t["tr2"], t["recv2"])
            first, second = rest_of(dims)
            m, l, scales = merge_stats([t["st1"][me[first], me[second]]] + [t["tr2"][n] for n in range(15)])
            inverse = 1.0 / l
            for k, a in enumerate(scales):
                t["ax2"][k] = expand(a * inverse, l0, w)

    send1, recv1 = cp.new("send"), [cp.new("recv") for _ in range(4)]

    def reduce1(j):
        dim = PARTS[SEQUENCE[j] // 2][2][0]

        def send(*offsets):
            for o in offsets:
                cp.remote(s1.at[j, o - 1], r1.at[j, o - 1], peer(dim, o), send1, recv1[j])

        for o in (2, 1):
            s1[j, o - 1] = weighted(j, dim, (me[dim] + o) % 4).astype(BF16)
        if j == 3:
            send(2, 1)
        s1[j, 2] = weighted(j, dim, (me[dim] + 3) % 4).astype(BF16)
        own1[j] = weighted(j, dim, me[dim])
        if j == 3:
            send(3)
        else:
            send(2, 1, 3)

    with scope("stats0"):
        stats0()
        B.to_y(2)
    with scope("zy1"):
        A[1].from_z("near")
    with scope("s1"):
        A[1].complete("same")
    with scope("early1"):
        early(1)
    with scope("zo1"):
        A[1].from_z("far")
    with scope("c0"):
        A[0].complete("cross")
    with scope("late0"):
        reduce1(0)
    with scope("s2"):
        A[2].complete("same")
    with scope("early2"):
        early(2)
    with scope("zy2"):
        A[2].from_z("near")
    with scope("zo2"):
        A[2].from_z("far")
    with scope("c1"):
        A[1].complete("cross")
    with scope("late1"):
        reduce1(1)
    with scope("s3"):
        A[3].complete("same")
    with scope("early3"):
        early(3)
    with scope("zy3"):
        A[3].from_z("near")
    with scope("zo3"):
        A[3].from_z("far")
    with scope("c2"):
        A[2].complete("cross")
    with scope("late2"):
        reduce1(2)
    with scope("B_y"):
        B.from_z("own")
        B.from_y("near")
    with scope("c3"):
        A[3].complete("cross")
    with scope("late3"):
        reduce1(3)
    with scope("B_o"):
        B.from_y("far")
    with scope("stats1"):
        stats1()
    with scope("expand1"):
        expand1()

    send2, recv2 = cp.new("send"), [cp.new("recv") for _ in range(4)]

    def part_of(j):
        b = SEQUENCE[j]
        t, (l0, _, dims) = T[b // 2], PARTS[b // 2]
        return t, dims, slice(BLOCK * b - l0, BLOCK * b - l0 + BLOCK)

    def reduce2(j):
        t, dims, cols = part_of(j)
        with scope("w_c1"):
            cp.wait(r1.at[j], recv1[j])
        total = t["ax1"][0, :, cols] * own1[j]
        for o in range(3):
            total = total + t["ax1"][o + 1, :, cols] * r1[j, o].astype(F32)
        total = total.reshape(4, 4, 8, BLOCK)
        m1[j] = total
        s2[j] = total.astype(BF16)
        for n, (o, p) in enumerate(plane):
            i, k, device = plane_peer(dims, o, p)
            cp.remote(s2.at[j, i, k], r2.at[j, n], device, send2, recv2[j])

    def result(j):
        t, dims, cols = part_of(j)
        first, second = rest_of(dims)
        with scope("w_c2"):
            cp.wait(r2.at[j], recv2[j])
        total = t["ax2"][0, :, cols] * m1[j, me[first], me[second]]
        for n in range(15):
            total = total + t["ax2"][n + 1, :, cols] * r2[j, n].astype(F32)
        return total

    for j in range(3):
        reduce2(j)
    with scope("B_z"):
        B.from_z("near")
    reduce2(3)
    with scope("B_z2"):
        B.from_z("far")
    with scope("stats2"):
        stats2()
    context = [result(j) for j in (0, 1, 2)]
    with scope("B_c"):
        B.complete("same")
        B.complete("cross")
    with scope("w_sends0"):
        for gather in A + [B]:
            gather.finish()
        cp.wait(qkg.at[0:15], qk_send)
        cp.wait(tokv.at[1], tok_send)
        cp.wait(s1, send1)
        for t in T:
            cp.wait(t["ts1"], t["send1"])
            cp.wait(t["tr2"], t["send2"])
    context.append(result(3))
    with scope("tail"):
        context = jnp.concatenate([context[SEQUENCE.index(b)] for b in range(4)], axis=1).astype(BF16)
        out[...] = jnp.dot(context, go[...], preferred_element_type=F32).astype(BF16)
    with scope("w_sends"):
        cp.wait(r2, send2)


def shards(tokens, var_embed, query, key_weight, value_weight, out_weight, var_slot):
    vm = pl.BlockSpec(memory_space=pltpu.VMEM)
    hbm = pl.BlockSpec(memory_space=pl.ANY)
    V = pltpu.VMEM
    part = []
    for _, w, _ in PARTS:
        part += [
            V((3, 32, 128), F32), V((3, 32, 128), F32), V((15, 8, 128), F32),
            V((4, 128, w), F32), V((16, 8, w), F32), V((4, 4, 8, 128), F32), V((4, 128, 128), F32),
        ]
    result = pl.pallas_call(
        kernel,
        out_shape=jax.ShapeDtypeStruct((8, D), BF16),
        in_specs=[hbm] * 7,
        out_specs=vm,
        scratch_shapes=[
            V((91, D), BF16), V((8, 128), BF16), V((1, 91), jnp.int32), V((128, D), BF16), V((2, 4, 4, 4, 8, D), BF16),
            V((1024, D), BF16), V((1024, D), BF16), V((4, D, BLOCK), BF16), V((D, D), BF16),
            V((4, 1024, BLOCK), F32), V((4, 128, BLOCK), F32), V((4, 4, 4, 8, 128), F32),
            V((8, 128), F32), V((16, 8, 128), F32), V((128, D), BF16), V((8, D), F32), V((8, 128), F32),
            V((2, 4, 4, 4, 8, 128), F32),
            V((4, 3, 128, BLOCK), BF16), V((4, 3, 128, BLOCK), BF16),
            V((4, 4, 4, 8, BLOCK), BF16), V((4, 15, 8, BLOCK), BF16), V((4, 4, 4, 8, BLOCK), F32),
            *part,
            pltpu.SemaphoreType.DMA((SENDS,)), pltpu.SemaphoreType.DMA((RECVS,)), pltpu.SemaphoreType.DMA((10,)),
        ],
        compiler_params=pltpu.CompilerParams(
            collective_id=0, has_side_effects=True, vmem_limit_bytes=60 * 1024 * 1024
        ),
    )(
        tokens.reshape(4, 4, 4, 2, 8, D), var_embed, query.reshape(8, 128), key_weight, value_weight, out_weight,
        var_slot.reshape(1, -1),
    )
    return result.reshape(1, 8, D)


def solution(mesh):
    placed = (
        P(("vx", "vy"), None, None, None), P(), P(), P("vy", None), P("vy", None), P("vy", None), P(),
    )
    return jax.shard_map(
        shards, mesh=mesh, in_specs=placed, out_specs=P(None, ("vx", "vy"), None), check_vma=False
    )
```

```python
import contextlib
import functools

import jax
import jax.numpy as jnp
from jax import lax
from jax.experimental import pallas as pl
from jax.experimental.pallas import tpu as pltpu
from jax.sharding import PartitionSpec as P

MESH = pl.DeviceIdType.MESH
F32, BF16 = jnp.float32, jnp.bfloat16
HEADS = 16
D = 1024
BIG = -1e30

NAT = ("x", "z", "y")
PARTS = ((0, 512, ("x", "y", "z")), (512, 512, ("y", "x", "z")))
SEQUENCE = (0, 2, 1, 3)
BLOCK = 256
SENDS, RECVS = 10, 49


def scope(name):
    return contextlib.nullcontext()


def device_of(x, y, z, c):
    return (x * 2 + z // 2, (z % 2) * 8 + y * 2 + c)


class Copies:
    def __init__(self, send, recv, local):
        self.sems = {"send": send, "recv": recv}
        self.local, self.k, self.used = local, 0, {"send": 0, "recv": 0}

    def new(self, side):
        self.used[side] += 1
        return self.sems[side].at[self.used[side] - 1]

    def remote(self, src, dst, device, send, recv):
        pltpu.make_async_remote_copy(
            src_ref=src, dst_ref=dst, send_sem=send, recv_sem=recv, device_id=device, device_id_type=MESH
        ).start()

    def here(self, src, dst):
        copy = pltpu.make_async_copy(src, dst, self.local.at[self.k])
        self.k += 1
        copy.start()
        return copy

    def wait(self, like, sem):
        pltpu.make_async_copy(like, like, sem).wait()


def lanes_iota(rows):
    return lax.broadcasted_iota(jnp.int32, (rows, 128), 1)


def expand(a, l0, w):
    half = lanes_iota(a.shape[0]) // 64
    tiles = [jnp.take_along_axis(a, half + 2 * t, axis=1, mode="promise_in_bounds") for t in range(l0 // 128, (l0 + w) // 128)]
    return jnp.concatenate(tiles, axis=1)


def fold(rows):
    lane = lanes_iota(rows.shape[0])
    rows = jnp.where(lane < 32, rows, 0.0)
    q = rows.shape[0] // 4
    out = rows[:q]
    for g in range(1, 4):
        out = out + pltpu.roll(rows[g * q : (g + 1) * q], 32 * g, axis=1)
    return out


def unfold(packed):
    pieces = [packed]
    for g in range(1, 4):
        pieces.append(pltpu.roll(packed, 128 - 32 * g, axis=1))
    return jnp.concatenate(pieces, axis=0)


def pack_stats(m, l):
    lane = lanes_iota(m.shape[0])
    return jnp.where(lane < 16, m, jnp.where(lane < 32, pltpu.roll(l, 16, axis=1), 0.0))


def merge_stats(stats):
    m = functools.reduce(jnp.maximum, stats)
    scales = [jnp.exp(s - m) for s in stats]
    l = sum(a * pltpu.roll(s, 112, axis=1) for a, s in zip(scales, stats))
    return m, l, scales


def pick(ref, axis, index, lanes, ndim):
    where = [slice(None)] * (ndim + 2)
    where[axis] = index
    where[-1] = lanes
    got = ref[tuple(where)]
    return got.reshape(-1, got.shape[-1])


def kernel(tok, emb_h, query_h, wk, wv, wo, vslot_h, out, emb, query, vslot, wk_v, tokv, mixed, mixed_y,
           gv, go, V, own1, st0, qk_o, qkg, qkt, er, used, sc, s1, r1, s2, r2, m1, partial, *rest):
    ssem, rsem, lsem = rest[-3:]
    names = ("ts1", "tr1", "tr2", "ax1", "ax2", "st1", "a1")
    T = [dict(zip(names, rest[i * 7 : (i + 1) * 7])) for i in range(len(PARTS))]
    cp = Copies(ssem, rsem, lsem)

    vx, vy = lax.axis_index("vx"), lax.axis_index("vy")
    x, z = vx // 2, (vx % 2) * 2 + vy // 8
    y, c = (vy // 2) % 4, vy % 2
    zl = z % 2
    zmate = z + 1 - 2 * zl
    me = {"x": x, "y": y, "z": z}

    def peer(dim, offset):
        at = dict(me)
        at[dim] = (me[dim] + offset) % 4
        return device_of(at["x"], at["y"], at["z"], c)

    other = device_of(x, y, z, 1 - c)
    group_peers = [other, device_of(x, y, zmate, c), device_of(x, y, zmate, 1 - c)]
    for o in (1, 2, 3):
        group_peers += [device_of(x, (y + o) % 4, zz, cc) for zz in (z, zmate) for cc in (c, 1 - c)]

    def row_of(yy, zz, cc):
        return pl.multiple_of(((zz * 4 + yy) * 2 + cc) * 64, 64)

    kinds = {"own": (0,), "near": (3, 1), "far": (2,)}
    kind_of = {0: "own", 1: "near", 2: "far", 3: "near"}

    class Gather:
        def __init__(self, g, local, send):
            self.g, self.send = g, send
            local.wait()
            self.recv = {name: cp.new("recv") for name in ("ynear", "yfar", "zown", "znear", "zfar", "same", "cross")}

        def put(self, o, half, zz, device, recv):
            rows = 64 if half is None else 32
            start = row_of((y + o) % 4, zz, c) + (half or 0) * 32
            ref = self.g.at[pl.ds(pl.multiple_of(start, 32), rows), :]
            cp.remote(ref, ref, device, self.send, self.recv[recv])

        def to_z(self, o):
            for half in (0, 1):
                self.put(o, half, zl, peer("z", 1 + 2 * half), "z" + kind_of[o])

        def to_core(self, o, far):
            self.put(o, None, 1 - zl if far else zl, other, "cross" if far else "same")

        def to_y(self, *order):
            for o in order:
                self.put(0, None, zl, peer("y", o), "y" + kind_of[o])

        def start(self, *order):
            self.to_y(*order)
            self.to_z(0)
            self.to_core(0, False)

        def wait(self, way, kind, rows):
            cp.wait(self.g.at[pl.ds(0, rows * len(kinds[kind])), :], self.recv[way + kind])

        def from_y(self, kind):
            self.wait("y", kind, 64)
            for o in kinds[kind]:
                self.to_z(o)
                self.to_core(o, False)

        def from_z(self, kind):
            self.wait("z", kind, 64)
            for o in kinds[kind]:
                self.to_core(o, True)

        def complete(self, half):
            cp.wait(self.g.at[0:256, :], self.recv[half])

    with scope("signals"):
        barrier = pltpu.get_barrier_semaphore()
        partners = group_peers + [peer("x", o) for o in (1, 2, 3)] + [device_of(x, y, (zmate + 2) % 4, c), peer("z", 2)]
        for p in partners:
            pl.semaphore_signal(barrier, inc=1, device_id=p, device_id_type=MESH)
    own_rows = pl.ds(row_of(y, zl, c), 64)
    load_wv = [cp.here(wv.at[:, BLOCK * b : BLOCK * b + BLOCK], gv.at[j, own_rows, :]) for j, b in enumerate(SEQUENCE)]
    load_wo = cp.here(wo, go.at[own_rows, :])
    load_wk = cp.here(wk, wk_v.at[pl.ds(0, 64), :])
    load_query = cp.here(query_h, query)
    load_slot = cp.here(vslot_h, vslot)
    load_emb = cp.here(emb_h, emb)
    load_tok = cp.here(tok.at[:, :, :, c], tokv.at[0])

    with scope("w_barrier"):
        pl.semaphore_wait(barrier, len(partners))

    with scope("gatherA"):
        send_v, send_o = cp.new("send"), cp.new("send")
        A = [Gather(gv.at[0], load_wv[0], send_v)]
        A[0].start(2, 1, 3)

    head_lane = lax.broadcasted_iota(jnp.int32, (HEADS, D), 1) // 64
    head_row = lax.broadcasted_iota(jnp.int32, (HEADS, D), 0)
    own_head = head_lane == head_row
    wk_v[64:128, :] = jnp.zeros((64, D), BF16)
    load_query.wait()
    q8 = query[...].astype(F32)
    q_row = jnp.concatenate([q8[k : k + 1, :] for k in range(8)], axis=1)
    q_matrix = jnp.where(own_head, q_row, 0.0).astype(BF16)
    with scope("w_wk"):
        load_wk.wait()
    nt = (((1,), (1,)), ((), ()))
    qk = lax.dot_general(q_matrix, wk_v[...], nt, preferred_element_type=F32) * 0.125
    qk_o[...] = qk[:8] + pltpu.roll(qk[8:], 64, axis=1)

    mine = (zl * 4 + y) * 2 + c
    qk_send, qk_recv = cp.new("send"), cp.new("recv")
    for p in group_peers:
        cp.remote(qk_o, qkg.at[mine], p, qk_send, qk_recv)
    with scope("gatherA2"):
        tok_send, tok_recv = cp.new("send"), cp.new("recv")
        cp.remote(tok.at[:, :, :, 1 - c], tokv.at[1], other, tok_send, tok_recv)
        for b in range(1, 4):
            A.append(Gather(gv.at[b], load_wv[b], send_v))
            A[b].start(2, 1, 3)
        B = Gather(go, load_wo, send_o)
        B.start(1, 3)

    position = vx * 16 + vy
    partner_pos = position + 1 - 2 * c
    load_slot.wait()
    n_vars = vslot.shape[1]
    row8 = lax.broadcasted_iota(jnp.int32, (8, n_vars), 0)
    slot_id = jnp.where(row8 == 0, position, jnp.where(row8 == 1, partner_pos, -1))
    match = (vslot[...] == slot_id).astype(F32)
    load_emb.wait()
    er[...] = jnp.dot(match.astype(BF16), emb[...], preferred_element_type=F32)
    used[...] = jnp.broadcast_to(jnp.sum(match, axis=1, keepdims=True), (8, 128))

    def mix(k):
        def step(i, carry):
            at = pl.ds(pl.multiple_of(k * 512 + i * 64, 64), 64)
            half = pl.ds(2 * (i % 2), 2)
            t = tokv[k, i // 2, half].astype(F32).reshape(64, D)
            mixed[at, :] = (t + er[k : k + 1, :]).astype(BF16)
            t = tokv[k, half, :, i // 2].astype(F32).reshape(64, D)
            mixed_y[at, :] = (t + er[k : k + 1, :]).astype(BF16)
            return carry

        lax.fori_loop(0, 8, step, 0)

    def score(k):
        d = lax.dot_general(mixed[k * 512 : k * 512 + 512, :], qkt[...], nt, preferred_element_type=F32)
        d = d + pltpu.roll(d, 112, axis=1)
        sc[k] = jnp.where(used[k : k + 1, :] > 0, d, BIG).reshape(4, 4, 4, 8, 128)

    def pair_stats(i, carry):
        s0, s1_ = sc[0, i].reshape(128, 128), sc[1, i].reshape(128, 128)
        m = jnp.maximum(s0, s1_)
        w0 = used[0:1, :] * jnp.exp(s0 - m)
        w1 = used[1:2, :] * jnp.exp(s1_ - m)
        st0[i] = pack_stats(m, w0 + w1).reshape(4, 4, 8, 128)
        sc[0, i] = w0.reshape(4, 4, 8, 128)
        sc[1, i] = w1.reshape(4, 4, 8, 128)
        return carry

    def product(j, half, source, start, rows):
        at = pl.ds(pl.multiple_of(start, rows), rows)
        features = pl.ds(pl.multiple_of(half * 512, 512), 512)
        return jnp.dot(source[at, features], gv[j, features, :], preferred_element_type=F32)

    def early(j):
        def step(i, carry):
            at = pl.ds(pl.multiple_of(i * 512, 512), 512)
            V[j, at, :] = product(j, zl, mixed if SEQUENCE[j] < 2 else mixed_y, i * 512, 512)
            return carry

        lax.fori_loop(0, 2, step, 0)

    def weighted(j, dim, index):
        total = None
        for k in range(2):
            start = k * 512 + index * 128
            r = product(j, 1 - zl, mixed if dim == "x" else mixed_y, start, 128)
            r = r + V[j, pl.ds(pl.multiple_of(start, 128), 128), :]
            w = (sc[k, index] if dim == "x" else sc[k, :, :, index]).reshape(128, 128)
            r = r * expand(w, BLOCK * SEQUENCE[j], BLOCK)
            total = r if total is None else total + r
        return total

    with scope("mix0"):
        load_tok.wait()
        mix(0)
    with scope("y0"):
        A[0].from_y("near")
    with scope("w_tok"):
        cp.wait(tokv.at[1], tok_recv)
    with scope("mix1"):
        mix(1)
    with scope("o0"):
        A[0].from_y("far")
    with scope("z00"):
        A[0].from_z("own")
    with scope("y1"):
        A[1].from_y("near")
        A[1].from_z("own")
    with scope("o1"):
        A[1].from_y("far")
    with scope("s0"):
        A[0].complete("same")
    with scope("early0"):
        early(0)
    with scope("w_qk"):
        cp.wait(qkg.at[0:15], qk_recv)
    with scope("qkt"):
        qkg[mine] = qk_o[...]
        left = lax.broadcasted_iota(jnp.int32, (8, 128), 1) < 64
        columns = []
        for k in range(8):
            a, b = qkg[2 * k], qkg[2 * k + 1]
            top = jnp.where(left, a, pltpu.roll(b, 64, axis=1))
            bottom = jnp.where(left, pltpu.roll(a, 64, axis=1), b)
            columns.append(jnp.concatenate([top, bottom], axis=0))
        q_keys = jnp.concatenate(columns, axis=1)
        q_high = q_keys.astype(BF16)
        q_low = (q_keys - q_high.astype(F32)).astype(BF16)
        qkt[...] = jnp.concatenate([q_high, q_low, jnp.zeros((96, D), BF16)], axis=0)
    with scope("score0"):
        score(0)
    with scope("y2"):
        A[2].from_y("near")
        A[2].from_z("own")
    with scope("o2"):
        A[2].from_y("far")
    with scope("zy0"):
        A[0].from_z("near")
    with scope("score1"):
        score(1)
    with scope("zo0"):
        A[0].from_z("far")
    with scope("pair_stats"):
        lax.fori_loop(0, 4, pair_stats, 0)
    with scope("y3"):
        A[3].from_y("near")
        A[3].from_z("own")
    with scope("o3"):
        A[3].from_y("far")

    def stats0():
        for t, (l0, w, dims) in zip(T, PARTS):
            axis = NAT.index(dims[0])
            for o in (1, 2, 3):
                rows = pick(st0, axis, (me[dims[0]] + o) % 4, slice(None), 3)
                t["ts1"][o - 1] = fold(rows)
        for t, (l0, w, dims) in zip(T, PARTS):
            t["send1"], t["recv1"] = cp.new("send"), cp.new("recv")
            for o in (1, 2, 3):
                cp.remote(t["ts1"].at[o - 1], t["tr1"].at[o - 1], peer(dims[0], o), t["send1"], t["recv1"])

    plane = sorted([(o, p) for o in range(4) for p in range(4) if o or p], key=lambda q: -sum(min(k, 4 - k) for k in q))

    def rest_of(dims):
        return [d for d in NAT if d != dims[0]]

    def plane_peer(dims, o, p):
        at = dict(me)
        first, second = rest_of(dims)
        at[first], at[second] = (me[first] + o) % 4, (me[second] + p) % 4
        return at[first], at[second], device_of(at["x"], at["y"], at["z"], c)

    def stats1():
        for t, (l0, w, dims) in zip(T, PARTS):
            cp.wait(t["tr1"], t["recv1"])
            own = pick(st0, NAT.index(dims[0]), me[dims[0]], slice(None), 3)
            m, l, scales = merge_stats([own] + [unfold(t["tr1"][o]) for o in range(3)])
            t["st1"][...] = pack_stats(m, l).reshape(4, 4, 8, 128)
            for k, a in enumerate(scales):
                t["a1"][k] = a
        for t, (l0, w, dims) in zip(T, PARTS):
            t["send2"], t["recv2"] = cp.new("send"), cp.new("recv")
            for n, (o, p) in enumerate(plane):
                i, k, device = plane_peer(dims, o, p)
                cp.remote(t["st1"].at[i, k], t["tr2"].at[n], device, t["send2"], t["recv2"])

    def expand1():
        for t, (l0, w, dims) in zip(T, PARTS):
            for k in range(4):
                t["ax1"][k] = expand(t["a1"][k], l0, w)

    def stats2():
        for t, (l0, w, dims) in zip(T, PARTS):
            cp.wait(t["tr2"], t["recv2"])
            first, second = rest_of(dims)
            m, l, scales = merge_stats([t["st1"][me[first], me[second]]] + [t["tr2"][n] for n in range(15)])
            inverse = 1.0 / l
            for k, a in enumerate(scales):
                t["ax2"][k] = expand(a * inverse, l0, w)

    send1, recv1 = cp.new("send"), [cp.new("recv") for _ in range(4)]

    def reduce1(j):
        dim = PARTS[SEQUENCE[j] // 2][2][0]

        def send(*offsets):
            for o in offsets:
                cp.remote(s1.at[j, o - 1], r1.at[j, o - 1], peer(dim, o), send1, recv1[j])

        for o in (2, 1):
            s1[j, o - 1] = weighted(j, dim, (me[dim] + o) % 4).astype(BF16)
        if j == 3:
            send(2, 1)
        s1[j, 2] = weighted(j, dim, (me[dim] + 3) % 4).astype(BF16)
        own1[j] = weighted(j, dim, me[dim])
        if j == 3:
            send(3)
        else:
            send(2, 1, 3)

    with scope("stats0"):
        stats0()
        B.to_y(2)
    with scope("zy1"):
        A[1].from_z("near")
    with scope("s1"):
        A[1].complete("same")
    with scope("early1"):
        early(1)
    with scope("zo1"):
        A[1].from_z("far")
    with scope("c0"):
        A[0].complete("cross")
    with scope("late0"):
        reduce1(0)
    with scope("s2"):
        A[2].complete("same")
    with scope("early2"):
        early(2)
    with scope("zy2"):
        A[2].from_z("near")
    with scope("zo2"):
        A[2].from_z("far")
    with scope("c1"):
        A[1].complete("cross")
    with scope("late1"):
        reduce1(1)
    with scope("s3"):
        A[3].complete("same")
    with scope("early3"):
        early(3)
    with scope("zy3"):
        A[3].from_z("near")
    with scope("zo3"):
        A[3].from_z("far")
    with scope("c2"):
        A[2].complete("cross")
    with scope("late2"):
        reduce1(2)
    with scope("B_y"):
        B.from_z("own")
        B.from_y("near")
    with scope("c3"):
        A[3].complete("cross")
    with scope("late3"):
        reduce1(3)
    with scope("stats1"):
        stats1()
    with scope("B_o"):
        B.from_y("far")
    with scope("expand1"):
        expand1()

    send2, recv2 = cp.new("send"), [cp.new("recv") for _ in range(4)]

    def part_of(j):
        b = SEQUENCE[j]
        t, (l0, _, dims) = T[b // 2], PARTS[b // 2]
        return t, dims, slice(BLOCK * b - l0, BLOCK * b - l0 + BLOCK)

    def reduce2(j):
        t, dims, cols = part_of(j)
        with scope("w_c1"):
            cp.wait(r1.at[j], recv1[j])
        total = t["ax1"][0, :, cols] * own1[j]
        for o in range(3):
            total = total + t["ax1"][o + 1, :, cols] * r1[j, o].astype(F32)
        total = total.reshape(4, 4, 8, BLOCK)
        m1[j] = total
        s2[j] = total.astype(BF16)
        for n, (o, p) in enumerate(plane):
            i, k, device = plane_peer(dims, o, p)
            cp.remote(s2.at[j, i, k], r2.at[j, n], device, send2, recv2[j])

    def result(j):
        t, dims, cols = part_of(j)
        first, second = rest_of(dims)
        with scope("w_c2"):
            cp.wait(r2.at[j], recv2[j])
        total = t["ax2"][0, :, cols] * m1[j, me[first], me[second]]
        for n in range(15):
            total = total + t["ax2"][n + 1, :, cols] * r2[j, n].astype(F32)
        return total

    for j in range(3):
        reduce2(j)
    reduce2(3)
    with scope("B_z"):
        B.from_z("near")
    with scope("B_z2"):
        B.from_z("far")
    with scope("stats2"):
        stats2()
    def projected(j, context):
        rows = slice(BLOCK * SEQUENCE[j], BLOCK * SEQUENCE[j] + BLOCK)
        return jnp.dot(context.astype(BF16), go[rows, :], preferred_element_type=F32)

    context = [result(j) for j in (0, 1, 2)]
    with scope("B_c"):
        B.complete("same")
        B.complete("cross")
    with scope("tail0"):
        partial[...] = sum(projected(j, context[j]) for j in (0, 1, 2))
    with scope("w_sends0"):
        cp.wait(gv.at[:, 0:960, :], send_v)
        cp.wait(go.at[0:960, :], send_o)
        cp.wait(qkg.at[0:15], qk_send)
        cp.wait(tokv.at[1], tok_send)
        cp.wait(s1, send1)
        for t in T:
            cp.wait(t["ts1"], t["send1"])
            cp.wait(t["tr2"], t["send2"])
    last = result(3)
    with scope("tail"):
        out[...] = (partial[...] + projected(3, last)).astype(BF16)
    with scope("w_sends"):
        cp.wait(r2, send2)


def shards(tokens, var_embed, query, key_weight, value_weight, out_weight, var_slot):
    vm = pl.BlockSpec(memory_space=pltpu.VMEM)
    hbm = pl.BlockSpec(memory_space=pl.ANY)
    V = pltpu.VMEM
    part = []
    for _, w, _ in PARTS:
        part += [
            V((3, 32, 128), F32), V((3, 32, 128), F32), V((15, 8, 128), F32),
            V((4, 128, w), F32), V((16, 8, w), F32), V((4, 4, 8, 128), F32), V((4, 128, 128), F32),
        ]
    result = pl.pallas_call(
        kernel,
        out_shape=jax.ShapeDtypeStruct((8, D), BF16),
        in_specs=[hbm] * 7,
        out_specs=vm,
        scratch_shapes=[
            V((91, D), BF16), V((8, 128), BF16), V((1, 91), jnp.int32), V((128, D), BF16), V((2, 4, 4, 4, 8, D), BF16),
            V((1024, D), BF16), V((1024, D), BF16), V((4, D, BLOCK), BF16), V((D, D), BF16),
            V((4, 1024, BLOCK), F32), V((4, 128, BLOCK), F32), V((4, 4, 4, 8, 128), F32),
            V((8, 128), F32), V((16, 8, 128), F32), V((128, D), BF16), V((8, D), F32), V((8, 128), F32),
            V((2, 4, 4, 4, 8, 128), F32),
            V((4, 3, 128, BLOCK), BF16), V((4, 3, 128, BLOCK), BF16),
            V((4, 4, 4, 8, BLOCK), BF16), V((4, 15, 8, BLOCK), BF16), V((4, 4, 4, 8, BLOCK), F32),
            V((8, D), F32), *part,
            pltpu.SemaphoreType.DMA((SENDS,)), pltpu.SemaphoreType.DMA((RECVS,)), pltpu.SemaphoreType.DMA((10,)),
        ],
        compiler_params=pltpu.CompilerParams(
            collective_id=0, has_side_effects=True, vmem_limit_bytes=60 * 1024 * 1024
        ),
    )(
        tokens.reshape(4, 4, 4, 2, 8, D), var_embed, query.reshape(8, 128), key_weight, value_weight, out_weight,
        var_slot.reshape(1, -1),
    )
    return result.reshape(1, 8, D)


def solution(mesh):
    placed = (
        P(("vx", "vy"), None, None, None), P(), P(), P("vy", None), P("vy", None), P("vy", None), P(),
    )
    return jax.shard_map(
        shards, mesh=mesh, in_specs=placed, out_specs=P(None, ("vx", "vy"), None), check_vma=False
    )
```

```python
import contextlib
import functools

import jax
import jax.numpy as jnp
from jax import lax
from jax.experimental import pallas as pl
from jax.experimental.pallas import tpu as pltpu
from jax.sharding import PartitionSpec as P

MESH = pl.DeviceIdType.MESH
F32, BF16 = jnp.float32, jnp.bfloat16
HEADS = 16
D = 1024
BIG = -1e30

NAT = ("x", "z", "y")
PARTS = ((0, 512, ("x", "y", "z")), (512, 512, ("y", "x", "z")))
SEQUENCE = (0, 2, 1, 3)
BLOCK = 256
SENDS, RECVS = 10, 47


def scope(name):
    return contextlib.nullcontext()


def device_of(x, y, z, c):
    return (x * 2 + z // 2, (z % 2) * 8 + y * 2 + c)


class Copies:
    def __init__(self, send, recv, local):
        self.sems = {"send": send, "recv": recv}
        self.local, self.k, self.used = local, 0, {"send": 0, "recv": 0}

    def new(self, side):
        self.used[side] += 1
        return self.sems[side].at[self.used[side] - 1]

    def remote(self, src, dst, device, send, recv):
        pltpu.make_async_remote_copy(
            src_ref=src, dst_ref=dst, send_sem=send, recv_sem=recv, device_id=device, device_id_type=MESH
        ).start()

    def here(self, src, dst, again=False):
        self.k += 0 if again else 1
        copy = pltpu.make_async_copy(src, dst, self.local.at[self.k - 1])
        copy.start()
        return copy

    def wait(self, like, sem):
        pltpu.make_async_copy(like, like, sem).wait()


def lanes_iota(rows):
    return lax.broadcasted_iota(jnp.int32, (rows, 128), 1)


def expand(a, l0, w):
    half = lanes_iota(a.shape[0]) // 64
    tiles = [jnp.take_along_axis(a, half + 2 * t, axis=1, mode="promise_in_bounds") for t in range(l0 // 128, (l0 + w) // 128)]
    return jnp.concatenate(tiles, axis=1)


def fold(rows):
    lane = lanes_iota(rows.shape[0])
    rows = jnp.where(lane < 32, rows, 0.0)
    q = rows.shape[0] // 4
    out = rows[:q]
    for g in range(1, 4):
        out = out + pltpu.roll(rows[g * q : (g + 1) * q], 32 * g, axis=1)
    return out


def unfold(packed):
    pieces = [packed]
    for g in range(1, 4):
        pieces.append(pltpu.roll(packed, 128 - 32 * g, axis=1))
    return jnp.concatenate(pieces, axis=0)


def pack_stats(m, l):
    lane = lanes_iota(m.shape[0])
    return jnp.where(lane < 16, m, jnp.where(lane < 32, pltpu.roll(l, 16, axis=1), 0.0))


def merge_stats(stats):
    m = functools.reduce(jnp.maximum, stats)
    scales = [jnp.exp(s - m) for s in stats]
    l = sum(a * pltpu.roll(s, 112, axis=1) for a, s in zip(scales, stats))
    return m, l, scales


def pick(ref, axis, index, lanes, ndim):
    where = [slice(None)] * (ndim + 2)
    where[axis] = index
    where[-1] = lanes
    got = ref[tuple(where)]
    return got.reshape(-1, got.shape[-1])


def kernel(tok, emb_h, query_h, wk, wv, wo, vslot_h, out, emb, query, vslot, wk_v, tokv, mixed, mixed_y,
           gv, go, V, own1, st0, qk_o, qkg, qkt, er, used, sc, s1, r1, s2, r2, m1, partial, *rest):
    ssem, rsem, lsem = rest[-3:]
    names = ("ts1", "tr1", "tr2", "ax1", "ax2", "st1", "a1")
    T = [dict(zip(names, rest[i * 7 : (i + 1) * 7])) for i in range(len(PARTS))]
    cp = Copies(ssem, rsem, lsem)

    vx, vy = lax.axis_index("vx"), lax.axis_index("vy")
    x, z = vx // 2, (vx % 2) * 2 + vy // 8
    y, c = (vy // 2) % 4, vy % 2
    zl = z % 2
    zmate = z + 1 - 2 * zl
    me = {"x": x, "y": y, "z": z}

    def peer(dim, offset):
        at = dict(me)
        at[dim] = (me[dim] + offset) % 4
        return device_of(at["x"], at["y"], at["z"], c)

    other = device_of(x, y, z, 1 - c)
    group_peers = [other, device_of(x, y, zmate, c), device_of(x, y, zmate, 1 - c)]
    for o in (1, 2, 3):
        group_peers += [device_of(x, (y + o) % 4, zz, cc) for zz in (z, zmate) for cc in (c, 1 - c)]

    def row_of(yy, zz, cc):
        return pl.multiple_of(((zz * 4 + yy) * 2 + cc) * 64, 64)

    kinds = {"own": (0,), "near": (3, 1), "far": (2,)}
    kind_of = {0: "own", 1: "near", 2: "far", 3: "near"}

    class Gather:
        def __init__(self, g, local, send):
            self.g, self.send = g, send
            if local is not None:
                local.wait()
            self.recv = {name: cp.new("recv") for name in ("ynear", "yfar", "zown", "znear", "zfar", "same", "cross")}

        def put(self, o, half, zz, device, recv):
            rows = 64 if half is None else 32
            start = row_of((y + o) % 4, zz, c) + (half or 0) * 32
            ref = self.g.at[pl.ds(pl.multiple_of(start, 32), rows), :]
            cp.remote(ref, ref, device, self.send, self.recv[recv])

        def to_z(self, o):
            for half in (0, 1):
                self.put(o, half, zl, peer("z", 1 + 2 * half), "z" + kind_of[o])

        def to_core(self, o, far):
            self.put(o, None, 1 - zl if far else zl, other, "cross" if far else "same")

        def to_y(self, *order):
            for o in order:
                self.put(0, None, zl, peer("y", o), "y" + kind_of[o])

        def start(self, *order):
            self.to_y(*order)
            self.to_z(0)
            self.to_core(0, False)

        def wait(self, way, kind, rows):
            cp.wait(self.g.at[pl.ds(0, rows * len(kinds[kind])), :], self.recv[way + kind])

        def from_y(self, kind):
            self.wait("y", kind, 64)
            for o in kinds[kind]:
                self.to_z(o)
                self.to_core(o, False)

        def from_z(self, kind):
            self.wait("z", kind, 64)
            for o in kinds[kind]:
                self.to_core(o, True)

        def complete(self, half):
            cp.wait(self.g.at[0:256, :], self.recv[half])

    with scope("signals"):
        barrier = pltpu.get_barrier_semaphore()
        partners = group_peers + [peer("x", o) for o in (1, 2, 3)] + [device_of(x, y, (zmate + 2) % 4, c), peer("z", 2)]
        for p in partners:
            pl.semaphore_signal(barrier, inc=1, device_id=p, device_id_type=MESH)
    own_rows = pl.ds(row_of(y, zl, c), 64)
    _ = [cp.here(wv.at[:, BLOCK * b : BLOCK * b + BLOCK], gv.at[j, own_rows, :], j > 0) for j, b in enumerate(SEQUENCE)]
    wv_sem = lsem.at[cp.k - 1]
    load_wo = cp.here(wo, go.at[own_rows, :])
    load_wk = cp.here(wk, wk_v.at[pl.ds(0, 64), :])
    load_query = cp.here(query_h, query)
    load_slot = cp.here(vslot_h, vslot)
    load_emb = cp.here(emb_h, emb)
    load_tok = cp.here(tok.at[:, :, :, c], tokv.at[0])

    with scope("w_barrier"):
        pl.semaphore_wait(barrier, len(partners))

    with scope("gatherA"):
        send_v, send_o = cp.new("send"), cp.new("send")
        cp.wait(gv.at[:, 0:64, :], wv_sem)
        A = [Gather(gv.at[0], None, send_v)]
        A[0].start(2, 1, 3)

    head_lane = lax.broadcasted_iota(jnp.int32, (HEADS, D), 1) // 64
    head_row = lax.broadcasted_iota(jnp.int32, (HEADS, D), 0)
    own_head = head_lane == head_row
    wk_v[64:128, :] = jnp.zeros((64, D), BF16)
    load_query.wait()
    q8 = query[...].astype(F32)
    q_row = jnp.concatenate([q8[k : k + 1, :] for k in range(8)], axis=1)
    q_matrix = jnp.where(own_head, q_row, 0.0).astype(BF16)
    with scope("w_wk"):
        load_wk.wait()
    nt = (((1,), (1,)), ((), ()))
    qk = lax.dot_general(q_matrix, wk_v[...], nt, preferred_element_type=F32) * 0.125
    qk_o[...] = qk[:8] + pltpu.roll(qk[8:], 64, axis=1)

    mine = (zl * 4 + y) * 2 + c
    qk_send, qk_recv = cp.new("send"), cp.new("recv")
    for p in group_peers:
        cp.remote(qk_o, qkg.at[mine], p, qk_send, qk_recv)
    with scope("gatherA2"):
        tok_send, tok_recv = cp.new("send"), cp.new("recv")
        cp.remote(tok.at[:, :, :, 1 - c], tokv.at[1], other, tok_send, tok_recv)
        for b in range(1, 4):
            A.append(Gather(gv.at[b], None, send_v))
            A[b].start(2, 1, 3)
        B = Gather(go, load_wo, send_o)
        B.start(1, 3)

    position = vx * 16 + vy
    partner_pos = position + 1 - 2 * c
    load_slot.wait()
    n_vars = vslot.shape[1]
    row8 = lax.broadcasted_iota(jnp.int32, (8, n_vars), 0)
    slot_id = jnp.where(row8 == 0, position, jnp.where(row8 == 1, partner_pos, -1))
    match = (vslot[...] == slot_id).astype(F32)
    load_emb.wait()
    er[...] = jnp.dot(match.astype(BF16), emb[...], preferred_element_type=F32)
    used[...] = jnp.broadcast_to(jnp.sum(match, axis=1, keepdims=True), (8, 128))

    def mix(k):
        def step(i, carry):
            at = pl.ds(pl.multiple_of(k * 512 + i * 64, 64), 64)
            half = pl.ds(2 * (i % 2), 2)
            t = tokv[k, i // 2, half].astype(F32).reshape(64, D)
            mixed[at, :] = (t + er[k : k + 1, :]).astype(BF16)
            t = tokv[k, half, :, i // 2].astype(F32).reshape(64, D)
            mixed_y[at, :] = (t + er[k : k + 1, :]).astype(BF16)
            return carry

        lax.fori_loop(0, 8, step, 0)

    def score(k):
        d = lax.dot_general(mixed[k * 512 : k * 512 + 512, :], qkt[...], nt, preferred_element_type=F32)
        d = d + pltpu.roll(d, 112, axis=1)
        sc[k] = jnp.where(used[k : k + 1, :] > 0, d, BIG).reshape(4, 4, 4, 8, 128)

    def pair_stats(i, carry):
        s0, s1_ = sc[0, i].reshape(128, 128), sc[1, i].reshape(128, 128)
        m = jnp.maximum(s0, s1_)
        w0 = used[0:1, :] * jnp.exp(s0 - m)
        w1 = used[1:2, :] * jnp.exp(s1_ - m)
        st0[i] = pack_stats(m, w0 + w1).reshape(4, 4, 8, 128)
        sc[0, i] = w0.reshape(4, 4, 8, 128)
        sc[1, i] = w1.reshape(4, 4, 8, 128)
        return carry

    def product(j, half, source, start, rows):
        at = pl.ds(pl.multiple_of(start, rows), rows)
        features = pl.ds(pl.multiple_of(half * 512, 512), 512)
        return jnp.dot(source[at, features], gv[j, features, :], preferred_element_type=F32)

    def early(j):
        def step(i, carry):
            at = pl.ds(pl.multiple_of(i * 512, 512), 512)
            V[j, at, :] = product(j, zl, mixed if SEQUENCE[j] < 2 else mixed_y, i * 512, 512)
            return carry

        lax.fori_loop(0, 2, step, 0)

    def weighted(j, dim, index):
        total = None
        for k in range(2):
            start = k * 512 + index * 128
            r = product(j, 1 - zl, mixed if dim == "x" else mixed_y, start, 128)
            r = r + V[j, pl.ds(pl.multiple_of(start, 128), 128), :]
            w = (sc[k, index] if dim == "x" else sc[k, :, :, index]).reshape(128, 128)
            r = r * expand(w, BLOCK * SEQUENCE[j], BLOCK)
            total = r if total is None else total + r
        return total

    with scope("mix0"):
        load_tok.wait()
        mix(0)
    with scope("y0"):
        A[0].from_y("near")
    with scope("w_tok"):
        cp.wait(tokv.at[1], tok_recv)
    with scope("mix1"):
        mix(1)
    with scope("o0"):
        A[0].from_y("far")
    with scope("z00"):
        A[0].from_z("own")
    with scope("y1"):
        A[1].from_y("near")
        A[1].from_z("own")
    with scope("o1"):
        A[1].from_y("far")
    with scope("s0"):
        A[0].complete("same")
    with scope("early0"):
        early(0)
    with scope("w_qk"):
        cp.wait(qkg.at[0:15], qk_recv)
    with scope("qkt"):
        qkg[mine] = qk_o[...]
        left = lax.broadcasted_iota(jnp.int32, (8, 128), 1) < 64
        columns = []
        for k in range(8):
            a, b = qkg[2 * k], qkg[2 * k + 1]
            top = jnp.where(left, a, pltpu.roll(b, 64, axis=1))
            bottom = jnp.where(left, pltpu.roll(a, 64, axis=1), b)
            columns.append(jnp.concatenate([top, bottom], axis=0))
        q_keys = jnp.concatenate(columns, axis=1)
        q_high = q_keys.astype(BF16)
        q_low = (q_keys - q_high.astype(F32)).astype(BF16)
        qkt[...] = jnp.concatenate([q_high, q_low, jnp.zeros((96, D), BF16)], axis=0)
    with scope("score0"):
        score(0)
    with scope("y2"):
        A[2].from_y("near")
        A[2].from_z("own")
    with scope("o2"):
        A[2].from_y("far")
    with scope("zy0"):
        A[0].from_z("near")
    with scope("score1"):
        score(1)
    with scope("zo0"):
        A[0].from_z("far")
    with scope("pair_stats"):
        lax.fori_loop(0, 4, pair_stats, 0)
    with scope("y3"):
        A[3].from_y("near")
        A[3].from_z("own")
    with scope("o3"):
        A[3].from_y("far")

    def stats0():
        for t, (l0, w, dims) in zip(T, PARTS):
            axis = NAT.index(dims[0])
            for o in (1, 2, 3):
                rows = pick(st0, axis, (me[dims[0]] + o) % 4, slice(None), 3)
                t["ts1"][o - 1] = fold(rows)
        for t, (l0, w, dims) in zip(T, PARTS):
            t["send1"], t["recv1"] = cp.new("send"), cp.new("recv")
            for o in (1, 2, 3):
                cp.remote(t["ts1"].at[o - 1], t["tr1"].at[o - 1], peer(dims[0], o), t["send1"], t["recv1"])

    plane = sorted([(o, p) for o in range(4) for p in range(4) if o or p], key=lambda q: -sum(min(k, 4 - k) for k in q))

    def rest_of(dims):
        return [d for d in NAT if d != dims[0]]

    def plane_peer(dims, o, p):
        at = dict(me)
        first, second = rest_of(dims)
        at[first], at[second] = (me[first] + o) % 4, (me[second] + p) % 4
        return at[first], at[second], device_of(at["x"], at["y"], at["z"], c)

    def stats1():
        for t, (l0, w, dims) in zip(T, PARTS):
            cp.wait(t["tr1"], t["recv1"])
            own = pick(st0, NAT.index(dims[0]), me[dims[0]], slice(None), 3)
            m, l, scales = merge_stats([own] + [unfold(t["tr1"][o]) for o in range(3)])
            t["st1"][...] = pack_stats(m, l).reshape(4, 4, 8, 128)
            for k, a in enumerate(scales):
                t["a1"][k] = a
        for t, (l0, w, dims) in zip(T, PARTS):
            t["send2"], t["recv2"] = cp.new("send"), cp.new("recv")
            for n, (o, p) in enumerate(plane):
                i, k, device = plane_peer(dims, o, p)
                cp.remote(t["st1"].at[i, k], t["tr2"].at[n], device, t["send2"], t["recv2"])

    def expand1():
        for t, (l0, w, dims) in zip(T, PARTS):
            for k in range(4):
                t["ax1"][k] = expand(t["a1"][k], l0, w)

    def stats2():
        for t, (l0, w, dims) in zip(T, PARTS):
            cp.wait(t["tr2"], t["recv2"])
            first, second = rest_of(dims)
            m, l, scales = merge_stats([t["st1"][me[first], me[second]]] + [t["tr2"][n] for n in range(15)])
            inverse = 1.0 / l
            for k, a in enumerate(scales):
                t["ax2"][k] = expand(a * inverse, l0, w)

    send1, recv1 = cp.new("send"), [cp.new("recv") for _ in range(4)]

    def reduce1(j):
        dim = PARTS[SEQUENCE[j] // 2][2][0]

        def send(*offsets):
            for o in offsets:
                cp.remote(s1.at[j, o - 1], r1.at[j, o - 1], peer(dim, o), send1, recv1[j])

        for o in (2, 1):
            s1[j, o - 1] = weighted(j, dim, (me[dim] + o) % 4).astype(BF16)
        if j == 3:
            send(2, 1)
        s1[j, 2] = weighted(j, dim, (me[dim] + 3) % 4).astype(BF16)
        own1[j] = weighted(j, dim, me[dim])
        if j == 3:
            send(3)
        else:
            send(2, 1, 3)

    with scope("stats0"):
        stats0()
        B.to_y(2)
    with scope("zy1"):
        A[1].from_z("near")
    with scope("s1"):
        A[1].complete("same")
    with scope("early1"):
        early(1)
    with scope("zo1"):
        A[1].from_z("far")
    with scope("c0"):
        A[0].complete("cross")
    with scope("late0"):
        reduce1(0)
    with scope("s2"):
        A[2].complete("same")
    with scope("early2"):
        early(2)
    with scope("zy2"):
        A[2].from_z("near")
    with scope("zo2"):
        A[2].from_z("far")
    with scope("c1"):
        A[1].complete("cross")
    with scope("late1"):
        reduce1(1)
    with scope("s3"):
        A[3].complete("same")
    with scope("early3"):
        early(3)
    with scope("zy3"):
        A[3].from_z("near")
    with scope("zo3"):
        A[3].from_z("far")
    with scope("c2"):
        A[2].complete("cross")
    with scope("late2"):
        reduce1(2)
    with scope("B_y"):
        B.from_z("own")
        B.from_y("near")
    with scope("c3"):
        A[3].complete("cross")
    with scope("late3"):
        reduce1(3)
    with scope("stats1"):
        stats1()
    with scope("B_o"):
        B.from_y("far")
    with scope("expand1"):
        expand1()

    send2, recv2 = cp.new("send"), [cp.new("recv")] * 3 + [cp.new("recv")]

    def part_of(j):
        b = SEQUENCE[j]
        t, (l0, _, dims) = T[b // 2], PARTS[b // 2]
        return t, dims, slice(BLOCK * b - l0, BLOCK * b - l0 + BLOCK)

    def reduce2(j):
        t, dims, cols = part_of(j)
        with scope("w_c1"):
            cp.wait(r1.at[j], recv1[j])
        total = t["ax1"][0, :, cols] * own1[j]
        for o in range(3):
            total = total + t["ax1"][o + 1, :, cols] * r1[j, o].astype(F32)
        total = total.reshape(4, 4, 8, BLOCK)
        m1[j] = total
        s2[j] = total.astype(BF16)
        for n, (o, p) in enumerate(plane):
            i, k, device = plane_peer(dims, o, p)
            cp.remote(s2.at[j, i, k], r2.at[j, n], device, send2, recv2[j])

    def result(j):
        t, dims, cols = part_of(j)
        first, second = rest_of(dims)
        with scope("w_c2"):
            if j == 0:
                cp.wait(r2.at[0:3], recv2[0])
            elif j == 3:
                cp.wait(r2.at[3], recv2[3])
        total = t["ax2"][0, :, cols] * m1[j, me[first], me[second]]
        for n in range(15):
            total = total + t["ax2"][n + 1, :, cols] * r2[j, n].astype(F32)
        return total

    for j in range(3):
        reduce2(j)
    reduce2(3)
    with scope("B_z"):
        B.from_z("near")
    with scope("B_z2"):
        B.from_z("far")
    with scope("stats2"):
        stats2()
    def projected(j, context):
        rows = slice(BLOCK * SEQUENCE[j], BLOCK * SEQUENCE[j] + BLOCK)
        return jnp.dot(context.astype(BF16), go[rows, :], preferred_element_type=F32)

    context = [result(j) for j in (0, 1, 2)]
    with scope("B_c"):
        B.complete("same")
        B.complete("cross")
    with scope("tail0"):
        partial[...] = sum(projected(j, context[j]) for j in (0, 1, 2))
    with scope("w_sends0"):
        cp.wait(gv.at[:, 0:960, :], send_v)
        cp.wait(go.at[0:960, :], send_o)
        cp.wait(qkg.at[0:15], qk_send)
        cp.wait(tokv.at[1], tok_send)
        cp.wait(s1, send1)
        for t in T:
            cp.wait(t["ts1"], t["send1"])
            cp.wait(t["tr2"], t["send2"])
    last = result(3)
    with scope("tail"):
        out[...] = (partial[...] + projected(3, last)).astype(BF16)
    with scope("w_sends"):
        cp.wait(r2, send2)


def shards(tokens, var_embed, query, key_weight, value_weight, out_weight, var_slot):
    vm = pl.BlockSpec(memory_space=pltpu.VMEM)
    hbm = pl.BlockSpec(memory_space=pl.ANY)
    V = pltpu.VMEM
    part = []
    for _, w, _ in PARTS:
        part += [
            V((3, 32, 128), F32), V((3, 32, 128), F32), V((15, 8, 128), F32),
            V((4, 128, w), F32), V((16, 8, w), F32), V((4, 4, 8, 128), F32), V((4, 128, 128), F32),
        ]
    result = pl.pallas_call(
        kernel,
        out_shape=jax.ShapeDtypeStruct((8, D), BF16),
        in_specs=[hbm] * 7,
        out_specs=vm,
        scratch_shapes=[
            V((91, D), BF16), V((8, 128), BF16), V((1, 91), jnp.int32), V((128, D), BF16), V((2, 4, 4, 4, 8, D), BF16),
            V((1024, D), BF16), V((1024, D), BF16), V((4, D, BLOCK), BF16), V((D, D), BF16),
            V((4, 1024, BLOCK), F32), V((4, 128, BLOCK), F32), V((4, 4, 4, 8, 128), F32),
            V((8, 128), F32), V((16, 8, 128), F32), V((128, D), BF16), V((8, D), F32), V((8, 128), F32),
            V((2, 4, 4, 4, 8, 128), F32),
            V((4, 3, 128, BLOCK), BF16), V((4, 3, 128, BLOCK), BF16),
            V((4, 4, 4, 8, BLOCK), BF16), V((4, 15, 8, BLOCK), BF16), V((4, 4, 4, 8, BLOCK), F32),
            V((8, D), F32), *part,
            pltpu.SemaphoreType.DMA((SENDS,)), pltpu.SemaphoreType.DMA((RECVS,)), pltpu.SemaphoreType.DMA((7,)),
        ],
        compiler_params=pltpu.CompilerParams(
            collective_id=0, has_side_effects=True, vmem_limit_bytes=60 * 1024 * 1024
        ),
    )(
        tokens.reshape(4, 4, 4, 2, 8, D), var_embed, query.reshape(8, 128), key_weight, value_weight, out_weight,
        var_slot.reshape(1, -1),
    )
    return result.reshape(1, 8, D)


def solution(mesh):
    placed = (
        P(("vx", "vy"), None, None, None), P(), P(), P("vy", None), P("vy", None), P("vy", None), P(),
    )
    return jax.shard_map(
        shards, mesh=mesh, in_specs=placed, out_specs=P(None, ("vx", "vy"), None), check_vma=False
    )
```

```python
import contextlib
import functools

import jax
import jax.numpy as jnp
from jax import lax
from jax.experimental import pallas as pl
from jax.experimental.pallas import tpu as pltpu
from jax.sharding import PartitionSpec as P

MESH = pl.DeviceIdType.MESH
F32, BF16 = jnp.float32, jnp.bfloat16
HEADS = 16
D = 1024
BIG = -1e30

NAT = ("x", "z", "y")
PARTS = ((0, 512, ("x", "y", "z")), (512, 512, ("y", "x", "z")))
SEQUENCE = (0, 2, 1, 3)
BLOCK = 256
SENDS, RECVS = 10, 49


def scope(name):
    return contextlib.nullcontext()


def device_of(x, y, z, c):
    return (x * 2 + z // 2, (z % 2) * 8 + y * 2 + c)


class Copies:
    def __init__(self, send, recv, local):
        self.sems = {"send": send, "recv": recv}
        self.local, self.k, self.used = local, 0, {"send": 0, "recv": 0}

    def new(self, side):
        self.used[side] += 1
        return self.sems[side].at[self.used[side] - 1]

    def remote(self, src, dst, device, send, recv):
        pltpu.make_async_remote_copy(
            src_ref=src, dst_ref=dst, send_sem=send, recv_sem=recv, device_id=device, device_id_type=MESH
        ).start()

    def here(self, src, dst):
        copy = pltpu.make_async_copy(src, dst, self.local.at[self.k])
        self.k += 1
        copy.start()
        return copy

    def wait(self, like, sem):
        pltpu.make_async_copy(like, like, sem).wait()


def lanes_iota(rows):
    return lax.broadcasted_iota(jnp.int32, (rows, 128), 1)


def expand(a, l0, w):
    half = lanes_iota(a.shape[0]) // 64
    tiles = [jnp.take_along_axis(a, half + 2 * t, axis=1, mode="promise_in_bounds") for t in range(l0 // 128, (l0 + w) // 128)]
    return jnp.concatenate(tiles, axis=1)


def fold(rows):
    lane = lanes_iota(rows.shape[0])
    rows = jnp.where(lane < 32, rows, 0.0)
    q = rows.shape[0] // 4
    out = rows[:q]
    for g in range(1, 4):
        out = out + pltpu.roll(rows[g * q : (g + 1) * q], 32 * g, axis=1)
    return out


def unfold(packed):
    pieces = [packed]
    for g in range(1, 4):
        pieces.append(pltpu.roll(packed, 128 - 32 * g, axis=1))
    return jnp.concatenate(pieces, axis=0)


def pack_stats(m, l):
    lane = lanes_iota(m.shape[0])
    return jnp.where(lane < 16, m, jnp.where(lane < 32, pltpu.roll(l, 16, axis=1), 0.0))


def merge_stats(stats):
    m = functools.reduce(jnp.maximum, stats)
    scales = [jnp.exp(s - m) for s in stats]
    l = sum(a * pltpu.roll(s, 112, axis=1) for a, s in zip(scales, stats))
    return m, l, scales


def pick(ref, axis, index, lanes, ndim):
    where = [slice(None)] * (ndim + 2)
    where[axis] = index
    where[-1] = lanes
    got = ref[tuple(where)]
    return got.reshape(-1, got.shape[-1])


def kernel(tok, emb_h, query_h, wk, wv, wo, vslot_h, out, emb, query, vslot, wk_v, tokv, mixed, mixed_y,
           gv, go, V, own1, st0, qk_o, qkg, qkt, er, used, sc, s1, r1, s2, r2, m1, partial, *rest):
    ssem, rsem, lsem = rest[-3:]
    names = ("ts1", "tr1", "tr2", "ax1", "ax2", "st1", "a1")
    T = [dict(zip(names, rest[i * 7 : (i + 1) * 7])) for i in range(len(PARTS))]
    cp = Copies(ssem, rsem, lsem)

    vx, vy = lax.axis_index("vx"), lax.axis_index("vy")
    x, z = vx // 2, (vx % 2) * 2 + vy // 8
    y, c = (vy // 2) % 4, vy % 2
    zl = z % 2
    zmate = z + 1 - 2 * zl
    me = {"x": x, "y": y, "z": z}

    def peer(dim, offset):
        at = dict(me)
        at[dim] = (me[dim] + offset) % 4
        return device_of(at["x"], at["y"], at["z"], c)

    other = device_of(x, y, z, 1 - c)
    group_peers = [other, device_of(x, y, zmate, c), device_of(x, y, zmate, 1 - c)]
    for o in (1, 2, 3):
        group_peers += [device_of(x, (y + o) % 4, zz, cc) for zz in (z, zmate) for cc in (c, 1 - c)]

    def row_of(yy, zz, cc):
        return pl.multiple_of(((zz * 4 + yy) * 2 + cc) * 64, 64)

    kinds = {"own": (0,), "near": (3, 1), "far": (2,)}
    kind_of = {0: "own", 1: "near", 2: "far", 3: "near"}

    class Gather:
        def __init__(self, g, local, send):
            self.g, self.send = g, send
            local.wait()
            self.recv = {name: cp.new("recv") for name in ("ynear", "yfar", "zown", "znear", "zfar", "same", "cross")}

        def put(self, o, half, zz, device, recv):
            rows = 64 if half is None else 32
            start = row_of((y + o) % 4, zz, c) + (half or 0) * 32
            ref = self.g.at[pl.ds(pl.multiple_of(start, 32), rows), :]
            cp.remote(ref, ref, device, self.send, self.recv[recv])

        def to_z(self, o):
            for half in (0, 1):
                self.put(o, half, zl, peer("z", 1 + 2 * half), "z" + kind_of[o])

        def to_core(self, o, far):
            self.put(o, None, 1 - zl if far else zl, other, "cross" if far else "same")

        def to_y(self, *order):
            for o in order:
                self.put(0, None, zl, peer("y", o), "y" + kind_of[o])

        def start(self, *order):
            self.to_y(*order)
            self.to_z(0)
            self.to_core(0, False)

        def wait(self, way, kind, rows):
            cp.wait(self.g.at[pl.ds(0, rows * len(kinds[kind])), :], self.recv[way + kind])

        def from_y(self, kind):
            self.wait("y", kind, 64)
            for o in kinds[kind]:
                self.to_z(o)
                self.to_core(o, False)

        def from_z(self, kind):
            self.wait("z", kind, 64)
            for o in kinds[kind]:
                self.to_core(o, True)

        def complete(self, half):
            cp.wait(self.g.at[0:256, :], self.recv[half])

    with scope("signals"):
        barrier = pltpu.get_barrier_semaphore()
        partners = group_peers + [peer("x", o) for o in (1, 2, 3)] + [device_of(x, y, (zmate + 2) % 4, c), peer("z", 2)]
        for p in partners:
            pl.semaphore_signal(barrier, inc=1, device_id=p, device_id_type=MESH)
    own_rows = pl.ds(row_of(y, zl, c), 64)
    load_wv = [cp.here(wv.at[:, BLOCK * b : BLOCK * b + BLOCK], gv.at[j, own_rows, :]) for j, b in enumerate(SEQUENCE)]
    load_wo = cp.here(wo, go.at[own_rows, :])
    load_wk = cp.here(wk, wk_v.at[pl.ds(0, 64), :])
    load_query = cp.here(query_h, query)
    load_slot = cp.here(vslot_h, vslot)
    load_emb = cp.here(emb_h, emb)
    load_tok = cp.here(tok.at[:, :, :, c], tokv.at[0])

    with scope("w_barrier"):
        pl.semaphore_wait(barrier, len(partners))

    with scope("gatherA"):
        send_v, send_o = cp.new("send"), cp.new("send")
        A = [Gather(gv.at[0], load_wv[0], send_v)]
        A[0].start(2, 1, 3)

    head_lane = lax.broadcasted_iota(jnp.int32, (HEADS, D), 1) // 64
    head_row = lax.broadcasted_iota(jnp.int32, (HEADS, D), 0)
    own_head = head_lane == head_row
    wk_v[64:128, :] = jnp.zeros((64, D), BF16)
    load_query.wait()
    q8 = query[...].astype(F32)
    q_row = jnp.concatenate([q8[k : k + 1, :] for k in range(8)], axis=1)
    q_matrix = jnp.where(own_head, q_row, 0.0).astype(BF16)
    with scope("w_wk"):
        load_wk.wait()
    nt = (((1,), (1,)), ((), ()))
    qk = lax.dot_general(q_matrix, wk_v[...], nt, preferred_element_type=F32) * 0.125
    qk_o[...] = qk[:8] + pltpu.roll(qk[8:], 64, axis=1)

    mine = (zl * 4 + y) * 2 + c
    qk_send, qk_recv = cp.new("send"), cp.new("recv")
    for p in group_peers:
        cp.remote(qk_o, qkg.at[mine], p, qk_send, qk_recv)
    with scope("gatherA2"):
        tok_send, tok_recv = cp.new("send"), cp.new("recv")
        cp.remote(tok.at[:, :, :, 1 - c], tokv.at[1], other, tok_send, tok_recv)
        for b in range(1, 4):
            A.append(Gather(gv.at[b], load_wv[b], send_v))
            A[b].start(2, 1, 3)
        B = Gather(go, load_wo, send_o)
        B.start(1, 3)

    position = vx * 16 + vy
    partner_pos = position + 1 - 2 * c
    load_slot.wait()
    n_vars = vslot.shape[1]
    row8 = lax.broadcasted_iota(jnp.int32, (8, n_vars), 0)
    slot_id = jnp.where(row8 == 0, position, jnp.where(row8 == 1, partner_pos, -1))
    match = (vslot[...] == slot_id).astype(F32)
    load_emb.wait()
    er[...] = jnp.dot(match.astype(BF16), emb[...], preferred_element_type=F32)
    used[...] = jnp.broadcast_to(jnp.sum(match, axis=1, keepdims=True), (8, 128))

    def mix(k):
        def step(i, carry):
            at = pl.ds(pl.multiple_of(k * 512 + i * 64, 64), 64)
            half = pl.ds(2 * (i % 2), 2)
            t = tokv[k, i // 2, half].astype(F32).reshape(64, D)
            mixed[at, :] = (t + er[k : k + 1, :]).astype(BF16)
            t = tokv[k, half, :, i // 2].astype(F32).reshape(64, D)
            mixed_y[at, :] = (t + er[k : k + 1, :]).astype(BF16)
            return carry

        lax.fori_loop(0, 8, step, 0)

    def score():
        d = lax.dot_general(mixed[...], qkt[...], nt, preferred_element_type=F32)
        d = d + pltpu.roll(d, 112, axis=1)
        for k in range(2):
            half = d[512 * k : 512 * k + 512]
            sc[k] = jnp.where(used[k : k + 1, :] > 0, half, BIG).reshape(4, 4, 4, 8, 128)

    def pair_stats(i, carry):
        s0, s1_ = sc[0, i].reshape(128, 128), sc[1, i].reshape(128, 128)
        m = jnp.maximum(s0, s1_)
        w0 = used[0:1, :] * jnp.exp(s0 - m)
        w1 = used[1:2, :] * jnp.exp(s1_ - m)
        st0[i] = pack_stats(m, w0 + w1).reshape(4, 4, 8, 128)
        sc[0, i] = w0.reshape(4, 4, 8, 128)
        sc[1, i] = w1.reshape(4, 4, 8, 128)
        return carry

    def product(j, half, source, start, rows):
        at = pl.ds(pl.multiple_of(start, rows), rows)
        features = pl.ds(pl.multiple_of(half * 512, 512), 512)
        return jnp.dot(source[at, features], gv[j, features, :], preferred_element_type=F32)

    def early(j):
        def step(i, carry):
            at = pl.ds(pl.multiple_of(i * 512, 512), 512)
            V[j, at, :] = product(j, zl, mixed if SEQUENCE[j] < 2 else mixed_y, i * 512, 512)
            return carry

        lax.fori_loop(0, 2, step, 0)

    def weighted(j, dim, index):
        total = None
        for k in range(2):
            start = k * 512 + index * 128
            r = product(j, 1 - zl, mixed if dim == "x" else mixed_y, start, 128)
            r = r + V[j, pl.ds(pl.multiple_of(start, 128), 128), :]
            w = (sc[k, index] if dim == "x" else sc[k, :, :, index]).reshape(128, 128)
            r = r * expand(w, BLOCK * SEQUENCE[j], BLOCK)
            total = r if total is None else total + r
        return total

    with scope("mix0"):
        load_tok.wait()
        mix(0)
    with scope("y0"):
        A[0].from_y("near")
    with scope("w_tok"):
        cp.wait(tokv.at[1], tok_recv)
    with scope("mix1"):
        mix(1)
    with scope("o0"):
        A[0].from_y("far")
    with scope("z00"):
        A[0].from_z("own")
    with scope("y1"):
        A[1].from_y("near")
        A[1].from_z("own")
    with scope("o1"):
        A[1].from_y("far")
    with scope("s0"):
        A[0].complete("same")
    with scope("early0"):
        early(0)
    with scope("w_qk"):
        cp.wait(qkg.at[0:15], qk_recv)
    with scope("qkt"):
        qkg[mine] = qk_o[...]
        left = lax.broadcasted_iota(jnp.int32, (8, 128), 1) < 64
        columns = []
        for k in range(8):
            a, b = qkg[2 * k], qkg[2 * k + 1]
            top = jnp.where(left, a, pltpu.roll(b, 64, axis=1))
            bottom = jnp.where(left, pltpu.roll(a, 64, axis=1), b)
            columns.append(jnp.concatenate([top, bottom], axis=0))
        q_keys = jnp.concatenate(columns, axis=1)
        q_high = q_keys.astype(BF16)
        q_low = (q_keys - q_high.astype(F32)).astype(BF16)
        qkt[...] = jnp.concatenate([q_high, q_low, jnp.zeros((96, D), BF16)], axis=0)
    with scope("score"):
        score()
    with scope("y2"):
        A[2].from_y("near")
        A[2].from_z("own")
    with scope("o2"):
        A[2].from_y("far")
    with scope("zy0"):
        A[0].from_z("near")
    with scope("zo0"):
        A[0].from_z("far")
    with scope("pair_stats"):
        lax.fori_loop(0, 4, pair_stats, 0)
    with scope("y3"):
        A[3].from_y("near")
        A[3].from_z("own")
    with scope("o3"):
        A[3].from_y("far")

    def stats0():
        for t, (l0, w, dims) in zip(T, PARTS):
            axis = NAT.index(dims[0])
            for o in (1, 2, 3):
                rows = pick(st0, axis, (me[dims[0]] + o) % 4, slice(None), 3)
                t["ts1"][o - 1] = fold(rows)
        for t, (l0, w, dims) in zip(T, PARTS):
            t["send1"], t["recv1"] = cp.new("send"), cp.new("recv")
            for o in (1, 2, 3):
                cp.remote(t["ts1"].at[o - 1], t["tr1"].at[o - 1], peer(dims[0], o), t["send1"], t["recv1"])

    plane = sorted([(o, p) for o in range(4) for p in range(4) if o or p], key=lambda q: -sum(min(k, 4 - k) for k in q))

    def rest_of(dims):
        return [d for d in NAT if d != dims[0]]

    def plane_peer(dims, o, p):
        at = dict(me)
        first, second = rest_of(dims)
        at[first], at[second] = (me[first] + o) % 4, (me[second] + p) % 4
        return at[first], at[second], device_of(at["x"], at["y"], at["z"], c)

    def stats1():
        for t, (l0, w, dims) in zip(T, PARTS):
            cp.wait(t["tr1"], t["recv1"])
            own = pick(st0, NAT.index(dims[0]), me[dims[0]], slice(None), 3)
            m, l, scales = merge_stats([own] + [unfold(t["tr1"][o]) for o in range(3)])
            t["st1"][...] = pack_stats(m, l).reshape(4, 4, 8, 128)
            for k, a in enumerate(scales):
                t["a1"][k] = a
        for t, (l0, w, dims) in zip(T, PARTS):
            t["send2"], t["recv2"] = cp.new("send"), cp.new("recv")
            for n, (o, p) in enumerate(plane):
                i, k, device = plane_peer(dims, o, p)
                cp.remote(t["st1"].at[i, k], t["tr2"].at[n], device, t["send2"], t["recv2"])

    def expand1():
        for t, (l0, w, dims) in zip(T, PARTS):
            for k in range(4):
                t["ax1"][k] = expand(t["a1"][k], l0, w)

    def stats2():
        for t, (l0, w, dims) in zip(T, PARTS):
            cp.wait(t["tr2"], t["recv2"])
            first, second = rest_of(dims)
            m, l, scales = merge_stats([t["st1"][me[first], me[second]]] + [t["tr2"][n] for n in range(15)])
            inverse = 1.0 / l
            for k, a in enumerate(scales):
                t["ax2"][k] = expand(a * inverse, l0, w)

    send1, recv1 = cp.new("send"), [cp.new("recv") for _ in range(4)]

    def reduce1(j):
        dim = PARTS[SEQUENCE[j] // 2][2][0]

        def send(*offsets):
            for o in offsets:
                cp.remote(s1.at[j, o - 1], r1.at[j, o - 1], peer(dim, o), send1, recv1[j])

        for o in (2, 1):
            s1[j, o - 1] = weighted(j, dim, (me[dim] + o) % 4).astype(BF16)
        if j == 3:
            send(2, 1)
        s1[j, 2] = weighted(j, dim, (me[dim] + 3) % 4).astype(BF16)
        own1[j] = weighted(j, dim, me[dim])
        if j == 3:
            send(3)
        else:
            send(2, 1, 3)

    with scope("stats0"):
        stats0()
        B.to_y(2)
    with scope("zy1"):
        A[1].from_z("near")
    with scope("s1"):
        A[1].complete("same")
    with scope("early1"):
        early(1)
    with scope("zo1"):
        A[1].from_z("far")
    with scope("c0"):
        A[0].complete("cross")
    with scope("late0"):
        reduce1(0)
    with scope("s2"):
        A[2].complete("same")
    with scope("early2"):
        early(2)
    with scope("zy2"):
        A[2].from_z("near")
    with scope("zo2"):
        A[2].from_z("far")
    with scope("c1"):
        A[1].complete("cross")
    with scope("late1"):
        reduce1(1)
    with scope("s3"):
        A[3].complete("same")
    with scope("early3"):
        early(3)
    with scope("zy3"):
        A[3].from_z("near")
    with scope("zo3"):
        A[3].from_z("far")
    with scope("c2"):
        A[2].complete("cross")
    with scope("late2"):
        reduce1(2)
    with scope("B_y"):
        B.from_z("own")
        B.from_y("near")
    with scope("c3"):
        A[3].complete("cross")
    with scope("late3"):
        reduce1(3)
    with scope("stats1"):
        stats1()
    with scope("B_o"):
        B.from_y("far")
    with scope("expand1"):
        expand1()

    send2, recv2 = cp.new("send"), [cp.new("recv") for _ in range(4)]

    def part_of(j):
        b = SEQUENCE[j]
        t, (l0, _, dims) = T[b // 2], PARTS[b // 2]
        return t, dims, slice(BLOCK * b - l0, BLOCK * b - l0 + BLOCK)

    def reduce2(j):
        t, dims, cols = part_of(j)
        with scope("w_c1"):
            cp.wait(r1.at[j], recv1[j])
        total = t["ax1"][0, :, cols] * own1[j]
        for o in range(3):
            total = total + t["ax1"][o + 1, :, cols] * r1[j, o].astype(F32)
        total = total.reshape(4, 4, 8, BLOCK)
        m1[j] = total
        s2[j] = total.astype(BF16)
        for n, (o, p) in enumerate(plane):
            i, k, device = plane_peer(dims, o, p)
            cp.remote(s2.at[j, i, k], r2.at[j, n], device, send2, recv2[j])

    def result(j):
        t, dims, cols = part_of(j)
        first, second = rest_of(dims)
        with scope("w_c2"):
            cp.wait(r2.at[j], recv2[j])
        total = t["ax2"][0, :, cols] * m1[j, me[first], me[second]]
        for n in range(15):
            total = total + t["ax2"][n + 1, :, cols] * r2[j, n].astype(F32)
        return total

    for j in range(3):
        reduce2(j)
    reduce2(3)
    with scope("B_z"):
        B.from_z("near")
    with scope("B_z2"):
        B.from_z("far")
    with scope("stats2"):
        stats2()
    def projected(j, context):
        rows = slice(BLOCK * SEQUENCE[j], BLOCK * SEQUENCE[j] + BLOCK)
        return jnp.dot(context.astype(BF16), go[rows, :], preferred_element_type=F32)

    context = [result(j) for j in (0, 1, 2)]
    with scope("B_c"):
        B.complete("same")
        B.complete("cross")
    with scope("tail0"):
        partial[...] = sum(projected(j, context[j]) for j in (0, 1, 2))
    with scope("w_sends0"):
        cp.wait(gv.at[:, 0:960, :], send_v)
        cp.wait(go.at[0:960, :], send_o)
        cp.wait(qkg.at[0:15], qk_send)
        cp.wait(tokv.at[1], tok_send)
        cp.wait(s1, send1)
        for t in T:
            cp.wait(t["ts1"], t["send1"])
            cp.wait(t["tr2"], t["send2"])
    last = result(3)
    with scope("tail"):
        out[...] = (partial[...] + projected(3, last)).astype(BF16)
    with scope("w_sends"):
        cp.wait(r2, send2)


def shards(tokens, var_embed, query, key_weight, value_weight, out_weight, var_slot):
    vm = pl.BlockSpec(memory_space=pltpu.VMEM)
    hbm = pl.BlockSpec(memory_space=pl.ANY)
    V = pltpu.VMEM
    part = []
    for _, w, _ in PARTS:
        part += [
            V((3, 32, 128), F32), V((3, 32, 128), F32), V((15, 8, 128), F32),
            V((4, 128, w), F32), V((16, 8, w), F32), V((4, 4, 8, 128), F32), V((4, 128, 128), F32),
        ]
    result = pl.pallas_call(
        kernel,
        out_shape=jax.ShapeDtypeStruct((8, D), BF16),
        in_specs=[hbm] * 7,
        out_specs=vm,
        scratch_shapes=[
            V((91, D), BF16), V((8, 128), BF16), V((1, 91), jnp.int32), V((128, D), BF16), V((2, 4, 4, 4, 8, D), BF16),
            V((1024, D), BF16), V((1024, D), BF16), V((4, D, BLOCK), BF16), V((D, D), BF16),
            V((4, 1024, BLOCK), F32), V((4, 128, BLOCK), F32), V((4, 4, 4, 8, 128), F32),
            V((8, 128), F32), V((16, 8, 128), F32), V((128, D), BF16), V((8, D), F32), V((8, 128), F32),
            V((2, 4, 4, 4, 8, 128), F32),
            V((4, 3, 128, BLOCK), BF16), V((4, 3, 128, BLOCK), BF16),
            V((4, 4, 4, 8, BLOCK), BF16), V((4, 15, 8, BLOCK), BF16), V((4, 4, 4, 8, BLOCK), F32),
            V((8, D), F32), *part,
            pltpu.SemaphoreType.DMA((SENDS,)), pltpu.SemaphoreType.DMA((RECVS,)), pltpu.SemaphoreType.DMA((10,)),
        ],
        compiler_params=pltpu.CompilerParams(
            collective_id=0, has_side_effects=True, vmem_limit_bytes=60 * 1024 * 1024
        ),
    )(
        tokens.reshape(4, 4, 4, 2, 8, D), var_embed, query.reshape(8, 128), key_weight, value_weight, out_weight,
        var_slot.reshape(1, -1),
    )
    return result.reshape(1, 8, D)


def solution(mesh):
    placed = (
        P(("vx", "vy"), None, None, None), P(), P(), P("vy", None), P("vy", None), P("vy", None), P(),
    )
    return jax.shard_map(
        shards, mesh=mesh, in_specs=placed, out_specs=P(None, ("vx", "vy"), None), check_vma=False
    )
```
